768 devices in a mesh: blk: 64 (over x, y, core), sub: 12 (over z).
Axes of the slice: x: 4, y: 8, z: 12, core: 2. Of those that a mesh axis runs over, the one named last changes fastest.
Arguments:
- flow_state: float32 [6, 512, 8, 1536], P(None, 'blk', None, 'sub'), may hold values from -6 to 6
- timestep: float32 [512, 8, 1536], P('blk', None, 'sub'), may hold values from 0.05 to 0.3
- coupling: float32 [3, 6, 6], replicated, may hold values from -2.5 to 2.5
- face_type: int32 [64, 2], P('blk'), may hold values from 0 to 3
- face_rot: int32 [64, 2], P('blk'), may hold values from 0 to 3
Outputs:
- updated: float32 [6, 512, 8, 1536], P(None, 'blk', None, 'sub')
- fine_residual: float32 [6, 512, 8, 1536], P(None, 'blk', None, 'sub')
The draws below stay inside these ranges and needn't reach their ends.
All inputs are finite; a program needn't handle non-finite values.
Results may differ from the reference program's by a relative error of at most 0.0003.
Values sent between devices are 32-bit elements; how exact they have to be, the bound alone decides.
No kernel may reach another device: no remote copies, remote signals or barrier semaphores. Data moves between devices by JAX's collectives and lax.ppermute only.
A program may use at most 64 MiB of HBM per device.

```python
import math
import jax
import jax.numpy as jnp
from jax import lax

VARS = 6
CJ = 8
BLOCKS = 64
NI = 512
NK = 1536


def with_ends(entries, own_key, low, high):
    longest = entries.shape.index(max(entries.shape))
    spots = []
    for shift in (0, 1):
        where = [jax.random.randint(jax.random.fold_in(own_key, axis), (), 0, length) for axis, length in enumerate(entries.shape)]
        where[longest] = (where[longest] + shift) % entries.shape[longest]
        spots.append(tuple(where))
    return entries.at[spots[0]].set(low).at[spots[1]].set(high)


def steps_of(stream_key, shape, pieces, low, top_value):
    level, own = 1.0, jax.random.fold_in(stream_key, 6)
    for position, shards_of in pieces:
        steps = jnp.exp(jax.random.uniform(jax.random.fold_in(own, position), (shards_of,), jnp.float32, low / len(pieces), top_value / len(pieces)))
        level = level * jnp.repeat(steps, shape[position] // shards_of).reshape([-1 if axis == position else 1 for axis in range(len(shape))])
    return level


def centred(own_key, extent, deviation, limit, shards=(), held_as=jnp.bfloat16):
    drawn = jax.random.normal(own_key, extent, jnp.float32) * deviation
    if len(shards) > 0:
        drawn = steps_of(own_key, extent, shards, -0.22, 0.18) * drawn
    return jnp.clip(drawn, min=-limit, max=limit).astype(held_as)


def setup_inputs(seed: int = 0) -> dict:
    seeds = jax.random.split(jax.random.key(seed), 6)
    return {
        "flow_state": centred(seeds[0], (VARS, NI, CJ, NK), 1.0, 6.0, ((1, 64), (3, 12)), jnp.float32),
        "timestep": jnp.clip(jnp.exp(math.log(0.3) - 1.7917595 * jax.random.uniform(seeds[1], (NI, CJ, NK), jnp.float32) ** steps_of(seeds[1], (NI, CJ, NK), ((0, 64), (2, 12)), -0.2, 0.2)), 0.05, 0.3),
        "coupling": centred(seeds[2], (3, VARS, VARS), VARS ** -0.5, 2.5, (), jnp.float32),
        "face_type": with_ends(jax.random.randint(seeds[3], (BLOCKS, 2), 0, 4), jax.random.fold_in(seeds[3], 1), 0, 3).astype(jnp.int32),
        "face_rot": with_ends(jax.random.randint(seeds[4], (BLOCKS, 2), 0, 4), jax.random.fold_in(seeds[4], 1), 0, 3).astype(jnp.int32),
    }


DAMP_TWO = 0.05
DAMP_FOUR = 0.02
SECTION_COEFFS = (0.4, 1.0)
PRECISE = lax.Precision.HIGHEST


def rotate_plane(plane, rot_code):
    flipped = jnp.where(rot_code % 2 == 1, plane[:, :, ::-1, :], plane)
    turned = jnp.stack([flipped[0], flipped[1], -flipped[3], flipped[2], flipped[4], flipped[5]])
    return jnp.where((rot_code // 2) % 2 == 1, turned, flipped)


def mirrored(rows_in, negated):
    sign_row = jnp.where(jnp.arange(6) == negated, -1.0, 1.0).astype(jnp.float32)
    return rows_in * sign_row[:, None, None, None]


def lower_ghosts(block_cells, prev_last, next_first, kind_code, rot_code):
    wall_rows = mirrored(block_cells[:, :2][:, ::-1], 1)
    picked = jnp.where(kind_code == 0, prev_last, jnp.where(kind_code == 1, next_first[:, ::-1], jnp.where(kind_code == 2, wall_rows, jnp.zeros_like(wall_rows))))
    return rotate_plane(picked, rot_code)


def upper_ghosts(block_cells, prev_last, next_first, kind_code, rot_code):
    wall_rows = mirrored(block_cells[:, -2:][:, ::-1], 1)
    picked = jnp.where(kind_code == 0, next_first, jnp.where(kind_code == 1, prev_last[:, ::-1], jnp.where(kind_code == 2, wall_rows, jnp.zeros_like(wall_rows))))
    return rotate_plane(picked, rot_code)


def flux_of(padded, coupling, direction):
    mixed = jnp.einsum('uv,vijk->uijk', coupling[direction], padded, precision=PRECISE)
    return mixed + 0.5 * padded[1 + direction][None] * padded


def divergence(padded, coupling, direction):
    axis_pos = direction + 1
    length = padded.shape[axis_pos] - 4
    fluxes = flux_of(padded, coupling, direction)
    face_count = length + 1

    def cut_axis(array, offset, amount):
        return lax.slice_in_dim(array, offset, offset + amount, axis=axis_pos)

    near_left = cut_axis(padded, 1, face_count)
    near_right = cut_axis(padded, 2, face_count)
    far_left = cut_axis(padded, 0, face_count)
    far_right = cut_axis(padded, 3, face_count)
    face_flux = 0.5 * (cut_axis(fluxes, 1, face_count) + cut_axis(fluxes, 2, face_count)) - DAMP_TWO * (near_right - near_left) + DAMP_FOUR * (far_right - 3.0 * near_right + 3.0 * near_left - far_left)
    return cut_axis(face_flux, 1, length) - cut_axis(face_flux, 0, length)


def cell_residual(along_i, along_k, block_cells, coupling):
    low_j = mirrored(block_cells[:, :, :2][:, :, ::-1], 2)
    high_j = mirrored(block_cells[:, :, -2:][:, :, ::-1], 2)
    along_j = jnp.concatenate([low_j, block_cells, high_j], axis=2)
    return divergence(along_i, coupling, 0) + divergence(along_j, coupling, 1) + divergence(along_k, coupling, 2)


def residual_whole(field_now, coupling, face_type, face_rot):
    blocks_count = face_type.shape[0]
    block_rows = field_now.shape[1] // blocks_count

    def per_block(number):
        row_start = (number * block_rows).astype(jnp.int32)
        block_cells = lax.dynamic_slice_in_dim(field_now, row_start, block_rows, axis=1)
        prev_start = (((number + blocks_count - 1) % blocks_count) * block_rows + block_rows - 2).astype(jnp.int32)
        next_start = (((number + 1) % blocks_count) * block_rows).astype(jnp.int32)
        prev_last = lax.dynamic_slice_in_dim(field_now, prev_start, 2, axis=1)
        next_first = lax.dynamic_slice_in_dim(field_now, next_start, 2, axis=1)
        low_ghost = lower_ghosts(block_cells, prev_last, next_first, face_type[number, 0], face_rot[number, 0])
        high_ghost = upper_ghosts(block_cells, prev_last, next_first, face_type[number, 1], face_rot[number, 1])
        along_i = jnp.concatenate([low_ghost, block_cells, high_ghost], axis=1)
        along_k = jnp.pad(block_cells, ((0, 0), (0, 0), (0, 0), (2, 2)))
        return cell_residual(along_i, along_k, block_cells, coupling)

    stacked = lax.map(per_block, jnp.arange(blocks_count, dtype=jnp.int32))
    shape_of = stacked.shape
    return jnp.transpose(stacked, (1, 0, 2, 3, 4)).reshape(shape_of[1], shape_of[0] * shape_of[2], shape_of[3], shape_of[4])


def restrict(array):
    shape_of = array.shape
    leading = shape_of[:-3]
    reshaped = array.reshape(leading + (shape_of[-3] // 2, 2, shape_of[-2] // 2, 2, shape_of[-1] // 2, 2))
    return reshaped.mean(axis=(-5, -3, -1))


def prolong(array):
    return jnp.repeat(jnp.repeat(jnp.repeat(array, 2, axis=-3), 2, axis=-2), 2, axis=-1)


def reference(flow_state, timestep, coupling, face_type, face_rot):
    fine_state = flow_state
    for section_alpha in SECTION_COEFFS:
        fine_state = flow_state - section_alpha * timestep[None] * residual_whole(fine_state, coupling, face_type, face_rot)
    fine_residual = residual_whole(fine_state, coupling, face_type, face_rot)
    coarse_start = restrict(fine_state)
    coarse_step = restrict(timestep)
    forcing = residual_whole(coarse_start, coupling, face_type, face_rot) - restrict(fine_residual)
    coarse = coarse_start
    for section_alpha in SECTION_COEFFS:
        coarse = coarse_start - section_alpha * coarse_step[None] * (residual_whole(coarse, coupling, face_type, face_rot) - forcing)
    updated = fine_state + prolong(coarse - coarse_start)
    return updated, fine_residual
```

```python
import functools

import jax
import jax.numpy as jnp
from jax import lax
from jax.experimental import pallas as pl
from jax.experimental.pallas import tpu as pltpu
from jax.sharding import PartitionSpec as P

NV = 6
NI = 8
HALO = 10
PER = 12
VMEM_LIMIT = 12 * 1024 * 1024

C0, C1, C2 = 0.44, -0.26, 0.04


def iota_j():
    return lax.broadcasted_iota(jnp.int32, (8, 128), 0)


def iota_k():
    return lax.broadcasted_iota(jnp.int32, (8, 128), 1)


def rotl(x, shift):
    return pltpu.roll(x, shift % 128, 1)


def rots(x, shift):
    return pltpu.roll(x, shift % 8, 0)


def reverse_j(x):
    j = iota_j()
    x = rots(x, 4)
    x = jnp.where((j // 2) % 2 == 0, rots(x, -2), rots(x, 2))
    return jnp.where(j % 2 == 0, rots(x, -1), rots(x, 1))


def ghost_rows(own2, prev2, next2, kind, rot):
    nearest = []
    for r in range(2):
        picked = []
        for v in range(NV):
            wall = -own2[r][v] if v == 1 else own2[r][v]
            x = jnp.where(kind == 2, wall, 0.0)
            x = jnp.where(kind == 1, next2[r][v], x)
            x = jnp.where(kind == 0, prev2[r][v], x)
            picked.append(jnp.where(rot % 2 == 1, reverse_j(x), x))
        turn = rot // 2 % 2 == 1
        a, b = picked[2], picked[3]
        picked[2], picked[3] = jnp.where(turn, -b, a), jnp.where(turn, a, b)
        nearest.append(picked)
    return nearest


def with_ghosts(rows, below, above, meta):
    t_lo, t_hi, r_lo, r_hi = meta
    lo = ghost_rows([rows[0], rows[1]], [below[1], below[0]], [above[0], above[1]], t_lo, r_lo)
    hi = ghost_rows([rows[-1], rows[-2]], [above[0], above[1]], [below[1], below[0]], t_hi, r_hi)
    return [lo[1], lo[0]] + rows + [hi[0], hi[1]]


def flux(q, a, d):
    half = 0.5 * q[1 + d]
    out = []
    for u in range(NV):
        acc = (a[d][u][u] + half) * q[u]
        for v in range(NV):
            if v != u:
                acc = acc + a[d][u][v] * q[v]
        out.append(acc)
    return out


def flux_j(q, a):
    out, mirrored = [], []
    for u in range(NV):
        even = None
        for v in range(NV):
            if v != 2:
                term = a[1][u][v] * q[v]
                even = term if even is None else even + term
        if u == 2:
            even = even + 0.5 * (q[2] * q[2])
            odd = a[1][2][2] * q[2]
        else:
            odd = q[2] * (a[1][u][2] + 0.5 * q[u])
        out.append(even + odd)
        mirrored.append(even - odd)
    return out, mirrored


def j_weights(unit):
    j = iota_j() // unit
    n = 8 // unit
    out = []
    for sign in (1.0, -1.0):
        end = (j == 0) | (j == n - 1)
        centre = jnp.where(end, C0 + sign * C1, C0) + 2 * C0
        near = C1 + sign * C2
        below = jnp.where(j == 0, 0.0, jnp.where((j == 1) | (j == n - 1), near, C1))
        above = jnp.where(j == n - 1, 0.0, jnp.where((j == 0) | (j == n - 2), near, C1))
        if n == 4:
            two = None
        else:
            two = (jnp.where(j >= 2, C2, 0.0), jnp.where(j <= n - 3, C2, 0.0))
        out.append((centre, below, above, two))
    return out


def residual2(padded, side, a, unit):
    n = len(padded) - 4
    k = iota_k()
    j = iota_j()
    weights = j_weights(unit)
    first_j, last_j = j < unit, j >= 8 - unit
    low1, low2 = k < unit, k < 2 * unit
    high1, high2 = k >= 128 - unit, k >= 128 - 2 * unit
    fi = {m: flux(padded[m], a, 0) for m in range(1, n + 3)}
    result = []
    for i in range(n):
        m = i + 2
        q = padded[m]
        fj, gj = flux_j(q, a)
        fk = flux(q, a, 2)
        fs = flux(side[i], a, 2)
        row = []
        for u in range(NV):
            x = q[u]
            s = side[i][u]
            centre, below, above, two = weights[1 if u == 2 else 0]
            acc = fi[m + 1][u] - fi[m - 1][u]
            acc = acc + C1 * (padded[m + 1][u] + padded[m - 1][u]) + C2 * (padded[m + 2][u] + padded[m - 2][u])
            acc = acc + centre * x
            acc = acc + below * rots(x, unit) + above * rots(x, -unit)
            if two is None:
                acc = acc + C2 * rots(x, 4)
            else:
                acc = acc + two[0] * rots(x, 2) + two[1] * rots(x, -2)
            up = jnp.where(last_j, gj[u], rots(fj[u], -unit))
            down = jnp.where(first_j, gj[u], rots(fj[u], unit))
            acc = acc + (up - down)
            tx, ts = C1 * x, C1 * s
            acc = acc + rotl(jnp.where(low1, fs[u] + ts, fk[u] + tx), -unit)
            acc = acc - rotl(jnp.where(high1, fs[u] - ts, fk[u] - tx), unit)
            acc = acc + C2 * (rotl(jnp.where(low2, s, x), -2 * unit) + rotl(jnp.where(high2, s, x), 2 * unit))
            row.append(acc)
        result.append(row)
    return result


def pair_mean(a, b):
    x = a + b
    x = x + jnp.where(iota_j() % 2 == 0, rots(x, -1), rots(x, 1))
    x = x + jnp.where(iota_k() % 2 == 0, rotl(x, -1), rotl(x, 1))
    return 0.125 * x


def restrict_rows(rows):
    return [[pair_mean(rows[2 * c][v], rows[2 * c + 1][v]) for v in range(len(rows[0]))] for c in range(len(rows) // 2)]


def load(ref, first, count):
    return [[ref[v, first + r] for v in range(NV)] for r in range(count)]


def store(ref, first, rows):
    for r, row in enumerate(rows):
        for v in range(NV):
            ref[v, first + r] = row[v]


def coefficients(a_ref):
    return [[[a_ref[d, u, v] for v in range(NV)] for u in range(NV)] for d in range(3)]


def meta_of(type_ref, rot_ref):
    return (type_ref[0, 0], type_ref[0, 1], rot_ref[0, 0], rot_ref[0, 1])


def halo_mask():
    k = iota_k()
    s = lax.axis_index("sub")
    last = lax.axis_size("sub") - 1
    return ((k < HALO) & (s != last)) | ((k >= 128 - HALO) & (s != 0))


def neighbours(ga, gb, first):
    even = lax.axis_index("blk") % 2 == 0
    a, b = load(ga, first, 2), load(gb, first, 2)
    below = [[jnp.where(even, b[r][v], a[r][v]) for v in range(NV)] for r in range(2)]
    above = [[jnp.where(even, a[r][v], b[r][v]) for v in range(NV)] for r in range(2)]
    return below, above


def send(ma, mb, first, rows):
    even = lax.axis_index("blk") % 2 == 0
    for r in range(2):
        for v in range(NV):
            lo, hi = rows[r][v], rows[len(rows) - 2 + r][v]
            ma[v, first + r] = jnp.where(even, hi, lo)
            mb[v, first + r] = jnp.where(even, lo, hi)


def pack_kernel(q_ref, dt_ref, ma, mb, to_left, to_right):
    k = iota_k()
    send(ma, mb, 0, load(q_ref, 0, NI))
    tiles = [q_ref[v, i] for v in range(NV) for i in range(NI)] + [dt_ref[i] for i in range(NI)]
    for g in range(-(-len(tiles) // PER)):
        left = right = jnp.zeros((8, 128), jnp.float32)
        for n, x in enumerate(tiles[g * PER : (g + 1) * PER]):
            at = n * HALO
            inside = (k >= at) & (k < at + HALO)
            left = jnp.where(inside, rotl(x, at), left)
            right = jnp.where(inside, rotl(x, at + HALO), right)
        to_left[g] = left
        to_right[g] = right


def unpack(from_right, from_left):
    k = iota_k()
    tiles = []
    for n in range(NV * NI + NI):
        g, at = n // PER, n % PER * HALO
        low = rotl(from_right[g], -at)
        high = rotl(from_left[g], -at - HALO)
        tiles.append(jnp.where(k < HALO, low, jnp.where(k >= 128 - HALO, high, 0.0)))
    return [[tiles[v * NI + i] for v in range(NV)] for i in range(NI)], tiles[NV * NI :]


def advance(start, dt, twice, factor):
    return [[start[i][v] - (0.5 * factor * dt[i]) * twice[i][v] for v in range(NV)] for i in range(len(start))]


def masked(rows):
    inside = halo_mask()
    return [[jnp.where(inside, x, 0.0) for x in row] for row in rows]


def first_kernel(a_ref, type_ref, rot_ref, q_ref, dt_ref, ga, gb, from_right, from_left, t1_ref, h0_ref, dth_ref, ma, mb):
    a, meta = coefficients(a_ref), meta_of(type_ref, rot_ref)
    h0, dth = unpack(from_right, from_left)
    store(h0_ref, 0, h0)
    for i in range(NI):
        dth_ref[i] = dth[i]
    send(ma, mb, 2, h0)
    t0 = load(q_ref, 0, NI)
    below, above = neighbours(ga, gb, 0)
    twice = residual2(with_ghosts(t0, below, above, meta), h0, a, 1)
    t1 = advance(t0, [dt_ref[i] for i in range(NI)], twice, 0.4)
    store(t1_ref, 0, t1)
    send(ma, mb, 0, t1)


def second_kernel(a_ref, type_ref, rot_ref, q_ref, t1_ref, h0_ref, dt_ref, dth_ref, ga, gb, t2_ref, h1_ref, ma, mb):
    a, meta = coefficients(a_ref), meta_of(type_ref, rot_ref)
    t0, h0 = load(q_ref, 0, NI), load(h0_ref, 0, NI)
    below, above = neighbours(ga, gb, 2)
    twice = residual2(with_ghosts(h0, below, above, meta), t0, a, 1)
    h1 = masked(advance(h0, [dth_ref[i] for i in range(NI)], twice, 0.4))
    store(h1_ref, 0, h1)
    send(ma, mb, 2, h1)
    t1 = load(t1_ref, 0, NI)
    below, above = neighbours(ga, gb, 0)
    twice = residual2(with_ghosts(t1, below, above, meta), h1, a, 1)
    t2 = advance(t0, [dt_ref[i] for i in range(NI)], twice, 1.0)
    store(t2_ref, 0, t2)
    send(ma, mb, 0, t2)


def third_kernel(
    a_ref, type_ref, rot_ref, t1_ref, t2_ref, h0_ref, h1_ref, dt_ref, dth_ref, ga, gb, res_ref, h2_ref, c1_ref, ma, mb
):
    a, meta = coefficients(a_ref), meta_of(type_ref, rot_ref)
    h0, h1, t1 = load(h0_ref, 0, NI), load(h1_ref, 0, NI), load(t1_ref, 0, NI)
    below, above = neighbours(ga, gb, 2)
    twice = residual2(with_ghosts(h1, below, above, meta), t1, a, 1)
    h2 = masked(advance(h0, [dth_ref[i] for i in range(NI)], twice, 1.0))
    store(h2_ref, 0, h2)
    send(ma, mb, 4, h2)
    t2 = load(t2_ref, 0, NI)
    below, above = neighbours(ga, gb, 0)
    twice = residual2(with_ghosts(t2, below, above, meta), h2, a, 1)
    res = [[0.5 * x for x in row] for row in twice]
    store(res_ref, 0, res)
    start = restrict_rows(t2)
    mean = restrict_rows(res)
    step = [pair_mean(dt_ref[2 * c], dt_ref[2 * c + 1]) for c in range(NI // 2)]
    c1 = [[start[c][v] - (0.4 * step[c]) * mean[c][v] for v in range(NV)] for c in range(NI // 2)]
    store(c1_ref, 0, c1)
    send(ma, mb, 0, c1)
    send(ma, mb, 2, start)


def fourth_kernel(a_ref, type_ref, rot_ref, t2_ref, h2_ref, res_ref, c1_ref, dt_ref, dth_ref, ga, gb, out_ref):
    a, meta = coefficients(a_ref), meta_of(type_ref, rot_ref)
    half = NI // 2
    h2, t2 = load(h2_ref, 0, NI), load(t2_ref, 0, NI)
    below, above = neighbours(ga, gb, 4)
    twice = residual2(with_ghosts(h2, below, above, meta), t2, a, 1)
    mean = restrict_rows(twice)
    start_h = restrict_rows(h2)
    step_h = [pair_mean(dth_ref[2 * c], dth_ref[2 * c + 1]) for c in range(half)]
    c1_h = masked([[start_h[c][v] - (0.2 * step_h[c]) * mean[c][v] for v in range(NV)] for c in range(half)])
    start = restrict_rows(t2)
    below, above = neighbours(ga, gb, 2)
    twice_start = residual2(with_ghosts(start, below, above, meta), start_h, a, 2)
    c1 = load(c1_ref, 0, half)
    below, above = neighbours(ga, gb, 0)
    twice_c1 = residual2(with_ghosts(c1, below, above, meta), c1_h, a, 2)
    for c in range(half):
        step = pair_mean(dt_ref[2 * c], dt_ref[2 * c + 1])
        for v in range(NV):
            mean_res = pair_mean(res_ref[v, 2 * c], res_ref[v, 2 * c + 1])
            change = -step * (0.5 * (twice_c1[c][v] - twice_start[c][v]) + mean_res)
            out_ref[v, 2 * c] = t2[2 * c][v] + change
            out_ref[v, 2 * c + 1] = t2[2 * c + 1][v] + change


def field(rows):
    return (NV, rows, 8, 128)


def call(kernel, scalars, arrays, outs):
    smem, vmem = pl.BlockSpec(memory_space=pltpu.SMEM), pl.BlockSpec(memory_space=pltpu.VMEM)
    return pl.pallas_call(
        kernel,
        out_shape=[jax.ShapeDtypeStruct(shape, jnp.float32) for shape in outs],
        in_specs=[smem] * len(scalars) + [vmem] * len(arrays),
        out_specs=[vmem] * len(outs),
        compiler_params=pltpu.CompilerParams(vmem_limit_bytes=VMEM_LIMIT),
    )(*scalars, *arrays)


def body(flow_state, timestep, coupling, face_type, face_rot):
    blocks, parts = lax.axis_size("blk"), lax.axis_size("sub")
    chip = [(b, b ^ 1) for b in range(blocks)]
    link = [(b, (b + 1) % blocks if b % 2 else (b - 1) % blocks) for b in range(blocks)]
    ahead = [(s, s + 1) for s in range(parts - 1)]
    back = [(s + 1, s) for s in range(parts - 1)]
    groups = -(-(NV * NI + NI) // PER)
    scalars = (coupling, face_type, face_rot)

    ma, mb, to_left, to_right = call(
        pack_kernel, (), (flow_state, timestep), (field(2), field(2), (groups, 8, 128), (groups, 8, 128))
    )
    ga, gb = lax.ppermute(ma, "blk", chip), lax.ppermute(mb, "blk", link)
    from_right, from_left = lax.ppermute(to_left, "sub", back), lax.ppermute(to_right, "sub", ahead)

    t1, h0, dth, ma, mb = call(
        first_kernel,
        scalars,
        (flow_state, timestep, ga, gb, from_right, from_left),
        (field(NI), field(NI), (NI, 8, 128), field(4), field(4)),
    )
    ga, gb = lax.ppermute(ma, "blk", chip), lax.ppermute(mb, "blk", link)

    t2, h1, ma, mb = call(
        second_kernel,
        scalars,
        (flow_state, t1, h0, timestep, dth, ga, gb),
        (field(NI), field(NI), field(4), field(4)),
    )
    ga, gb = lax.ppermute(ma, "blk", chip), lax.ppermute(mb, "blk", link)

    res, h2, c1, ma, mb = call(
        third_kernel,
        scalars,
        (t1, t2, h0, h1, timestep, dth, ga, gb),
        (field(NI), field(NI), field(NI // 2), field(6), field(6)),
    )
    ga, gb = lax.ppermute(ma, "blk", chip), lax.ppermute(mb, "blk", link)

    (updated,) = call(
        fourth_kernel, scalars, (t2, h2, res, c1, timestep, dth, ga, gb), (field(NI),)
    )
    return (updated, res)


def solution(mesh):
    return jax.shard_map(
        body,
        mesh=mesh,
        in_specs=(
            P(None, "blk", None, "sub"),
            P("blk", None, "sub"),
            P(),
            P("blk", None),
            P("blk", None),
        ),
        out_specs=(P(None, "blk", None, "sub"), P(None, "blk", None, "sub")),
        check_vma=False,
    )
```

```python
import jax
import jax.numpy as jnp
from jax import lax
from jax.experimental import pallas as pl
from jax.experimental.pallas import tpu as pltpu
from jax.sharding import PartitionSpec as P


NV = 6
NI = 8
HALO = 10
SEG = 32
VMEM_LIMIT = 12 * 1024 * 1024

C0, C1, C2 = 0.44, -0.26, 0.04


def iota_j():
    return lax.broadcasted_iota(jnp.int32, (8, 128), 0)


def iota_k():
    return lax.broadcasted_iota(jnp.int32, (8, 128), 1)


def rotl(x, shift):
    return pltpu.roll(x, shift % 128, 1)


def rots(x, shift):
    return pltpu.roll(x, shift % 8, 0)


def reverse_j(x):
    j = iota_j()
    x = rots(x, 4)
    x = jnp.where((j // 2) % 2 == 0, rots(x, -2), rots(x, 2))
    return jnp.where(j % 2 == 0, rots(x, -1), rots(x, 1))


def ghost_rows(own2, prev2, next2, kind, rot):
    nearest = []
    for r in range(2):
        picked = []
        for v in range(NV):
            wall = -own2[r][v] if v == 1 else own2[r][v]
            x = jnp.where(kind == 2, wall, 0.0)
            x = jnp.where(kind == 1, next2[r][v], x)
            x = jnp.where(kind == 0, prev2[r][v], x)
            picked.append(jnp.where(rot % 2 == 1, reverse_j(x), x))
        turn = rot // 2 % 2 == 1
        a, b = picked[2], picked[3]
        picked[2], picked[3] = jnp.where(turn, -b, a), jnp.where(turn, a, b)
        nearest.append(picked)
    return nearest


def with_ghosts(rows, below, above, meta):
    t_lo, t_hi, r_lo, r_hi = meta
    lo = ghost_rows([rows[0], rows[1]], [below[1], below[0]], [above[0], above[1]], t_lo, r_lo)
    hi = ghost_rows([rows[-1], rows[-2]], [above[0], above[1]], [below[1], below[0]], t_hi, r_hi)
    return [lo[1], lo[0]] + rows + [hi[0], hi[1]]


def flux(q, a, d):
    half = 0.5 * q[1 + d]
    out = []
    for u in range(NV):
        acc = (a[d][u][u] + half) * q[u]
        for v in range(NV):
            if v != u:
                acc = acc + a[d][u][v] * q[v]
        out.append(acc)
    return out


def flux_j(q, a):
    out, mirrored = [], []
    for u in range(NV):
        even = None
        for v in range(NV):
            if v != 2:
                term = a[1][u][v] * q[v]
                even = term if even is None else even + term
        if u == 2:
            even = even + 0.5 * (q[2] * q[2])
            odd = a[1][2][2] * q[2]
        else:
            odd = q[2] * (a[1][u][2] + 0.5 * q[u])
        out.append(even + odd)
        mirrored.append(even - odd)
    return out, mirrored


def j_weights(unit):
    j = iota_j() // unit
    n = 8 // unit
    out = []
    for sign in (1.0, -1.0):
        end = (j == 0) | (j == n - 1)
        centre = jnp.where(end, C0 + sign * C1, C0) + 2 * C0
        near = C1 + sign * C2
        below = jnp.where(j == 0, 0.0, jnp.where((j == 1) | (j == n - 1), near, C1))
        above = jnp.where(j == n - 1, 0.0, jnp.where((j == 0) | (j == n - 2), near, C1))
        if n == 4:
            two = None
        else:
            two = (jnp.where(j >= 2, C2, 0.0), jnp.where(j <= n - 3, C2, 0.0))
        out.append((centre, below, above, two))
    return out


def seg():
    return iota_k() // SEG


def place():
    return iota_k() % SEG


def second_index(fj, gj, q, u, unit, weights, ends):
    centre, below, above, two = weights[1 if u == 2 else 0]
    x = q[u]
    acc = centre * x + below * rots(x, unit) + above * rots(x, -unit)
    if two is None:
        acc = acc + C2 * rots(x, 4)
    else:
        acc = acc + two[0] * rots(x, 2) + two[1] * rots(x, -2)
    up = jnp.where(ends[1], gj[u], rots(fj[u], -unit))
    down = jnp.where(ends[0], gj[u], rots(fj[u], unit))
    return acc + (up - down)


def residual2(padded, halo, a, unit):
    n = len(padded) - 4
    k, j = iota_k(), iota_j()
    weights = j_weights(unit)
    ends = (j < unit, j >= 8 - unit)
    low1, low2 = k < unit, k < 2 * unit
    high1, high2 = k >= 128 - unit, k >= 128 - 2 * unit
    upper = place() >= HALO
    edge = []
    for tile in halo:
        f = flux(tile, a, 2)
        edge.append([jnp.where(upper, f[u] + C1 * tile[u], f[u] - C1 * tile[u]) for u in range(NV)])
    fi = {m: flux(padded[m], a, 0) for m in range(1, n + 3)}
    result = []
    for i in range(n):
        m = i + 2
        q = padded[m]
        fj, gj = flux_j(q, a)
        fk = flux(q, a, 2)
        g, first = unit * i // 4, unit * i % 4 * SEG + HALO
        row = []
        for u in range(NV):
            x = q[u]
            s, e = rotl(halo[g][u], -first), rotl(edge[g][u], -first)
            acc = second_index(fj, gj, q, u, unit, weights, ends)
            acc = acc + (fi[m + 1][u] - fi[m - 1][u])
            acc = acc + C1 * (padded[m + 1][u] + padded[m - 1][u]) + C2 * (padded[m + 2][u] + padded[m - 2][u])
            t = C1 * x
            acc = acc + rotl(jnp.where(low1, e, fk[u] + t), -unit)
            acc = acc - rotl(jnp.where(high1, e, fk[u] - t), unit)
            acc = acc + C2 * (rotl(jnp.where(low2, s, x), -2 * unit) + rotl(jnp.where(high2, s, x), 2 * unit))
            row.append(acc)
        result.append(row)
    return result


def halo_residual2(halo, ghost, own, a):
    r, o = seg(), place()
    j = iota_j()
    weights = j_weights(1)
    ends = (j < 1, j >= 7)
    first, last, low, high = r == 0, r == 3, r < 2, r >= 2
    tiles = [halo[0], halo[1], ghost]
    up_i, down_i = [], []
    for t in tiles:
        f = flux(t, a, 0)
        up_i.append([f[u] + C1 * t[u] for u in range(NV)])
        down_i.append([f[u] - C1 * t[u] for u in range(NV)])
    upper = o >= HALO
    after1, after2 = o == HALO, (o == HALO) | (o == HALO + 1)
    before1, before2 = o == HALO - 1, (o == HALO - 1) | (o == HALO - 2)
    result = []
    for g in range(2):
        q, nxt, prv = tiles[g], (g + 1) % 3, (g + 2) % 3
        fj, gj = flux_j(q, a)
        fk = flux(q, a, 2)
        fo = flux(own[g], a, 2)
        row = []
        for u in range(NV):
            x, y = q[u], own[g][u]
            acc = second_index(fj, gj, q, u, 1, weights, ends)
            acc = acc + rotl(jnp.where(first, up_i[nxt][u], up_i[g][u]), -SEG)
            acc = acc - rotl(jnp.where(last, down_i[prv][u], down_i[g][u]), SEG)
            acc = acc + C2 * rotl(jnp.where(low, tiles[nxt][u], x) + jnp.where(high, tiles[prv][u], x), 2 * SEG)
            t = C1 * x
            e = jnp.where(upper, fo[u] + C1 * y, fo[u] - C1 * y)
            acc = acc + rotl(jnp.where(after1, e, fk[u] + t), -1)
            acc = acc - rotl(jnp.where(before1, e, fk[u] - t), 1)
            acc = acc + C2 * (rotl(jnp.where(after2, y, x), -2) + rotl(jnp.where(before2, y, x), 2))
            row.append(acc)
        result.append(row)
    return result


def pack_ends(rows):
    r = seg()
    out = []
    for g in range(2):
        tile = []
        for v in range(NV):
            acc = rotl(rows[4 * g][v], HALO)
            for p in range(1, 4):
                acc = jnp.where(r == p, rotl(rows[4 * g + p][v], HALO + p * SEG), acc)
            tile.append(acc)
        out.append(tile)
    return out


def halo_ghost(halo, below, above, meta):
    t_lo, t_hi, r_lo, r_hi = meta
    r = seg()
    high_side = r < 2
    even_part = r % 2 == 0

    def turned(x):
        return jnp.where(even_part, rotl(x, SEG), rotl(x, -SEG))

    picked = []
    for v in range(NV):
        wall_lo, wall_hi = turned(halo[0][v]), turned(halo[1][v])
        if v == 1:
            wall_lo, wall_hi = -wall_lo, -wall_hi
        hi = jnp.where(t_hi == 2, wall_hi, 0.0)
        hi = jnp.where(t_hi == 1, turned(below[v]), hi)
        hi = jnp.where(t_hi == 0, above[v], hi)
        lo = jnp.where(t_lo == 2, wall_lo, 0.0)
        lo = jnp.where(t_lo == 1, turned(above[v]), lo)
        lo = jnp.where(t_lo == 0, below[v], lo)
        x = jnp.where(high_side, hi, lo)
        code = jnp.where(high_side, r_hi, r_lo)
        picked.append(jnp.where(code % 2 == 1, reverse_j(x), x))
    turn = jnp.where(high_side, r_hi, r_lo) // 2 % 2 == 1
    b, c = picked[2], picked[3]
    picked[2], picked[3] = jnp.where(turn, -c, b), jnp.where(turn, b, c)
    return picked


def cell_mean(x):
    x = x + jnp.where(iota_j() % 2 == 0, rots(x, -1), rots(x, 1))
    x = x + jnp.where(iota_k() % 2 == 0, rotl(x, -1), rotl(x, 1))
    return 0.125 * x


def restrict_rows(rows):
    return [[cell_mean(rows[2 * c][v] + rows[2 * c + 1][v]) for v in range(len(rows[0]))] for c in range(len(rows) // 2)]


def halo_mean(x):
    return cell_mean(x + jnp.where(seg() % 2 == 0, rotl(x, -SEG), rotl(x, SEG)))


def load(ref, first, count):
    return [[ref[v, first + r] for v in range(NV)] for r in range(count)]


def store(ref, first, rows):
    for r, row in enumerate(rows):
        for v in range(NV):
            ref[v, first + r] = row[v]


def load_tiles(ref):
    return [[ref[g, v] for v in range(NV)] for g in range(2)]


def store_tiles(ref, tiles):
    for g in range(2):
        for v in range(NV):
            ref[g, v] = tiles[g][v]


def coefficients(a_ref):
    return [[[a_ref[d, u, v] for v in range(NV)] for u in range(NV)] for d in range(3)]


def meta_of(type_ref, rot_ref):
    return (type_ref[0, 0], type_ref[0, 1], rot_ref[0, 0], rot_ref[0, 1])


def masked(tiles):
    o = place()
    s = lax.axis_index("sub")
    final = lax.axis_size("sub") - 1
    inside = ((o < HALO) & (s != 0)) | ((o >= HALO) & (o < 2 * HALO) & (s != final))
    return [[jnp.where(inside, x, 0.0) for x in tile] for tile in tiles]


def is_even():
    return lax.axis_index("blk") % 2 == 0


def send(ma, mb, at, first, last):
    even = is_even()
    for n, (lo, hi) in enumerate(zip(first, last)):
        ma[at + n] = jnp.where(even, hi, lo)
        mb[at + n] = jnp.where(even, lo, hi)


def receive(ga, gb, at, count):
    even = is_even()
    below, above = [], []
    for n in range(at, at + count):
        a, b = ga[n], gb[n]
        below.append(jnp.where(even, b, a))
        above.append(jnp.where(even, a, b))
    return below, above


def send_rows(ma, mb, at, rows):
    send(ma, mb, at, rows[0] + rows[1], rows[-2] + rows[-1])


def receive_rows(ga, gb, at):
    below, above = receive(ga, gb, at, 2 * NV)
    return [below[:NV], below[NV:]], [above[:NV], above[NV:]]


def send_halo(ma, mb, at, halo):
    low = seg() < 2
    first = [jnp.where(low, halo[0][p], rotl(halo[0][p + 1], 64)) for p in range(0, NV, 2)]
    last = [jnp.where(low, rotl(halo[1][p + 1], 64), halo[1][p]) for p in range(0, NV, 2)]
    send(ma, mb, at, first, last)


def receive_halo(ga, gb, at):
    below, above = receive(ga, gb, at, NV // 2)

    def spread(tiles):
        return [y for x in tiles for y in (x, rotl(x, 64))]

    return spread(below), spread(above)


def send_coarse(ma, mb, at, first, second):
    j_even, k_even = iota_j() % 2 == 0, iota_k() % 2 == 0

    def joined(r0, r1):
        out = []
        for v in range(NV):
            x, y = (jnp.where(j_even, first[r][v], second[r][v]) for r in (r0, r1))
            out.append(jnp.where(k_even, x, y))
        return out

    send(ma, mb, at, joined(0, 1), joined(-2, -1))


def receive_coarse(ga, gb, at):
    j_even, k_even = iota_j() % 2 == 0, iota_k() % 2 == 0
    fields = ([], [])
    for tiles in receive(ga, gb, at, NV):
        rows = ([], [])
        for x in tiles:
            rows[0].append(jnp.where(k_even, x, rotl(x, 1)))
            rows[1].append(jnp.where(k_even, rotl(x, -1), x))
        fields[0].append([[jnp.where(j_even, x, rots(x, 1)) for x in row] for row in rows])
        fields[1].append([[jnp.where(j_even, rots(x, -1), x) for x in row] for row in rows])
    return fields


def pack_kernel(q_hbm, dt_hbm, ends_ref, ma, mb, to_left, to_right, q_ref, dt_ref, sems):
    copies = (
        pltpu.make_async_copy(q_hbm, q_ref, sems.at[0]),
        pltpu.make_async_copy(dt_hbm, dt_ref, sems.at[1]),
    )
    for copy in copies:
        copy.start()
    for copy in copies:
        copy.wait()
    rows = load(q_ref, 0, NI)
    send_rows(ma, mb, 0, rows)
    ends = pack_ends(rows)
    store_tiles(ends_ref, ends)
    r, lower = seg(), place() < HALO
    tiles = ends[0] + ends[1]
    for g in range(2):
        acc = rotl(dt_ref[4 * g], HALO)
        for p in range(1, 4):
            acc = jnp.where(r == p, rotl(dt_ref[4 * g + p], HALO + p * SEG), acc)
        tiles.append(acc)
    for n in range(NV + 1):
        x, y = tiles[2 * n], tiles[2 * n + 1]
        to_right[n] = jnp.where(lower, x, rotl(y, HALO))
        to_left[n] = jnp.where(lower, rotl(y, -HALO), x)


def unpack(from_right, from_left):
    lower = place() < HALO
    tiles = []
    for n in range(NV + 1):
        x, y = from_left[n], from_right[n]
        tiles.append(jnp.where(lower, x, y))
        tiles.append(jnp.where(lower, rotl(x, -HALO), rotl(y, HALO)))
    halo = masked([tiles[:NV], tiles[NV : 2 * NV]])
    return halo, tiles[2 * NV :]


def advance(start, dt, twice, factor):
    return [[start[i][v] - (0.5 * factor * dt[i]) * twice[i][v] for v in range(NV)] for i in range(len(start))]


def first_kernel(a_ref, type_ref, rot_ref, q_ref, dt_ref, ga, gb, from_right, from_left, t1_ref, h0_ref, dth_ref, ma, mb):
    a, meta = coefficients(a_ref), meta_of(type_ref, rot_ref)
    h0, dth = unpack(from_right, from_left)
    store_tiles(h0_ref, h0)
    for g in range(2):
        dth_ref[g] = dth[g]
    send_halo(ma, mb, 2 * NV, h0)
    t0 = load(q_ref, 0, NI)
    below, above = receive_rows(ga, gb, 0)
    twice = residual2(with_ghosts(t0, below, above, meta), h0, a, 1)
    t1 = advance(t0, [dt_ref[i] for i in range(NI)], twice, 0.4)
    store(t1_ref, 0, t1)
    send_rows(ma, mb, 0, t1)


def second_kernel(
    a_ref, type_ref, rot_ref, q_ref, t1_ref, h0_ref, ends_ref, dt_ref, dth_ref, ga, gb, t2_ref, h1_ref, ma, mb
):
    a, meta = coefficients(a_ref), meta_of(type_ref, rot_ref)
    h0 = load_tiles(h0_ref)
    below, above = receive_halo(ga, gb, 2 * NV)
    twice = halo_residual2(h0, halo_ghost(h0, below, above, meta), load_tiles(ends_ref), a)
    h1 = masked(advance(h0, [dth_ref[g] for g in range(2)], twice, 0.4))
    store_tiles(h1_ref, h1)
    send_halo(ma, mb, 2 * NV, h1)
    t0, t1 = load(q_ref, 0, NI), load(t1_ref, 0, NI)
    below, above = receive_rows(ga, gb, 0)
    twice = residual2(with_ghosts(t1, below, above, meta), h1, a, 1)
    t2 = advance(t0, [dt_ref[i] for i in range(NI)], twice, 1.0)
    store(t2_ref, 0, t2)
    send_rows(ma, mb, 0, t2)


def third_kernel(
    a_ref, type_ref, rot_ref, t1_ref, t2_ref, h0_ref, h1_ref, dt_ref, dth_ref, ga, gb, res_ref, h2_ref, c1_ref, mean_ref, ma, mb
):
    a, meta = coefficients(a_ref), meta_of(type_ref, rot_ref)
    h0, h1 = load_tiles(h0_ref), load_tiles(h1_ref)
    below, above = receive_halo(ga, gb, 2 * NV)
    twice = halo_residual2(h1, halo_ghost(h1, below, above, meta), pack_ends(load(t1_ref, 0, NI)), a)
    h2 = masked(advance(h0, [dth_ref[g] for g in range(2)], twice, 1.0))
    store_tiles(h2_ref, h2)
    send_halo(ma, mb, NV, h2)
    t2 = load(t2_ref, 0, NI)
    below, above = receive_rows(ga, gb, 0)
    twice = residual2(with_ghosts(t2, below, above, meta), h2, a, 1)
    res = [[0.5 * x for x in row] for row in twice]
    store(res_ref, 0, res)
    start, mean = restrict_rows(t2), restrict_rows(res)
    store(mean_ref, 0, mean)
    c1 = []
    for c in range(NI // 2):
        step = cell_mean(dt_ref[2 * c] + dt_ref[2 * c + 1])
        c1.append([start[c][v] - (0.4 * step) * mean[c][v] for v in range(NV)])
    store(c1_ref, 0, c1)
    send_coarse(ma, mb, 0, c1, start)


def fourth_kernel(a_ref, type_ref, rot_ref, t2_ref, h2_ref, c1_ref, mean_ref, dt_ref, dth_ref, ga, gb, out_ref):
    a, meta = coefficients(a_ref), meta_of(type_ref, rot_ref)
    half = NI // 2
    h2, t2 = load_tiles(h2_ref), load(t2_ref, 0, NI)
    below, above = receive_halo(ga, gb, NV)
    twice = halo_residual2(h2, halo_ghost(h2, below, above, meta), pack_ends(t2), a)
    start_h = [[halo_mean(x) for x in tile] for tile in h2]
    c1_h = []
    for g in range(2):
        step = halo_mean(dth_ref[g])
        c1_h.append([start_h[g][v] - (0.2 * step) * halo_mean(twice[g][v]) for v in range(NV)])
    c1_h = masked(c1_h)
    start, c1 = restrict_rows(t2), load(c1_ref, 0, half)
    (below1, above1), (below0, above0) = receive_coarse(ga, gb, 0)
    twice0 = residual2(with_ghosts(start, below0, above0, meta), start_h, a, 2)
    twice1 = residual2(with_ghosts(c1, below1, above1, meta), c1_h, a, 2)
    for c in range(half):
        step = cell_mean(dt_ref[2 * c] + dt_ref[2 * c + 1])
        for v in range(NV):
            change = -step * (0.5 * (twice1[c][v] - twice0[c][v]) + mean_ref[v, c])
            out_ref[v, 2 * c] = t2[2 * c][v] + change
            out_ref[v, 2 * c + 1] = t2[2 * c + 1][v] + change


def field(rows):
    return (NV, rows, 8, 128)


def tiles_of(*count):
    return (*count, 8, 128)


def call(kernel, scalars, arrays, outs, in_hbm=False, scratch=()):
    smem, vmem = pl.BlockSpec(memory_space=pltpu.SMEM), pl.BlockSpec(memory_space=pltpu.VMEM)
    given = pl.BlockSpec(memory_space=pltpu.HBM) if in_hbm else vmem
    return pl.pallas_call(
        kernel,
        out_shape=[jax.ShapeDtypeStruct(shape, jnp.float32) for shape in outs],
        in_specs=[smem] * len(scalars) + [given] * len(arrays),
        out_specs=[vmem] * len(outs),
        scratch_shapes=scratch,
        compiler_params=pltpu.CompilerParams(vmem_limit_bytes=VMEM_LIMIT),
    )(*scalars, *arrays)


def cycle(flow_state, timestep, coupling, face_type, face_rot):
    blocks, parts = lax.axis_size("blk"), lax.axis_size("sub")
    chip = [(b, b ^ 1) for b in range(blocks)]
    link = [(b, (b + 1) % blocks if b % 2 else (b - 1) % blocks) for b in range(blocks)]
    ahead = [(s, s + 1) for s in range(parts - 1)]
    back = [(s + 1, s) for s in range(parts - 1)]
    scalars = (coupling, face_type, face_rot)
    pair = tiles_of(2, NV)

    def exchange(ma, mb):
        gb = lax.ppermute(mb, "blk", link)
        ga = lax.ppermute(ma, "blk", chip)
        return ga, gb

    ends, ma, mb, to_left, to_right = call(
        pack_kernel,
        (),
        (flow_state, timestep),
        (pair, tiles_of(2 * NV), tiles_of(2 * NV), tiles_of(NV + 1), tiles_of(NV + 1)),
        in_hbm=True,
        scratch=(
            pltpu.VMEM(field(NI), jnp.float32),
            pltpu.VMEM(tiles_of(NI), jnp.float32),
            pltpu.SemaphoreType.DMA((2,)),
        ),
    )
    ga, gb = exchange(ma, mb)
    from_right = lax.ppermute(to_left, "sub", back)
    from_left = lax.ppermute(to_right, "sub", ahead)

    message = tiles_of(2 * NV + NV // 2)
    t1, h0, dth, ma, mb = call(
        first_kernel,
        scalars,
        (flow_state, timestep, ga, gb, from_right, from_left),
        (field(NI), pair, tiles_of(2), message, message),
    )
    ga, gb = exchange(ma, mb)

    t2, h1, ma, mb = call(
        second_kernel,
        scalars,
        (flow_state, t1, h0, ends, timestep, dth, ga, gb),
        (field(NI), pair, message, message),
    )
    ga, gb = exchange(ma, mb)

    message = tiles_of(NV + NV // 2)
    res, h2, c1, mean, ma, mb = call(
        third_kernel,
        scalars,
        (t1, t2, h0, h1, timestep, dth, ga, gb),
        (field(NI), pair, field(NI // 2), field(NI // 2), message, message),
    )
    ga, gb = exchange(ma, mb)

    (updated,) = call(
        fourth_kernel, scalars, (t2, h2, c1, mean, timestep, dth, ga, gb), (field(NI),)
    )
    return (updated, res)


def solution(mesh):
    return jax.shard_map(
        cycle,
        mesh=mesh,
        in_specs=(
            P(None, "blk", None, "sub"),
            P("blk", None, "sub"),
            P(),
            P("blk", None),
            P("blk", None),
        ),
        out_specs=(P(None, "blk", None, "sub"), P(None, "blk", None, "sub")),
        check_vma=False,
    )
```

```python
import jax
import jax.numpy as jnp
from jax import lax
from jax.experimental import pallas as pl
from jax.experimental.pallas import tpu as pltpu
from jax.sharding import PartitionSpec as P


NV = 6
NI = 8
HALO = 10
SEG = 32
VMEM_LIMIT = 12 * 1024 * 1024

C0, C1, C2 = 0.44, -0.26, 0.04


def iota_j():
    return lax.broadcasted_iota(jnp.int32, (8, 128), 0)


def iota_k():
    return lax.broadcasted_iota(jnp.int32, (8, 128), 1)


def rotl(x, shift):
    return pltpu.roll(x, shift % 128, 1)


def rots(x, shift):
    return pltpu.roll(x, shift % 8, 0)


def reverse_j(x):
    j = iota_j()
    x = rots(x, 4)
    x = jnp.where((j // 2) % 2 == 0, rots(x, -2), rots(x, 2))
    return jnp.where(j % 2 == 0, rots(x, -1), rots(x, 1))


def ghost_rows(own2, prev2, next2, kind, flip, turn):
    nearest = []
    for r in range(2):
        picked = []
        for v in range(NV):
            wall = -own2[r][v] if v == 1 else own2[r][v]
            x = jnp.where(kind == 2, wall, 0.0)
            x = jnp.where(kind == 1, next2[r][v], x)
            x = jnp.where(kind == 0, prev2[r][v], x)
            picked.append(jnp.where(flip == 1, reverse_j(x), x))
        a, b = picked[2], picked[3]
        picked[2], picked[3] = jnp.where(turn == 1, -b, a), jnp.where(turn == 1, a, b)
        nearest.append(picked)
    return nearest


def with_ghosts(rows, below, above, meta):
    lo = ghost_rows([rows[0], rows[1]], [below[1], below[0]], [above[0], above[1]], *meta[:3])
    hi = ghost_rows([rows[-1], rows[-2]], [above[0], above[1]], [below[1], below[0]], *meta[3:])
    return [lo[1], lo[0]] + rows + [hi[0], hi[1]]


def flux(q, a, d):
    half = 0.5 * q[1 + d]
    out = []
    for u in range(NV):
        acc = (a(d, u, u) + half) * q[u]
        for v in range(NV):
            if v != u:
                acc = acc + a(d, u, v) * q[v]
        out.append(acc)
    return out


def flux_j(q, a):
    out, mirrored = [], []
    for u in range(NV):
        even = None
        for v in range(NV):
            if v != 2:
                term = a(1, u, v) * q[v]
                even = term if even is None else even + term
        if u == 2:
            even = even + 0.5 * (q[2] * q[2])
            odd = a(1, 2, 2) * q[2]
        else:
            odd = q[2] * (a(1, u, 2) + 0.5 * q[u])
        out.append(even + odd)
        mirrored.append(even - odd)
    return out, mirrored


def j_weights(unit):
    j = iota_j() // unit
    n = 8 // unit
    out = []
    for sign in (1.0, -1.0):
        end = (j == 0) | (j == n - 1)
        centre = jnp.where(end, C0 + sign * C1, C0) + 2 * C0
        near = C1 + sign * C2
        below = jnp.where(j == 0, 0.0, jnp.where((j == 1) | (j == n - 1), near, C1))
        above = jnp.where(j == n - 1, 0.0, jnp.where((j == 0) | (j == n - 2), near, C1))
        if n == 4:
            two = None
        else:
            two = (jnp.where(j >= 2, C2, 0.0), jnp.where(j <= n - 3, C2, 0.0))
        out.append((centre, below, above, two))
    return out


def seg():
    return iota_k() // SEG


def place():
    return iota_k() % SEG


def second_index(fj, gj, q, u, unit, weights, ends):
    centre, below, above, two = weights[1 if u == 2 else 0]
    x = q[u]
    acc = centre * x + below * rots(x, unit) + above * rots(x, -unit)
    if two is None:
        acc = acc + C2 * rots(x, 4)
    else:
        acc = acc + two[0] * rots(x, 2) + two[1] * rots(x, -2)
    up = jnp.where(ends[1], gj[u], rots(fj[u], -unit))
    down = jnp.where(ends[0], gj[u], rots(fj[u], unit))
    return acc + (up - down)


def residual2(padded, halo, a, unit):
    n = len(padded) - 4
    k, j = iota_k(), iota_j()
    weights = j_weights(unit)
    ends = (j < unit, j >= 8 - unit)
    low1, low2 = k < unit, k < 2 * unit
    high1, high2 = k >= 128 - unit, k >= 128 - 2 * unit
    upper = place() >= HALO
    edge = []
    for tile in halo:
        f = flux(tile, a, 2)
        edge.append([jnp.where(upper, f[u] + C1 * tile[u], f[u] - C1 * tile[u]) for u in range(NV)])
    beside = []
    for i in range(n):
        g, first = unit * i // 4, unit * i % 4 * SEG + HALO
        beside.append([(rotl(halo[g][u], -first), rotl(edge[g][u], -first)) for u in range(NV)])
    fi = {m: flux(padded[m], a, 0) for m in range(1, n + 3)}
    result = []
    for i in range(n):
        m = i + 2
        q = padded[m]
        fj, gj = flux_j(q, a)
        fk = flux(q, a, 2)
        row = []
        for u in range(NV):
            x = q[u]
            s, e = beside[i][u]
            acc = second_index(fj, gj, q, u, unit, weights, ends)
            acc = acc + (fi[m + 1][u] - fi[m - 1][u])
            acc = acc + C1 * (padded[m + 1][u] + padded[m - 1][u]) + C2 * (padded[m + 2][u] + padded[m - 2][u])
            t = C1 * x
            acc = acc + rotl(jnp.where(low1, e, fk[u] + t), -unit)
            acc = acc - rotl(jnp.where(high1, e, fk[u] - t), unit)
            acc = acc + C2 * (rotl(jnp.where(low2, s, x), -2 * unit) + rotl(jnp.where(high2, s, x), 2 * unit))
            row.append(acc)
        result.append(row)
    return result


def halo_residual2(halo, ghost, own, a):
    r, o = seg(), place()
    j = iota_j()
    weights = j_weights(1)
    ends = (j < 1, j >= 7)
    first, last, low, high = r == 0, r == 3, r < 2, r >= 2
    tiles = [halo[0], halo[1], ghost]
    up_i, down_i = [], []
    for t in tiles:
        f = flux(t, a, 0)
        up_i.append([f[u] + C1 * t[u] for u in range(NV)])
        down_i.append([f[u] - C1 * t[u] for u in range(NV)])
    upper = o >= HALO
    after1, after2 = o == HALO, (o == HALO) | (o == HALO + 1)
    before1, before2 = o == HALO - 1, (o == HALO - 1) | (o == HALO - 2)
    result = []
    for g in range(2):
        q, nxt, prv = tiles[g], (g + 1) % 3, (g + 2) % 3
        fj, gj = flux_j(q, a)
        fk = flux(q, a, 2)
        fo = flux(own[g], a, 2)
        row = []
        for u in range(NV):
            x, y = q[u], own[g][u]
            acc = second_index(fj, gj, q, u, 1, weights, ends)
            acc = acc + rotl(jnp.where(first, up_i[nxt][u], up_i[g][u]), -SEG)
            acc = acc - rotl(jnp.where(last, down_i[prv][u], down_i[g][u]), SEG)
            acc = acc + C2 * rotl(jnp.where(low, tiles[nxt][u], x) + jnp.where(high, tiles[prv][u], x), 2 * SEG)
            t = C1 * x
            e = jnp.where(upper, fo[u] + C1 * y, fo[u] - C1 * y)
            acc = acc + rotl(jnp.where(after1, e, fk[u] + t), -1)
            acc = acc - rotl(jnp.where(before1, e, fk[u] - t), 1)
            acc = acc + C2 * (rotl(jnp.where(after2, y, x), -2) + rotl(jnp.where(before2, y, x), 2))
            row.append(acc)
        result.append(row)
    return result


def pack_ends(rows):
    r = seg()
    out = []
    for g in range(2):
        tile = []
        for v in range(NV):
            acc = rotl(rows[4 * g][v], HALO)
            for p in range(1, 4):
                acc = jnp.where(r == p, rotl(rows[4 * g + p][v], HALO + p * SEG), acc)
            tile.append(acc)
        out.append(tile)
    return out


def halo_ghost(halo, below, above, meta):
    t_lo, flip_lo, turn_lo, t_hi, flip_hi, turn_hi = meta
    r = seg()
    high_side = r < 2
    even_part = r % 2 == 0

    def turned(x):
        return jnp.where(even_part, rotl(x, SEG), rotl(x, -SEG))

    flip = jnp.where(high_side, flip_hi, flip_lo)
    picked = []
    for v in range(NV):
        wall_lo, wall_hi = turned(halo[0][v]), turned(halo[1][v])
        if v == 1:
            wall_lo, wall_hi = -wall_lo, -wall_hi
        hi = jnp.where(t_hi == 2, wall_hi, 0.0)
        hi = jnp.where(t_hi == 1, turned(below[v]), hi)
        hi = jnp.where(t_hi == 0, above[v], hi)
        lo = jnp.where(t_lo == 2, wall_lo, 0.0)
        lo = jnp.where(t_lo == 1, turned(above[v]), lo)
        lo = jnp.where(t_lo == 0, below[v], lo)
        x = jnp.where(high_side, hi, lo)
        picked.append(jnp.where(flip == 1, reverse_j(x), x))
    turn = jnp.where(high_side, turn_hi, turn_lo) == 1
    b, c = picked[2], picked[3]
    picked[2], picked[3] = jnp.where(turn, -c, b), jnp.where(turn, b, c)
    return picked


def cell_mean(x):
    x = x + jnp.where(iota_j() % 2 == 0, rots(x, -1), rots(x, 1))
    x = x + jnp.where(iota_k() % 2 == 0, rotl(x, -1), rotl(x, 1))
    return 0.125 * x


def restrict_rows(rows):
    return [[cell_mean(rows[2 * c][v] + rows[2 * c + 1][v]) for v in range(len(rows[0]))] for c in range(len(rows) // 2)]


def halo_means(tiles):
    even = seg() % 2 == 0
    tiles = [x + jnp.where(even, rotl(x, -SEG), rotl(x, SEG)) for x in tiles]
    return [cell_mean(x) for x in tiles]


def load(ref, first, count):
    return [[ref[v, first + r] for v in range(NV)] for r in range(count)]


def store(ref, first, rows):
    for r, row in enumerate(rows):
        for v in range(NV):
            ref[v, first + r] = row[v]


def load_tiles(ref):
    return [[ref[g, v] for v in range(NV)] for g in range(2)]


def store_tiles(ref, tiles):
    for g in range(2):
        for v in range(NV):
            ref[g, v] = tiles[g][v]


def table_kernel(a_ref, type_ref, rot_ref, table_ref):
    values = [a_ref[d, u, v] for d in range(3) for u in range(NV) for v in range(NV)]
    for face in range(2):
        kind, rot = type_ref[0, face], rot_ref[0, face]
        values += [kind.astype(jnp.float32), (rot % 2).astype(jnp.float32), (rot // 2 % 2).astype(jnp.float32)]
    for n, value in enumerate(values):
        table_ref[n] = jnp.full((8, 128), value, jnp.float32)


def coefficients(table_ref):
    return lambda d, u, v: table_ref[(d * NV + u) * NV + v]


def meta_of(table_ref):
    first = 3 * NV * NV
    return [table_ref[first + n] for n in range(6)]


def masked(tiles):
    o = place()
    s = lax.axis_index("sub")
    final = lax.axis_size("sub") - 1
    inside = ((o < HALO) & (s != 0)) | ((o >= HALO) & (o < 2 * HALO) & (s != final))
    return [[jnp.where(inside, x, 0.0) for x in tile] for tile in tiles]


def is_even():
    return lax.axis_index("blk") % 2 == 0


def send(ma, mb, at, first, last):
    even = is_even()
    for n, (lo, hi) in enumerate(zip(first, last)):
        ma[at + n] = jnp.where(even, hi, lo)
        mb[at + n] = jnp.where(even, lo, hi)


def receive(ga, gb, at, count):
    even = is_even()
    below, above = [], []
    for n in range(at, at + count):
        a, b = ga[n], gb[n]
        below.append(jnp.where(even, b, a))
        above.append(jnp.where(even, a, b))
    return below, above


def send_rows(ma, mb, at, rows):
    send(ma, mb, at, rows[0] + rows[1], rows[-2] + rows[-1])


def receive_rows(ga, gb, at):
    below, above = receive(ga, gb, at, 2 * NV)
    return [below[:NV], below[NV:]], [above[:NV], above[NV:]]


def send_halo(ma, mb, at, halo):
    low = seg() < 2
    first = [jnp.where(low, halo[0][p], rotl(halo[0][p + 1], 64)) for p in range(0, NV, 2)]
    last = [jnp.where(low, rotl(halo[1][p + 1], 64), halo[1][p]) for p in range(0, NV, 2)]
    send(ma, mb, at, first, last)


def receive_halo(ga, gb, at):
    below, above = receive(ga, gb, at, NV // 2)

    def spread(tiles):
        return [y for x in tiles for y in (x, rotl(x, 64))]

    return spread(below), spread(above)


def send_coarse(ma, mb, at, first, second):
    j_even, k_even = iota_j() % 2 == 0, iota_k() % 2 == 0

    def joined(r0, r1):
        out = []
        for v in range(NV):
            x, y = (jnp.where(j_even, first[r][v], second[r][v]) for r in (r0, r1))
            out.append(jnp.where(k_even, x, y))
        return out

    send(ma, mb, at, joined(0, 1), joined(-2, -1))


def receive_coarse(ga, gb, at):
    j_even, k_even = iota_j() % 2 == 0, iota_k() % 2 == 0
    fields = ([], [])
    for tiles in receive(ga, gb, at, NV):
        rows = ([], [])
        for x in tiles:
            rows[0].append(jnp.where(k_even, x, rotl(x, 1)))
            rows[1].append(jnp.where(k_even, rotl(x, -1), x))
        fields[0].append([[jnp.where(j_even, x, rots(x, 1)) for x in row] for row in rows])
        fields[1].append([[jnp.where(j_even, rots(x, -1), x) for x in row] for row in rows])
    return fields


def pack_kernel(q_ref, dt_ref, ends_ref, ma, mb, to_left, to_right):
    rows = load(q_ref, 0, NI)
    ends = pack_ends(rows)
    store_tiles(ends_ref, ends)
    r, lower = seg(), place() < HALO
    tiles = ends[0] + ends[1]
    for g in range(2):
        acc = rotl(dt_ref[4 * g], HALO)
        for p in range(1, 4):
            acc = jnp.where(r == p, rotl(dt_ref[4 * g + p], HALO + p * SEG), acc)
        tiles.append(acc)
    for n in range(NV + 1):
        x, y = tiles[2 * n], tiles[2 * n + 1]
        to_right[n] = jnp.where(lower, x, rotl(y, HALO))
        to_left[n] = jnp.where(lower, rotl(y, -HALO), x)
    send_rows(ma, mb, 0, rows)


def unpack(from_right, from_left):
    lower = place() < HALO
    tiles = []
    for n in range(NV + 1):
        x, y = from_left[n], from_right[n]
        tiles.append(jnp.where(lower, x, y))
        tiles.append(jnp.where(lower, rotl(x, -HALO), rotl(y, HALO)))
    halo = masked([tiles[:NV], tiles[NV : 2 * NV]])
    return halo, tiles[2 * NV :]


def advance(start, dt, twice, factor):
    return [[start[i][v] - (0.5 * factor * dt[i]) * twice[i][v] for v in range(NV)] for i in range(len(start))]


def first_kernel(table_ref, q_ref, dt_ref, ga, gb, from_right, from_left, t1_ref, h0_ref, dth_ref, ma, mb):
    a, meta = coefficients(table_ref), meta_of(table_ref)
    h0, dth = unpack(from_right, from_left)
    store_tiles(h0_ref, h0)
    for g in range(2):
        dth_ref[g] = dth[g]
    send_halo(ma, mb, 2 * NV, h0)
    t0 = load(q_ref, 0, NI)
    below, above = receive_rows(ga, gb, 0)
    twice = residual2(with_ghosts(t0, below, above, meta), h0, a, 1)
    t1 = advance(t0, [dt_ref[i] for i in range(NI)], twice, 0.4)
    store(t1_ref, 0, t1)
    send_rows(ma, mb, 0, t1)


def second_kernel(
    table_ref, q_ref, t1_ref, h0_ref, ends_ref, dt_ref, dth_ref, ga, gb, t2_ref, h1_ref, ma, mb
):
    a, meta = coefficients(table_ref), meta_of(table_ref)
    h0 = load_tiles(h0_ref)
    below, above = receive_halo(ga, gb, 2 * NV)
    twice = halo_residual2(h0, halo_ghost(h0, below, above, meta), load_tiles(ends_ref), a)
    h1 = masked(advance(h0, [dth_ref[g] for g in range(2)], twice, 0.4))
    store_tiles(h1_ref, h1)
    send_halo(ma, mb, 2 * NV, h1)
    t0, t1 = load(q_ref, 0, NI), load(t1_ref, 0, NI)
    below, above = receive_rows(ga, gb, 0)
    twice = residual2(with_ghosts(t1, below, above, meta), h1, a, 1)
    t2 = advance(t0, [dt_ref[i] for i in range(NI)], twice, 1.0)
    store(t2_ref, 0, t2)
    send_rows(ma, mb, 0, t2)


def third_kernel(
    table_ref, t1_ref, t2_ref, h0_ref, h1_ref, dt_ref, dth_ref, ga, gb, res_ref, h2_ref, c1_ref, mean_ref, ma, mb
):
    a, meta = coefficients(table_ref), meta_of(table_ref)
    h0, h1 = load_tiles(h0_ref), load_tiles(h1_ref)
    below, above = receive_halo(ga, gb, 2 * NV)
    twice = halo_residual2(h1, halo_ghost(h1, below, above, meta), pack_ends(load(t1_ref, 0, NI)), a)
    h2 = masked(advance(h0, [dth_ref[g] for g in range(2)], twice, 1.0))
    store_tiles(h2_ref, h2)
    send_halo(ma, mb, NV, h2)
    t2 = load(t2_ref, 0, NI)
    below, above = receive_rows(ga, gb, 0)
    twice = residual2(with_ghosts(t2, below, above, meta), h2, a, 1)
    res = [[0.5 * x for x in row] for row in twice]
    store(res_ref, 0, res)
    start, mean = restrict_rows(t2), restrict_rows(res)
    store(mean_ref, 0, mean)
    c1 = []
    for c in range(NI // 2):
        step = cell_mean(dt_ref[2 * c] + dt_ref[2 * c + 1])
        c1.append([start[c][v] - (0.4 * step) * mean[c][v] for v in range(NV)])
    store(c1_ref, 0, c1)
    send_coarse(ma, mb, 0, c1, start)


def fourth_kernel(table_ref, t2_ref, h2_ref, c1_ref, mean_ref, dt_ref, dth_ref, res_ref, ga, gb, out_hbm, res_hbm, out_ref, sems):
    a, meta = coefficients(table_ref), meta_of(table_ref)
    half = NI // 2
    copies = [pltpu.make_async_copy(res_ref, res_hbm, sems.at[half])]
    copies[0].start()
    h2, t2 = load_tiles(h2_ref), load(t2_ref, 0, NI)
    below, above = receive_halo(ga, gb, NV)
    twice = halo_residual2(h2, halo_ghost(h2, below, above, meta), pack_ends(t2), a)
    means = halo_means(h2[0] + h2[1] + [dth_ref[0], dth_ref[1]] + twice[0] + twice[1])
    start_h, step_h, mean_h = means[: 2 * NV], means[2 * NV : 2 * NV + 2], means[2 * NV + 2 :]
    c1_h = [start_h[t] - (0.2 * step_h[t // NV]) * mean_h[t] for t in range(2 * NV)]
    start_h = [start_h[:NV], start_h[NV:]]
    c1_h = masked([c1_h[:NV], c1_h[NV:]])
    start, c1 = restrict_rows(t2), load(c1_ref, 0, half)
    (below1, above1), (below0, above0) = receive_coarse(ga, gb, 0)
    twice0 = residual2(with_ghosts(start, below0, above0, meta), start_h, a, 2)
    twice1 = residual2(with_ghosts(c1, below1, above1, meta), c1_h, a, 2)
    for c in range(half):
        step = cell_mean(dt_ref[2 * c] + dt_ref[2 * c + 1])
        for v in range(NV):
            change = -step * (0.5 * (twice1[c][v] - twice0[c][v]) + mean_ref[v, c])
            out_ref[v, 2 * c] = t2[2 * c][v] + change
            out_ref[v, 2 * c + 1] = t2[2 * c + 1][v] + change
    for c in range(half):
        rows = pl.ds(2 * c, 2)
        copies.append(pltpu.make_async_copy(out_ref.at[:, rows], out_hbm.at[:, rows], sems.at[c]))
        copies[-1].start()
    for copy in copies:
        copy.wait()


def field(rows):
    return (NV, rows, 8, 128)


def tiles_of(*count):
    return (*count, 8, 128)


def call(kernel, arrays, outs, scalars=(), out_space=pltpu.VMEM, scratch=()):
    smem, vmem = pl.BlockSpec(memory_space=pltpu.SMEM), pl.BlockSpec(memory_space=pltpu.VMEM)
    return pl.pallas_call(
        kernel,
        out_shape=[jax.ShapeDtypeStruct(shape, jnp.float32) for shape in outs],
        in_specs=[smem] * len(scalars) + [vmem] * len(arrays),
        out_specs=[pl.BlockSpec(memory_space=out_space)] * len(outs),
        scratch_shapes=scratch,
        compiler_params=pltpu.CompilerParams(vmem_limit_bytes=VMEM_LIMIT),
    )(*scalars, *arrays)


def cycle(flow_state, timestep, coupling, face_type, face_rot):
    blocks, parts = lax.axis_size("blk"), lax.axis_size("sub")
    chip = [(b, b ^ 1) for b in range(blocks)]
    link = [(b, (b + 1) % blocks if b % 2 else (b - 1) % blocks) for b in range(blocks)]
    ahead = [(s, s + 1) for s in range(parts - 1)]
    back = [(s + 1, s) for s in range(parts - 1)]
    pair = tiles_of(2, NV)

    def exchange(ma, mb):
        gb = lax.ppermute(mb, "blk", link)
        ga = lax.ppermute(ma, "blk", chip)
        return ga, gb

    (table,) = call(table_kernel, (), (tiles_of(3 * NV * NV + 6),), (coupling, face_type, face_rot))
    ends, ma, mb, to_left, to_right = call(
        pack_kernel,
        (flow_state, timestep),
        (pair, tiles_of(2 * NV), tiles_of(2 * NV), tiles_of(NV + 1), tiles_of(NV + 1)),
    )
    ga, gb = exchange(ma, mb)
    from_right = lax.ppermute(to_left, "sub", back)
    from_left = lax.ppermute(to_right, "sub", ahead)

    message = tiles_of(2 * NV + NV // 2)
    t1, h0, dth, ma, mb = call(
        first_kernel,
        (table, flow_state, timestep, ga, gb, from_right, from_left),
        (field(NI), pair, tiles_of(2), message, message),
    )
    ga, gb = exchange(ma, mb)

    t2, h1, ma, mb = call(
        second_kernel,
        (table, flow_state, t1, h0, ends, timestep, dth, ga, gb),
        (field(NI), pair, message, message),
    )
    ga, gb = exchange(ma, mb)

    message = tiles_of(NV + NV // 2)
    res, h2, c1, mean, ma, mb = call(
        third_kernel,
        (table, t1, t2, h0, h1, timestep, dth, ga, gb),
        (field(NI), pair, field(NI // 2), field(NI // 2), message, message),
    )
    ga, gb = exchange(ma, mb)

    updated, res = call(
        fourth_kernel,
        (table, t2, h2, c1, mean, timestep, dth, res, ga, gb),
        (field(NI), field(NI)),
        out_space=pltpu.HBM,
        scratch=(pltpu.VMEM(field(NI), jnp.float32), pltpu.SemaphoreType.DMA((NI // 2 + 1,))),
    )
    return (updated, res)


def solution(mesh):
    return jax.shard_map(
        cycle,
        mesh=mesh,
        in_specs=(
            P(None, "blk", None, "sub"),
            P("blk", None, "sub"),
            P(),
            P("blk", None),
            P("blk", None),
        ),
        out_specs=(P(None, "blk", None, "sub"), P(None, "blk", None, "sub")),
        check_vma=False,
    )
```

```python
import jax
import jax.numpy as jnp
from jax import lax
from jax.experimental import pallas as pl
from jax.experimental.pallas import tpu as pltpu
from jax.sharding import PartitionSpec as P


NV = 6
NI = 8
HALO = 10
SEG = 32
VMEM_LIMIT = 12 * 1024 * 1024

C0, C1, C2 = 0.44, -0.26, 0.04


def iota_j():
    return lax.broadcasted_iota(jnp.int32, (8, 128), 0)


def iota_k():
    return lax.broadcasted_iota(jnp.int32, (8, 128), 1)


def rotl(x, shift):
    return pltpu.roll(x, shift % 128, 1)


def rots(x, shift):
    return pltpu.roll(x, shift % 8, 0)


def reverse_j(x):
    j = iota_j()
    x = rots(x, 4)
    x = jnp.where((j // 2) % 2 == 0, rots(x, -2), rots(x, 2))
    return jnp.where(j % 2 == 0, rots(x, -1), rots(x, 1))


def ghost_rows(own2, prev2, next2, kind, flip, turn):
    nearest = []
    for r in range(2):
        picked = []
        for v in range(NV):
            wall = -own2[r][v] if v == 1 else own2[r][v]
            x = jnp.where(kind == 2, wall, 0.0)
            x = jnp.where(kind == 1, next2[r][v], x)
            x = jnp.where(kind == 0, prev2[r][v], x)
            picked.append(jnp.where(flip == 1, reverse_j(x), x))
        a, b = picked[2], picked[3]
        picked[2], picked[3] = jnp.where(turn == 1, -b, a), jnp.where(turn == 1, a, b)
        nearest.append(picked)
    return nearest


def with_ghosts(rows, below, above, meta):
    lo = ghost_rows([rows[0], rows[1]], [below[1], below[0]], [above[0], above[1]], *meta[:3])
    hi = ghost_rows([rows[-1], rows[-2]], [above[0], above[1]], [below[1], below[0]], *meta[3:])
    return [lo[1], lo[0]] + rows + [hi[0], hi[1]]


def flux(q, a, d):
    half = 0.5 * q[1 + d]
    out = []
    for u in range(NV):
        acc = (a(d, u, u) + half) * q[u]
        for v in range(NV):
            if v != u:
                acc = acc + a(d, u, v) * q[v]
        out.append(acc)
    return out


def flux_j(q, a):
    out, mirrored = [], []
    for u in range(NV):
        even = None
        for v in range(NV):
            if v != 2:
                term = a(1, u, v) * q[v]
                even = term if even is None else even + term
        if u == 2:
            even = even + 0.5 * (q[2] * q[2])
            odd = a(1, 2, 2) * q[2]
        else:
            odd = q[2] * (a(1, u, 2) + 0.5 * q[u])
        out.append(even + odd)
        mirrored.append(even - odd)
    return out, mirrored


def j_weights(unit):
    j = iota_j() // unit
    n = 8 // unit
    out = []
    for sign in (1.0, -1.0):
        end = (j == 0) | (j == n - 1)
        centre = jnp.where(end, C0 + sign * C1, C0) + 2 * C0
        near = C1 + sign * C2
        below = jnp.where(j == 0, 0.0, jnp.where((j == 1) | (j == n - 1), near, C1))
        above = jnp.where(j == n - 1, 0.0, jnp.where((j == 0) | (j == n - 2), near, C1))
        if n == 4:
            two = None
        else:
            two = (jnp.where(j >= 2, C2, 0.0), jnp.where(j <= n - 3, C2, 0.0))
        out.append((centre, below, above, two))
    return out


def seg():
    return iota_k() // SEG


def place():
    return iota_k() % SEG


def second_index(fj, gj, q, u, unit, weights, ends):
    centre, below, above, two = weights[1 if u == 2 else 0]
    x = q[u]
    acc = centre * x + below * rots(x, unit) + above * rots(x, -unit)
    if two is None:
        acc = acc + C2 * rots(x, 4)
    else:
        acc = acc + two[0] * rots(x, 2) + two[1] * rots(x, -2)
    up = jnp.where(ends[1], gj[u], rots(fj[u], -unit))
    down = jnp.where(ends[0], gj[u], rots(fj[u], unit))
    return acc + (up - down)


def residual2(padded, halo, a, unit):
    n = len(padded) - 4
    k, j = iota_k(), iota_j()
    weights = j_weights(unit)
    ends = (j < unit, j >= 8 - unit)
    low1, low2 = k < unit, k < 2 * unit
    high1, high2 = k >= 128 - unit, k >= 128 - 2 * unit
    upper = place() >= HALO
    edge = []
    for tile in halo:
        f = flux(tile, a, 2)
        edge.append([jnp.where(upper, f[u] + C1 * tile[u], f[u] - C1 * tile[u]) for u in range(NV)])
    beside = []
    for i in range(n):
        g, first = unit * i // 4, unit * i % 4 * SEG + HALO
        beside.append([(rotl(halo[g][u], -first), rotl(edge[g][u], -first)) for u in range(NV)])
    fi = {m: flux(padded[m], a, 0) for m in range(1, n + 3)}
    result = []
    for i in range(n):
        m = i + 2
        q = padded[m]
        fj, gj = flux_j(q, a)
        fk = flux(q, a, 2)
        row = []
        for u in range(NV):
            x = q[u]
            s, e = beside[i][u]
            acc = second_index(fj, gj, q, u, unit, weights, ends)
            acc = acc + (fi[m + 1][u] - fi[m - 1][u])
            acc = acc + C1 * (padded[m + 1][u] + padded[m - 1][u]) + C2 * (padded[m + 2][u] + padded[m - 2][u])
            t = C1 * x
            acc = acc + rotl(jnp.where(low1, e, fk[u] + t), -unit)
            acc = acc - rotl(jnp.where(high1, e, fk[u] - t), unit)
            acc = acc + C2 * (rotl(jnp.where(low2, s, x), -2 * unit) + rotl(jnp.where(high2, s, x), 2 * unit))
            row.append(acc)
        result.append(row)
    return result


def halo_residual2(halo, ghost, own, a):
    r, o = seg(), place()
    j = iota_j()
    weights = j_weights(1)
    ends = (j < 1, j >= 7)
    first, last, low, high = r == 0, r == 3, r < 2, r >= 2
    tiles = [halo[0], halo[1], ghost]
    up_i, down_i = [], []
    for t in tiles:
        f = flux(t, a, 0)
        up_i.append([f[u] + C1 * t[u] for u in range(NV)])
        down_i.append([f[u] - C1 * t[u] for u in range(NV)])
    upper = o >= HALO
    after1, after2 = o == HALO, (o == HALO) | (o == HALO + 1)
    before1, before2 = o == HALO - 1, (o == HALO - 1) | (o == HALO - 2)
    result = []
    for g in range(2):
        q, nxt, prv = tiles[g], (g + 1) % 3, (g + 2) % 3
        fj, gj = flux_j(q, a)
        fk = flux(q, a, 2)
        fo = flux(own[g], a, 2)
        row = []
        for u in range(NV):
            x, y = q[u], own[g][u]
            acc = second_index(fj, gj, q, u, 1, weights, ends)
            acc = acc + rotl(jnp.where(first, up_i[nxt][u], up_i[g][u]), -SEG)
            acc = acc - rotl(jnp.where(last, down_i[prv][u], down_i[g][u]), SEG)
            acc = acc + C2 * rotl(jnp.where(low, tiles[nxt][u], x) + jnp.where(high, tiles[prv][u], x), 2 * SEG)
            t = C1 * x
            e = jnp.where(upper, fo[u] + C1 * y, fo[u] - C1 * y)
            acc = acc + rotl(jnp.where(after1, e, fk[u] + t), -1)
            acc = acc - rotl(jnp.where(before1, e, fk[u] - t), 1)
            acc = acc + C2 * (rotl(jnp.where(after2, y, x), -2) + rotl(jnp.where(before2, y, x), 2))
            row.append(acc)
        result.append(row)
    return result


def pack_ends(rows):
    r = seg()
    out = []
    for g in range(2):
        tile = []
        for v in range(NV):
            acc = rotl(rows[4 * g][v], HALO)
            for p in range(1, 4):
                acc = jnp.where(r == p, rotl(rows[4 * g + p][v], HALO + p * SEG), acc)
            tile.append(acc)
        out.append(tile)
    return out


def halo_ghost(halo, below, above, meta):
    t_lo, flip_lo, turn_lo, t_hi, flip_hi, turn_hi = meta
    r = seg()
    high_side = r < 2
    even_part = r % 2 == 0

    def turned(x):
        return jnp.where(even_part, rotl(x, SEG), rotl(x, -SEG))

    flip = jnp.where(high_side, flip_hi, flip_lo)
    picked = []
    for v in range(NV):
        wall_lo, wall_hi = turned(halo[0][v]), turned(halo[1][v])
        if v == 1:
            wall_lo, wall_hi = -wall_lo, -wall_hi
        hi = jnp.where(t_hi == 2, wall_hi, 0.0)
        hi = jnp.where(t_hi == 1, turned(below[v]), hi)
        hi = jnp.where(t_hi == 0, above[v], hi)
        lo = jnp.where(t_lo == 2, wall_lo, 0.0)
        lo = jnp.where(t_lo == 1, turned(above[v]), lo)
        lo = jnp.where(t_lo == 0, below[v], lo)
        x = jnp.where(high_side, hi, lo)
        picked.append(jnp.where(flip == 1, reverse_j(x), x))
    turn = jnp.where(high_side, turn_hi, turn_lo) == 1
    b, c = picked[2], picked[3]
    picked[2], picked[3] = jnp.where(turn, -c, b), jnp.where(turn, b, c)
    return picked


def cell_mean(x):
    x = x + jnp.where(iota_j() % 2 == 0, rots(x, -1), rots(x, 1))
    x = x + jnp.where(iota_k() % 2 == 0, rotl(x, -1), rotl(x, 1))
    return 0.125 * x


def restrict_rows(rows):
    return [[cell_mean(rows[2 * c][v] + rows[2 * c + 1][v]) for v in range(len(rows[0]))] for c in range(len(rows) // 2)]


def halo_means(tiles):
    even = seg() % 2 == 0
    tiles = [x + jnp.where(even, rotl(x, -SEG), rotl(x, SEG)) for x in tiles]
    return [cell_mean(x) for x in tiles]


def load(ref, first, count):
    return [[ref[v, first + r] for v in range(NV)] for r in range(count)]


def store(ref, first, rows):
    for r, row in enumerate(rows):
        for v in range(NV):
            ref[v, first + r] = row[v]


def load_tiles(ref):
    return [[ref[g, v] for v in range(NV)] for g in range(2)]


def store_tiles(ref, tiles):
    for g in range(2):
        for v in range(NV):
            ref[g, v] = tiles[g][v]


def table_kernel(a_ref, type_ref, rot_ref, table_ref):
    values = [a_ref[d, u, v] for d in range(3) for u in range(NV) for v in range(NV)]
    for face in range(2):
        kind, rot = type_ref[0, face], rot_ref[0, face]
        values += [kind.astype(jnp.float32), (rot % 2).astype(jnp.float32), (rot // 2 % 2).astype(jnp.float32)]
    for n, value in enumerate(values):
        table_ref[n] = jnp.full((8, 128), value, jnp.float32)


def coefficients(table_ref):
    return lambda d, u, v: table_ref[(d * NV + u) * NV + v]


def meta_of(table_ref):
    first = 3 * NV * NV
    return [table_ref[first + n] for n in range(6)]


def masked(tiles):
    o = place()
    s = lax.axis_index("sub")
    final = lax.axis_size("sub") - 1
    inside = ((o < HALO) & (s != 0)) | ((o >= HALO) & (o < 2 * HALO) & (s != final))
    return [[jnp.where(inside, x, 0.0) for x in tile] for tile in tiles]


def is_even():
    return lax.axis_index("blk") % 2 == 0


def send(ma, mb, at, first, last):
    even = is_even()
    for n, (lo, hi) in enumerate(zip(first, last)):
        ma[at + n] = jnp.where(even, hi, lo)
        mb[at + n] = jnp.where(even, lo, hi)


def receive(ga, gb, at, count):
    even = is_even()
    below, above = [], []
    for n in range(at, at + count):
        a, b = ga[n], gb[n]
        below.append(jnp.where(even, b, a))
        above.append(jnp.where(even, a, b))
    return below, above


def send_rows(ma, mb, at, rows):
    send(ma, mb, at, rows[0] + rows[1], rows[-2] + rows[-1])


def receive_rows(ga, gb, at):
    below, above = receive(ga, gb, at, 2 * NV)
    return [below[:NV], below[NV:]], [above[:NV], above[NV:]]


def send_halo(ma, mb, at, halo):
    low = seg() < 2
    first = [jnp.where(low, halo[0][p], rotl(halo[0][p + 1], 64)) for p in range(0, NV, 2)]
    last = [jnp.where(low, rotl(halo[1][p + 1], 64), halo[1][p]) for p in range(0, NV, 2)]
    send(ma, mb, at, first, last)


def receive_halo(ga, gb, at):
    below, above = receive(ga, gb, at, NV // 2)

    def spread(tiles):
        return [y for x in tiles for y in (x, rotl(x, 64))]

    return spread(below), spread(above)


def send_coarse(ma, mb, at, first, second):
    j_even, k_even = iota_j() % 2 == 0, iota_k() % 2 == 0

    def joined(r0, r1):
        out = []
        for v in range(NV):
            x, y = (jnp.where(j_even, first[r][v], second[r][v]) for r in (r0, r1))
            out.append(jnp.where(k_even, x, y))
        return out

    send(ma, mb, at, joined(0, 1), joined(-2, -1))


def receive_coarse(ga, gb, at):
    j_even, k_even = iota_j() % 2 == 0, iota_k() % 2 == 0
    fields = ([], [])
    for tiles in receive(ga, gb, at, NV):
        rows = ([], [])
        for x in tiles:
            rows[0].append(jnp.where(k_even, x, rotl(x, 1)))
            rows[1].append(jnp.where(k_even, rotl(x, -1), x))
        fields[0].append([[jnp.where(j_even, x, rots(x, 1)) for x in row] for row in rows])
        fields[1].append([[jnp.where(j_even, rots(x, -1), x) for x in row] for row in rows])
    return fields


def prime_kernel(out_ref):
    out_ref[...] = jnp.zeros_like(out_ref)


def pack_kernel(prime_ref, q_ref, dt_ref, ends_ref, ma, mb, to_left, to_right):
    rows = load(q_ref, 0, NI)
    ends = pack_ends(rows)
    store_tiles(ends_ref, ends)
    r, lower = seg(), place() < HALO
    tiles = ends[0] + ends[1]
    for g in range(2):
        acc = rotl(dt_ref[4 * g], HALO)
        for p in range(1, 4):
            acc = jnp.where(r == p, rotl(dt_ref[4 * g + p], HALO + p * SEG), acc)
        tiles.append(acc)
    for n in range(NV + 1):
        x, y = tiles[2 * n], tiles[2 * n + 1]
        to_right[n] = jnp.where(lower, x, rotl(y, HALO))
        to_left[n] = jnp.where(lower, rotl(y, -HALO), x)
    send_rows(ma, mb, 0, rows)


def unpack(from_right, from_left):
    lower = place() < HALO
    tiles = []
    for n in range(NV + 1):
        x, y = from_left[n], from_right[n]
        tiles.append(jnp.where(lower, x, y))
        tiles.append(jnp.where(lower, rotl(x, -HALO), rotl(y, HALO)))
    halo = masked([tiles[:NV], tiles[NV : 2 * NV]])
    return halo, tiles[2 * NV :]


def advance(start, dt, twice, factor):
    return [[start[i][v] - (0.5 * factor * dt[i]) * twice[i][v] for v in range(NV)] for i in range(len(start))]


def first_kernel(table_ref, q_ref, dt_ref, ga, gb, from_right, from_left, t1_ref, h0_ref, dth_ref, ma, mb):
    a, meta = coefficients(table_ref), meta_of(table_ref)
    h0, dth = unpack(from_right, from_left)
    store_tiles(h0_ref, h0)
    for g in range(2):
        dth_ref[g] = dth[g]
    send_halo(ma, mb, 2 * NV, h0)
    t0 = load(q_ref, 0, NI)
    below, above = receive_rows(ga, gb, 0)
    twice = residual2(with_ghosts(t0, below, above, meta), h0, a, 1)
    t1 = advance(t0, [dt_ref[i] for i in range(NI)], twice, 0.4)
    store(t1_ref, 0, t1)
    send_rows(ma, mb, 0, t1)


def second_kernel(
    table_ref, q_ref, t1_ref, h0_ref, ends_ref, dt_ref, dth_ref, ga, gb, t2_ref, h1_ref, ma, mb
):
    a, meta = coefficients(table_ref), meta_of(table_ref)
    h0 = load_tiles(h0_ref)
    below, above = receive_halo(ga, gb, 2 * NV)
    twice = halo_residual2(h0, halo_ghost(h0, below, above, meta), load_tiles(ends_ref), a)
    h1 = masked(advance(h0, [dth_ref[g] for g in range(2)], twice, 0.4))
    store_tiles(h1_ref, h1)
    send_halo(ma, mb, 2 * NV, h1)
    t0, t1 = load(q_ref, 0, NI), load(t1_ref, 0, NI)
    below, above = receive_rows(ga, gb, 0)
    twice = residual2(with_ghosts(t1, below, above, meta), h1, a, 1)
    t2 = advance(t0, [dt_ref[i] for i in range(NI)], twice, 1.0)
    store(t2_ref, 0, t2)
    send_rows(ma, mb, 0, t2)


def third_kernel(
    table_ref, t1_ref, t2_ref, h0_ref, h1_ref, dt_ref, dth_ref, ga, gb, res_ref, h2_ref, c1_ref, mean_ref, ma, mb
):
    a, meta = coefficients(table_ref), meta_of(table_ref)
    h0, h1 = load_tiles(h0_ref), load_tiles(h1_ref)
    below, above = receive_halo(ga, gb, 2 * NV)
    twice = halo_residual2(h1, halo_ghost(h1, below, above, meta), pack_ends(load(t1_ref, 0, NI)), a)
    h2 = masked(advance(h0, [dth_ref[g] for g in range(2)], twice, 1.0))
    store_tiles(h2_ref, h2)
    send_halo(ma, mb, NV, h2)
    t2 = load(t2_ref, 0, NI)
    below, above = receive_rows(ga, gb, 0)
    twice = residual2(with_ghosts(t2, below, above, meta), h2, a, 1)
    res = [[0.5 * x for x in row] for row in twice]
    store(res_ref, 0, res)
    start, mean = restrict_rows(t2), restrict_rows(res)
    store(mean_ref, 0, mean)
    c1 = []
    for c in range(NI // 2):
        step = cell_mean(dt_ref[2 * c] + dt_ref[2 * c + 1])
        c1.append([start[c][v] - (0.4 * step) * mean[c][v] for v in range(NV)])
    store(c1_ref, 0, c1)
    send_coarse(ma, mb, 0, c1, start)


def fourth_kernel(table_ref, t2_ref, h2_ref, c1_ref, mean_ref, dt_ref, dth_ref, res_ref, ga, gb, out_hbm, res_hbm, out_ref, sems):
    a, meta = coefficients(table_ref), meta_of(table_ref)
    half = NI // 2
    copies = [pltpu.make_async_copy(res_ref, res_hbm, sems.at[half])]
    copies[0].start()
    h2, t2 = load_tiles(h2_ref), load(t2_ref, 0, NI)
    below, above = receive_halo(ga, gb, NV)
    twice = halo_residual2(h2, halo_ghost(h2, below, above, meta), pack_ends(t2), a)
    means = halo_means(h2[0] + h2[1] + [dth_ref[0], dth_ref[1]] + twice[0] + twice[1])
    start_h, step_h, mean_h = means[: 2 * NV], means[2 * NV : 2 * NV + 2], means[2 * NV + 2 :]
    c1_h = [start_h[t] - (0.2 * step_h[t // NV]) * mean_h[t] for t in range(2 * NV)]
    start_h = [start_h[:NV], start_h[NV:]]
    c1_h = masked([c1_h[:NV], c1_h[NV:]])
    start, c1 = restrict_rows(t2), load(c1_ref, 0, half)
    (below1, above1), (below0, above0) = receive_coarse(ga, gb, 0)
    twice0 = residual2(with_ghosts(start, below0, above0, meta), start_h, a, 2)
    twice1 = residual2(with_ghosts(c1, below1, above1, meta), c1_h, a, 2)
    for c in range(half):
        step = cell_mean(dt_ref[2 * c] + dt_ref[2 * c + 1])
        for v in range(NV):
            change = -step * (0.5 * (twice1[c][v] - twice0[c][v]) + mean_ref[v, c])
            out_ref[v, 2 * c] = t2[2 * c][v] + change
            out_ref[v, 2 * c + 1] = t2[2 * c + 1][v] + change
    for c in range(half):
        rows = pl.ds(2 * c, 2)
        copies.append(pltpu.make_async_copy(out_ref.at[:, rows], out_hbm.at[:, rows], sems.at[c]))
        copies[-1].start()
    for copy in copies:
        copy.wait()


def field(rows):
    return (NV, rows, 8, 128)


def tiles_of(*count):
    return (*count, 8, 128)


def call(kernel, arrays, outs, scalars=(), out_space=pltpu.VMEM, scratch=()):
    smem, vmem = pl.BlockSpec(memory_space=pltpu.SMEM), pl.BlockSpec(memory_space=pltpu.VMEM)
    return pl.pallas_call(
        kernel,
        out_shape=[jax.ShapeDtypeStruct(shape, jnp.float32) for shape in outs],
        in_specs=[smem] * len(scalars) + [vmem] * len(arrays),
        out_specs=[pl.BlockSpec(memory_space=out_space)] * len(outs),
        scratch_shapes=scratch,
        compiler_params=pltpu.CompilerParams(vmem_limit_bytes=VMEM_LIMIT),
    )(*scalars, *arrays)


def cycle(flow_state, timestep, coupling, face_type, face_rot):
    blocks, parts = lax.axis_size("blk"), lax.axis_size("sub")
    chip = [(b, b ^ 1) for b in range(blocks)]
    link = [(b, (b + 1) % blocks if b % 2 else (b - 1) % blocks) for b in range(blocks)]
    ahead = [(s, s + 1) for s in range(parts - 1)]
    back = [(s + 1, s) for s in range(parts - 1)]
    pair = tiles_of(2, NV)

    def exchange(ma, mb):
        gb = lax.ppermute(mb, "blk", link)
        ga = lax.ppermute(ma, "blk", chip)
        return ga, gb

    (table,) = call(table_kernel, (), (tiles_of(3 * NV * NV + 6),), (coupling, face_type, face_rot))
    (prime,) = call(prime_kernel, (), (tiles_of(114),))
    ends, ma, mb, to_left, to_right = call(
        pack_kernel,
        (prime, flow_state, timestep),
        (pair, tiles_of(2 * NV), tiles_of(2 * NV), tiles_of(NV + 1), tiles_of(NV + 1)),
    )
    ga, gb = exchange(ma, mb)
    from_right = lax.ppermute(to_left, "sub", back)
    from_left = lax.ppermute(to_right, "sub", ahead)

    message = tiles_of(2 * NV + NV // 2)
    t1, h0, dth, ma, mb = call(
        first_kernel,
        (table, flow_state, timestep, ga, gb, from_right, from_left),
        (field(NI), pair, tiles_of(2), message, message),
    )
    ga, gb = exchange(ma, mb)

    t2, h1, ma, mb = call(
        second_kernel,
        (table, flow_state, t1, h0, ends, timestep, dth, ga, gb),
        (field(NI), pair, message, message),
    )
    ga, gb = exchange(ma, mb)

    message = tiles_of(NV + NV // 2)
    res, h2, c1, mean, ma, mb = call(
        third_kernel,
        (table, t1, t2, h0, h1, timestep, dth, ga, gb),
        (field(NI), pair, field(NI // 2), field(NI // 2), message, message),
    )
    ga, gb = exchange(ma, mb)

    updated, res = call(
        fourth_kernel,
        (table, t2, h2, c1, mean, timestep, dth, res, ga, gb),
        (field(NI), field(NI)),
        out_space=pltpu.HBM,
        scratch=(pltpu.VMEM(field(NI), jnp.float32), pltpu.SemaphoreType.DMA((NI // 2 + 1,))),
    )
    return (updated, res)


def solution(mesh):
    return jax.shard_map(
        cycle,
        mesh=mesh,
        in_specs=(
            P(None, "blk", None, "sub"),
            P("blk", None, "sub"),
            P(),
            P("blk", None),
            P("blk", None),
        ),
        out_specs=(P(None, "blk", None, "sub"), P(None, "blk", None, "sub")),
        check_vma=False,
    )
```

```python
import jax
import jax.numpy as jnp
from jax import lax
from jax.experimental import pallas as pl
from jax.experimental.pallas import tpu as pltpu
from jax.sharding import PartitionSpec as P


NV = 6
NI = 8
HALO = 10
SEG = 32
VMEM_LIMIT = 12 * 1024 * 1024

C0, C1, C2 = 0.44, -0.26, 0.04


def iota_j():
    return lax.broadcasted_iota(jnp.int32, (8, 128), 0)


def iota_k():
    return lax.broadcasted_iota(jnp.int32, (8, 128), 1)


def rotl(x, shift):
    return pltpu.roll(x, shift % 128, 1)


def rots(x, shift):
    return pltpu.roll(x, shift % 8, 0)


def reverse_j(x):
    j = iota_j()
    x = rots(x, 4)
    x = jnp.where((j // 2) % 2 == 0, rots(x, -2), rots(x, 2))
    return jnp.where(j % 2 == 0, rots(x, -1), rots(x, 1))


def ghost_rows(own2, prev2, next2, kind, flip, turn):
    nearest = []
    for r in range(2):
        picked = []
        for v in range(NV):
            wall = -own2[r][v] if v == 1 else own2[r][v]
            x = jnp.where(kind == 2, wall, 0.0)
            x = jnp.where(kind == 1, next2[r][v], x)
            x = jnp.where(kind == 0, prev2[r][v], x)
            picked.append(jnp.where(flip == 1, reverse_j(x), x))
        a, b = picked[2], picked[3]
        picked[2], picked[3] = jnp.where(turn == 1, -b, a), jnp.where(turn == 1, a, b)
        nearest.append(picked)
    return nearest


def low_ghosts(rows, below, above, meta):
    lo = ghost_rows([rows[0], rows[1]], [below[1], below[0]], [above[0], above[1]], *meta[:3])
    return [lo[1], lo[0]]


def high_ghosts(rows, below, above, meta):
    return ghost_rows([rows[-1], rows[-2]], [above[0], above[1]], [below[1], below[0]], *meta[3:])


def with_ghosts(rows, below, above, meta):
    return low_ghosts(rows, below, above, meta) + rows + high_ghosts(rows, below, above, meta)


def flux(q, a, d):
    half = 0.5 * q[1 + d]
    out = []
    for u in range(NV):
        acc = (a(d, u, u) + half) * q[u]
        for v in range(NV):
            if v != u:
                acc = acc + a(d, u, v) * q[v]
        out.append(acc)
    return out


def flux_j(q, a):
    out, mirrored = [], []
    for u in range(NV):
        even = None
        for v in range(NV):
            if v != 2:
                term = a(1, u, v) * q[v]
                even = term if even is None else even + term
        if u == 2:
            even = even + 0.5 * (q[2] * q[2])
            odd = a(1, 2, 2) * q[2]
        else:
            odd = q[2] * (a(1, u, 2) + 0.5 * q[u])
        out.append(even + odd)
        mirrored.append(even - odd)
    return out, mirrored


def j_weights(unit):
    j = iota_j() // unit
    n = 8 // unit
    out = []
    for sign in (1.0, -1.0):
        end = (j == 0) | (j == n - 1)
        centre = jnp.where(end, C0 + sign * C1, C0) + 2 * C0
        near = C1 + sign * C2
        below = jnp.where(j == 0, 0.0, jnp.where((j == 1) | (j == n - 1), near, C1))
        above = jnp.where(j == n - 1, 0.0, jnp.where((j == 0) | (j == n - 2), near, C1))
        if n == 4:
            two = None
        else:
            two = (jnp.where(j >= 2, C2, 0.0), jnp.where(j <= n - 3, C2, 0.0))
        out.append((centre, below, above, two))
    return out


def seg():
    return iota_k() // SEG


def place():
    return iota_k() % SEG


def second_index(fj, gj, q, u, unit, weights, ends):
    centre, below, above, two = weights[1 if u == 2 else 0]
    x = q[u]
    acc = centre * x + below * rots(x, unit) + above * rots(x, -unit)
    if two is None:
        acc = acc + C2 * rots(x, 4)
    else:
        acc = acc + two[0] * rots(x, 2) + two[1] * rots(x, -2)
    up = jnp.where(ends[1], gj[u], rots(fj[u], -unit))
    down = jnp.where(ends[0], gj[u], rots(fj[u], unit))
    return acc + (up - down)


def residual2(padded, halo, a, unit, start=0):
    n = len(padded) - 4
    k, j = iota_k(), iota_j()
    weights = j_weights(unit)
    ends = (j < unit, j >= 8 - unit)
    low1, low2 = k < unit, k < 2 * unit
    high1, high2 = k >= 128 - unit, k >= 128 - 2 * unit
    upper = place() >= HALO
    edge = []
    for tile in halo:
        f = flux(tile, a, 2)
        edge.append([jnp.where(upper, f[u] + C1 * tile[u], f[u] - C1 * tile[u]) for u in range(NV)])
    beside = []
    for i in range(n):
        g, first = unit * (start + i) // 4, unit * (start + i) % 4 * SEG + HALO
        beside.append([(rotl(halo[g][u], -first), rotl(edge[g][u], -first)) for u in range(NV)])
    fi = {m: flux(padded[m], a, 0) for m in range(1, n + 3)}
    result = []
    for i in range(n):
        m = i + 2
        q = padded[m]
        fj, gj = flux_j(q, a)
        fk = flux(q, a, 2)
        row = []
        for u in range(NV):
            x = q[u]
            s, e = beside[i][u]
            acc = second_index(fj, gj, q, u, unit, weights, ends)
            acc = acc + (fi[m + 1][u] - fi[m - 1][u])
            acc = acc + C1 * (padded[m + 1][u] + padded[m - 1][u]) + C2 * (padded[m + 2][u] + padded[m - 2][u])
            t = C1 * x
            acc = acc + rotl(jnp.where(low1, e, fk[u] + t), -unit)
            acc = acc - rotl(jnp.where(high1, e, fk[u] - t), unit)
            acc = acc + C2 * (rotl(jnp.where(low2, s, x), -2 * unit) + rotl(jnp.where(high2, s, x), 2 * unit))
            row.append(acc)
        result.append(row)
    return result


def halo_residual2(halo, ghost, own, a):
    r, o = seg(), place()
    j = iota_j()
    weights = j_weights(1)
    ends = (j < 1, j >= 7)
    first, last, low, high = r == 0, r == 3, r < 2, r >= 2
    tiles = [halo[0], halo[1], ghost]
    up_i, down_i = [], []
    for t in tiles:
        f = flux(t, a, 0)
        up_i.append([f[u] + C1 * t[u] for u in range(NV)])
        down_i.append([f[u] - C1 * t[u] for u in range(NV)])
    upper = o >= HALO
    after1, after2 = o == HALO, (o == HALO) | (o == HALO + 1)
    before1, before2 = o == HALO - 1, (o == HALO - 1) | (o == HALO - 2)
    result = []
    for g in range(2):
        q, nxt, prv = tiles[g], (g + 1) % 3, (g + 2) % 3
        fj, gj = flux_j(q, a)
        fk = flux(q, a, 2)
        fo = flux(own[g], a, 2)
        row = []
        for u in range(NV):
            x, y = q[u], own[g][u]
            acc = second_index(fj, gj, q, u, 1, weights, ends)
            acc = acc + rotl(jnp.where(first, up_i[nxt][u], up_i[g][u]), -SEG)
            acc = acc - rotl(jnp.where(last, down_i[prv][u], down_i[g][u]), SEG)
            acc = acc + C2 * rotl(jnp.where(low, tiles[nxt][u], x) + jnp.where(high, tiles[prv][u], x), 2 * SEG)
            t = C1 * x
            e = jnp.where(upper, fo[u] + C1 * y, fo[u] - C1 * y)
            acc = acc + rotl(jnp.where(after1, e, fk[u] + t), -1)
            acc = acc - rotl(jnp.where(before1, e, fk[u] - t), 1)
            acc = acc + C2 * (rotl(jnp.where(after2, y, x), -2) + rotl(jnp.where(before2, y, x), 2))
            row.append(acc)
        result.append(row)
    return result


def pack_ends(rows):
    r = seg()
    out = []
    for g in range(2):
        tile = []
        for v in range(NV):
            acc = rotl(rows[4 * g][v], HALO)
            for p in range(1, 4):
                acc = jnp.where(r == p, rotl(rows[4 * g + p][v], HALO + p * SEG), acc)
            tile.append(acc)
        out.append(tile)
    return out


def halo_ghost(halo, below, above, meta):
    t_lo, flip_lo, turn_lo, t_hi, flip_hi, turn_hi = meta
    r = seg()
    high_side = r < 2
    even_part = r % 2 == 0

    def turned(x):
        return jnp.where(even_part, rotl(x, SEG), rotl(x, -SEG))

    flip = jnp.where(high_side, flip_hi, flip_lo)
    picked = []
    for v in range(NV):
        wall_lo, wall_hi = turned(halo[0][v]), turned(halo[1][v])
        if v == 1:
            wall_lo, wall_hi = -wall_lo, -wall_hi
        hi = jnp.where(t_hi == 2, wall_hi, 0.0)
        hi = jnp.where(t_hi == 1, turned(below[v]), hi)
        hi = jnp.where(t_hi == 0, above[v], hi)
        lo = jnp.where(t_lo == 2, wall_lo, 0.0)
        lo = jnp.where(t_lo == 1, turned(above[v]), lo)
        lo = jnp.where(t_lo == 0, below[v], lo)
        x = jnp.where(high_side, hi, lo)
        picked.append(jnp.where(flip == 1, reverse_j(x), x))
    turn = jnp.where(high_side, turn_hi, turn_lo) == 1
    b, c = picked[2], picked[3]
    picked[2], picked[3] = jnp.where(turn, -c, b), jnp.where(turn, b, c)
    return picked


def cell_mean(x):
    x = x + jnp.where(iota_j() % 2 == 0, rots(x, -1), rots(x, 1))
    x = x + jnp.where(iota_k() % 2 == 0, rotl(x, -1), rotl(x, 1))
    return 0.125 * x


def restrict_rows(rows):
    return [[cell_mean(rows[2 * c][v] + rows[2 * c + 1][v]) for v in range(len(rows[0]))] for c in range(len(rows) // 2)]


def halo_means(tiles):
    even = seg() % 2 == 0
    tiles = [x + jnp.where(even, rotl(x, -SEG), rotl(x, SEG)) for x in tiles]
    return [cell_mean(x) for x in tiles]


def load(ref, first, count):
    return [[ref[v, first + r] for v in range(NV)] for r in range(count)]


def store(ref, first, rows):
    for r, row in enumerate(rows):
        for v in range(NV):
            ref[v, first + r] = row[v]


def load_tiles(ref):
    return [[ref[g, v] for v in range(NV)] for g in range(2)]


def store_tiles(ref, tiles):
    for g in range(2):
        for v in range(NV):
            ref[g, v] = tiles[g][v]


def table_kernel(a_ref, type_ref, rot_ref, table_ref):
    values = [a_ref[d, u, v] for d in range(3) for u in range(NV) for v in range(NV)]
    for face in range(2):
        kind, rot = type_ref[0, face], rot_ref[0, face]
        values += [kind.astype(jnp.float32), (rot % 2).astype(jnp.float32), (rot // 2 % 2).astype(jnp.float32)]
    for n, value in enumerate(values):
        table_ref[n] = jnp.full((8, 128), value, jnp.float32)


def coefficients(table_ref):
    return lambda d, u, v: table_ref[(d * NV + u) * NV + v]


def meta_of(table_ref):
    first = 3 * NV * NV
    return [table_ref[first + n] for n in range(6)]


def masked(tiles):
    o = place()
    s = lax.axis_index("sub")
    final = lax.axis_size("sub") - 1
    inside = ((o < HALO) & (s != 0)) | ((o >= HALO) & (o < 2 * HALO) & (s != final))
    return [[jnp.where(inside, x, 0.0) for x in tile] for tile in tiles]


def is_even():
    return lax.axis_index("blk") % 2 == 0


def send(ma, mb, at, first, last):
    even = is_even()
    for n, (lo, hi) in enumerate(zip(first, last)):
        ma[at + n] = jnp.where(even, hi, lo)
        if mb is not None:
            mb[at + n] = jnp.where(even, lo, hi)


def at_link(work):
    even = is_even()
    pl.when(even)(lambda: work(True))
    pl.when(jnp.logical_not(even))(lambda: work(False))


def put(ref, at, tiles):
    for n, x in enumerate(tiles):
        ref[at + n] = x


def receive(ga, gb, at, count):
    even = is_even()
    below, above = [], []
    for n in range(at, at + count):
        a, b = ga[n], gb[n]
        below.append(jnp.where(even, b, a))
        above.append(jnp.where(even, a, b))
    return below, above


def send_rows(ma, mb, at, rows):
    send(ma, mb, at, rows[0] + rows[1], rows[-2] + rows[-1])


def receive_rows(ga, gb, at):
    below, above = receive(ga, gb, at, 2 * NV)
    return [below[:NV], below[NV:]], [above[:NV], above[NV:]]


def halo_first(halo):
    low = seg() < 2
    return [jnp.where(low, halo[0][p], rotl(halo[0][p + 1], 64)) for p in range(0, NV, 2)]


def halo_last(halo):
    low = seg() < 2
    return [jnp.where(low, rotl(halo[1][p + 1], 64), halo[1][p]) for p in range(0, NV, 2)]


def send_halo(ma, at, halo):
    send(ma, None, at, halo_first(halo), halo_last(halo))


def receive_halo(ga, gb, at):
    below, above = receive(ga, gb, at, NV // 2)

    def spread(tiles):
        return [y for x in tiles for y in (x, rotl(x, 64))]

    return spread(below), spread(above)


def joined(first, second):
    j_even, k_even = iota_j() % 2 == 0, iota_k() % 2 == 0
    out = []
    for v in range(NV):
        x, y = (jnp.where(j_even, first[r][v], second[r][v]) for r in range(2))
        out.append(jnp.where(k_even, x, y))
    return out


def receive_coarse(ga, gb, at):
    j_even, k_even = iota_j() % 2 == 0, iota_k() % 2 == 0
    fields = ([], [])
    for tiles in receive(ga, gb, at, NV):
        rows = ([], [])
        for x in tiles:
            rows[0].append(jnp.where(k_even, x, rotl(x, 1)))
            rows[1].append(jnp.where(k_even, rotl(x, -1), x))
        fields[0].append([[jnp.where(j_even, x, rots(x, 1)) for x in row] for row in rows])
        fields[1].append([[jnp.where(j_even, rots(x, -1), x) for x in row] for row in rows])
    return fields


def prime_kernel(out_ref):
    out_ref[...] = jnp.zeros_like(out_ref)


def pack_kernel(prime_ref, q_ref, dt_ref, ends_ref, ma, mb, to_left, to_right):
    rows = load(q_ref, 0, NI)
    ends = pack_ends(rows)
    store_tiles(ends_ref, ends)
    r, lower = seg(), place() < HALO
    tiles = ends[0] + ends[1]
    for g in range(2):
        acc = rotl(dt_ref[4 * g], HALO)
        for p in range(1, 4):
            acc = jnp.where(r == p, rotl(dt_ref[4 * g + p], HALO + p * SEG), acc)
        tiles.append(acc)
    for n in range(NV + 1):
        x, y = tiles[2 * n], tiles[2 * n + 1]
        to_right[n] = jnp.where(lower, x, rotl(y, HALO))
        to_left[n] = jnp.where(lower, rotl(y, -HALO), x)
    send_rows(ma, mb, 0, rows)


def unpack(from_right, from_left):
    lower = place() < HALO
    tiles = []
    for n in range(NV + 1):
        x, y = from_left[n], from_right[n]
        tiles.append(jnp.where(lower, x, y))
        tiles.append(jnp.where(lower, rotl(x, -HALO), rotl(y, HALO)))
    halo = masked([tiles[:NV], tiles[NV : 2 * NV]])
    return halo, tiles[2 * NV :]


def advance(start, dt, twice, factor):
    return [[start[i][v] - (0.5 * factor * dt[i]) * twice[i][v] for v in range(NV)] for i in range(len(start))]


def link_rows(rows, below, above, meta, count, lower):
    if lower:
        return low_ghosts(rows, below, above, meta) + rows[: count + 2]
    return rows[-count - 2 :] + high_ghosts(rows, below, above, meta)


def at_end(rows, count, lower):
    return rows[:count] if lower else rows[-count:]


def first_link_kernel(table_ref, q_ref, dt_ref, ga, gb, from_right, from_left, h0_ref, dth_ref, mb):
    a, meta = coefficients(table_ref), meta_of(table_ref)
    h0, dth = unpack(from_right, from_left)
    store_tiles(h0_ref, h0)
    put(dth_ref, 0, dth)

    def work(lower):
        rows = load(q_ref, 0, NI)
        below, above = receive_rows(ga, gb, 0)
        padded = link_rows(rows, below, above, meta, 2, lower)
        twice = residual2(padded, h0, a, 1, 0 if lower else NI - 2)
        dt = at_end([dt_ref[i] for i in range(NI)], 2, lower)
        done = advance(at_end(rows, 2, lower), dt, twice, 0.4)
        put(mb, 0, done[0] + done[1])
        put(mb, 2 * NV, halo_first(h0) if lower else halo_last(h0))

    at_link(work)


def first_kernel(table_ref, q_ref, dt_ref, ga, gb, h0_ref, t1_ref, ma):
    a, meta = coefficients(table_ref), meta_of(table_ref)
    h0 = load_tiles(h0_ref)
    send_halo(ma, 2 * NV, h0)
    t0 = load(q_ref, 0, NI)
    below, above = receive_rows(ga, gb, 0)
    twice = residual2(with_ghosts(t0, below, above, meta), h0, a, 1)
    t1 = advance(t0, [dt_ref[i] for i in range(NI)], twice, 0.4)
    store(t1_ref, 0, t1)
    send_rows(ma, None, 0, t1)


def second_link_kernel(table_ref, q_ref, t1_ref, h0_ref, ends_ref, dt_ref, dth_ref, ga, gb, h1_ref, mb):
    a, meta = coefficients(table_ref), meta_of(table_ref)
    h0 = load_tiles(h0_ref)
    below, above = receive_halo(ga, gb, 2 * NV)
    twice = halo_residual2(h0, halo_ghost(h0, below, above, meta), load_tiles(ends_ref), a)
    h1 = masked(advance(h0, [dth_ref[g] for g in range(2)], twice, 0.4))
    store_tiles(h1_ref, h1)

    def work(lower):
        rows = load(t1_ref, 0, NI)
        below, above = receive_rows(ga, gb, 0)
        padded = link_rows(rows, below, above, meta, 2, lower)
        twice = residual2(padded, h1, a, 1, 0 if lower else NI - 2)
        dt = at_end([dt_ref[i] for i in range(NI)], 2, lower)
        done = advance(at_end(load(q_ref, 0, NI), 2, lower), dt, twice, 1.0)
        put(mb, 0, done[0] + done[1])
        put(mb, 2 * NV, halo_first(h1) if lower else halo_last(h1))

    at_link(work)


def second_kernel(table_ref, q_ref, t1_ref, h1_ref, dt_ref, ga, gb, t2_ref, ma):
    a, meta = coefficients(table_ref), meta_of(table_ref)
    h1 = load_tiles(h1_ref)
    send_halo(ma, 2 * NV, h1)
    t0, t1 = load(q_ref, 0, NI), load(t1_ref, 0, NI)
    below, above = receive_rows(ga, gb, 0)
    twice = residual2(with_ghosts(t1, below, above, meta), h1, a, 1)
    t2 = advance(t0, [dt_ref[i] for i in range(NI)], twice, 1.0)
    store(t2_ref, 0, t2)
    send_rows(ma, None, 0, t2)


def first_section(rows, res, dt):
    start, mean = restrict_rows(rows), restrict_rows(res)
    c1 = []
    for c in range(len(start)):
        step = cell_mean(dt[2 * c] + dt[2 * c + 1])
        c1.append([start[c][v] - (0.4 * step) * mean[c][v] for v in range(NV)])
    return start, mean, c1


def third_link_kernel(table_ref, t1_ref, t2_ref, h0_ref, h1_ref, dt_ref, dth_ref, ga, gb, h2_ref, mb):
    a, meta = coefficients(table_ref), meta_of(table_ref)
    h0, h1 = load_tiles(h0_ref), load_tiles(h1_ref)
    below, above = receive_halo(ga, gb, 2 * NV)
    twice = halo_residual2(h1, halo_ghost(h1, below, above, meta), pack_ends(load(t1_ref, 0, NI)), a)
    h2 = masked(advance(h0, [dth_ref[g] for g in range(2)], twice, 1.0))
    store_tiles(h2_ref, h2)

    def work(lower):
        rows = load(t2_ref, 0, NI)
        below, above = receive_rows(ga, gb, 0)
        padded = link_rows(rows, below, above, meta, 4, lower)
        twice = residual2(padded, h2, a, 1, 0 if lower else NI - 4)
        res = [[0.5 * x for x in row] for row in twice]
        dt = at_end([dt_ref[i] for i in range(NI)], 4, lower)
        start, _, c1 = first_section(at_end(rows, 4, lower), res, dt)
        put(mb, 0, joined(c1, start))
        put(mb, NV, halo_first(h2) if lower else halo_last(h2))

    at_link(work)


def third_kernel(table_ref, t2_ref, h2_ref, dt_ref, ga, gb, res_ref, c1_ref, mean_ref, ma):
    a, meta = coefficients(table_ref), meta_of(table_ref)
    h2, t2 = load_tiles(h2_ref), load(t2_ref, 0, NI)
    send_halo(ma, NV, h2)
    below, above = receive_rows(ga, gb, 0)
    twice = residual2(with_ghosts(t2, below, above, meta), h2, a, 1)
    res = [[0.5 * x for x in row] for row in twice]
    store(res_ref, 0, res)
    start, mean, c1 = first_section(t2, res, [dt_ref[i] for i in range(NI)])
    store(mean_ref, 0, mean)
    store(c1_ref, 0, c1)
    send(ma, None, 0, joined(c1[:2], start[:2]), joined(c1[2:], start[2:]))


def fourth_kernel(table_ref, t2_ref, h2_ref, c1_ref, mean_ref, dt_ref, dth_ref, res_ref, ga, gb, out_hbm, res_hbm, out_ref, sems):
    a, meta = coefficients(table_ref), meta_of(table_ref)
    half = NI // 2
    copies = [pltpu.make_async_copy(res_ref, res_hbm, sems.at[half])]
    copies[0].start()
    h2, t2 = load_tiles(h2_ref), load(t2_ref, 0, NI)
    below, above = receive_halo(ga, gb, NV)
    twice = halo_residual2(h2, halo_ghost(h2, below, above, meta), pack_ends(t2), a)
    means = halo_means(h2[0] + h2[1] + [dth_ref[0], dth_ref[1]] + twice[0] + twice[1])
    start_h, step_h, mean_h = means[: 2 * NV], means[2 * NV : 2 * NV + 2], means[2 * NV + 2 :]
    c1_h = [start_h[t] - (0.2 * step_h[t // NV]) * mean_h[t] for t in range(2 * NV)]
    start_h = [start_h[:NV], start_h[NV:]]
    c1_h = masked([c1_h[:NV], c1_h[NV:]])
    start, c1 = restrict_rows(t2), load(c1_ref, 0, half)
    (below1, above1), (below0, above0) = receive_coarse(ga, gb, 0)
    twice0 = residual2(with_ghosts(start, below0, above0, meta), start_h, a, 2)
    twice1 = residual2(with_ghosts(c1, below1, above1, meta), c1_h, a, 2)
    for c in range(half):
        step = cell_mean(dt_ref[2 * c] + dt_ref[2 * c + 1])
        for v in range(NV):
            change = -step * (0.5 * (twice1[c][v] - twice0[c][v]) + mean_ref[v, c])
            out_ref[v, 2 * c] = t2[2 * c][v] + change
            out_ref[v, 2 * c + 1] = t2[2 * c + 1][v] + change
    for c in range(half):
        rows = pl.ds(2 * c, 2)
        copies.append(pltpu.make_async_copy(out_ref.at[:, rows], out_hbm.at[:, rows], sems.at[c]))
        copies[-1].start()
    for copy in copies:
        copy.wait()


def field(rows):
    return (NV, rows, 8, 128)


def tiles_of(*count):
    return (*count, 8, 128)


def call(kernel, arrays, outs, scalars=(), out_space=pltpu.VMEM, scratch=()):
    smem, vmem = pl.BlockSpec(memory_space=pltpu.SMEM), pl.BlockSpec(memory_space=pltpu.VMEM)
    return pl.pallas_call(
        kernel,
        out_shape=[jax.ShapeDtypeStruct(shape, jnp.float32) for shape in outs],
        in_specs=[smem] * len(scalars) + [vmem] * len(arrays),
        out_specs=[pl.BlockSpec(memory_space=out_space)] * len(outs),
        scratch_shapes=scratch,
        compiler_params=pltpu.CompilerParams(vmem_limit_bytes=VMEM_LIMIT),
    )(*scalars, *arrays)


def cycle(flow_state, timestep, coupling, face_type, face_rot):
    blocks, parts = lax.axis_size("blk"), lax.axis_size("sub")
    chip = [(b, b ^ 1) for b in range(blocks)]
    link = [(b, (b + 1) % blocks if b % 2 else (b - 1) % blocks) for b in range(blocks)]
    ahead = [(s, s + 1) for s in range(parts - 1)]
    back = [(s + 1, s) for s in range(parts - 1)]
    pair = tiles_of(2, NV)

    def exchange(ma, mb):
        gb = lax.ppermute(mb, "blk", link)
        ga = lax.ppermute(ma, "blk", chip)
        return ga, gb

    (table,) = call(table_kernel, (), (tiles_of(3 * NV * NV + 6),), (coupling, face_type, face_rot))
    (prime,) = call(prime_kernel, (), (tiles_of(114),))
    ends, ma, mb, to_left, to_right = call(
        pack_kernel,
        (prime, flow_state, timestep),
        (pair, tiles_of(2 * NV), tiles_of(2 * NV), tiles_of(NV + 1), tiles_of(NV + 1)),
    )
    ga, gb = exchange(ma, mb)
    from_right = lax.ppermute(to_left, "sub", back)
    from_left = lax.ppermute(to_right, "sub", ahead)

    message = tiles_of(2 * NV + NV // 2)
    h0, dth, mb = call(
        first_link_kernel,
        (table, flow_state, timestep, ga, gb, from_right, from_left),
        (pair, tiles_of(2), message),
    )
    t1, ma = call(first_kernel, (table, flow_state, timestep, ga, gb, h0), (field(NI), message))
    ga, gb = exchange(ma, mb)

    h1, mb = call(
        second_link_kernel, (table, flow_state, t1, h0, ends, timestep, dth, ga, gb), (pair, message)
    )
    t2, ma = call(second_kernel, (table, flow_state, t1, h1, timestep, ga, gb), (field(NI), message))
    ga, gb = exchange(ma, mb)

    message = tiles_of(NV + NV // 2)
    h2, mb = call(third_link_kernel, (table, t1, t2, h0, h1, timestep, dth, ga, gb), (pair, message))
    res, c1, mean, ma = call(
        third_kernel,
        (table, t2, h2, timestep, ga, gb),
        (field(NI), field(NI // 2), field(NI // 2), message),
    )
    ga, gb = exchange(ma, mb)

    updated, res = call(
        fourth_kernel,
        (table, t2, h2, c1, mean, timestep, dth, res, ga, gb),
        (field(NI), field(NI)),
        out_space=pltpu.HBM,
        scratch=(pltpu.VMEM(field(NI), jnp.float32), pltpu.SemaphoreType.DMA((NI // 2 + 1,))),
    )
    return (updated, res)


def solution(mesh):
    return jax.shard_map(
        cycle,
        mesh=mesh,
        in_specs=(
            P(None, "blk", None, "sub"),
            P("blk", None, "sub"),
            P(),
            P("blk", None),
            P("blk", None),
        ),
        out_specs=(P(None, "blk", None, "sub"), P(None, "blk", None, "sub")),
        check_vma=False,
    )
```

```python
import jax
import jax.numpy as jnp
from jax import lax
from jax.experimental import pallas as pl
from jax.experimental.pallas import tpu as pltpu
from jax.sharding import PartitionSpec as P


NV = 6
NI = 8
HALO = 10
SEG = 32
VMEM_LIMIT = 12 * 1024 * 1024

C0, C1, C2 = 0.44, -0.26, 0.04


def iota_j():
    return lax.broadcasted_iota(jnp.int32, (8, 128), 0)


def iota_k():
    return lax.broadcasted_iota(jnp.int32, (8, 128), 1)


def rotl(x, shift):
    return pltpu.roll(x, shift % 128, 1)


def rots(x, shift):
    return pltpu.roll(x, shift % 8, 0)


def reverse_j(x):
    j = iota_j()
    x = rots(x, 4)
    x = jnp.where((j // 2) % 2 == 0, rots(x, -2), rots(x, 2))
    return jnp.where(j % 2 == 0, rots(x, -1), rots(x, 1))


def ghost_rows(own2, prev2, next2, kind, flip, turn):
    nearest = []
    for r in range(2):
        picked = []
        for v in range(NV):
            wall = -own2[r][v] if v == 1 else own2[r][v]
            x = jnp.where(kind == 2, wall, 0.0)
            x = jnp.where(kind == 1, next2[r][v], x)
            x = jnp.where(kind == 0, prev2[r][v], x)
            picked.append(jnp.where(flip == 1, reverse_j(x), x))
        a, b = picked[2], picked[3]
        picked[2], picked[3] = jnp.where(turn == 1, -b, a), jnp.where(turn == 1, a, b)
        nearest.append(picked)
    return nearest


def low_ghosts(rows, below, above, meta):
    lo = ghost_rows([rows[0], rows[1]], [below[1], below[0]], [above[0], above[1]], *meta[:3])
    return [lo[1], lo[0]]


def high_ghosts(rows, below, above, meta):
    return ghost_rows([rows[-1], rows[-2]], [above[0], above[1]], [below[1], below[0]], *meta[3:])


def with_ghosts(rows, below, above, meta):
    return low_ghosts(rows, below, above, meta) + rows + high_ghosts(rows, below, above, meta)


def flux(q, a, d):
    half = 0.5 * q[1 + d]
    out = []
    for u in range(NV):
        acc = (a(d, u, u) + half) * q[u]
        for v in range(NV):
            if v != u:
                acc = acc + a(d, u, v) * q[v]
        out.append(acc)
    return out


def flux_j(q, a):
    out, mirrored = [], []
    for u in range(NV):
        even = None
        for v in range(NV):
            if v != 2:
                term = a(1, u, v) * q[v]
                even = term if even is None else even + term
        if u == 2:
            even = even + 0.5 * (q[2] * q[2])
            odd = a(1, 2, 2) * q[2]
        else:
            odd = q[2] * (a(1, u, 2) + 0.5 * q[u])
        out.append(even + odd)
        mirrored.append(even - odd)
    return out, mirrored


def j_weights(unit):
    j = iota_j() // unit
    n = 8 // unit
    out = []
    for sign in (1.0, -1.0):
        end = (j == 0) | (j == n - 1)
        centre = jnp.where(end, C0 + sign * C1, C0) + 2 * C0
        near = C1 + sign * C2
        below = jnp.where(j == 0, 0.0, jnp.where((j == 1) | (j == n - 1), near, C1))
        above = jnp.where(j == n - 1, 0.0, jnp.where((j == 0) | (j == n - 2), near, C1))
        if n == 4:
            two = None
        else:
            two = (jnp.where(j >= 2, C2, 0.0), jnp.where(j <= n - 3, C2, 0.0))
        out.append((centre, below, above, two))
    return out


def seg():
    return iota_k() // SEG


def place():
    return iota_k() % SEG


def second_index(fj, gj, q, u, unit, weights, ends):
    centre, below, above, two = weights[1 if u == 2 else 0]
    x = q[u]
    acc = centre * x + below * rots(x, unit) + above * rots(x, -unit)
    if two is None:
        acc = acc + C2 * rots(x, 4)
    else:
        acc = acc + two[0] * rots(x, 2) + two[1] * rots(x, -2)
    up = jnp.where(ends[1], gj[u], rots(fj[u], -unit))
    down = jnp.where(ends[0], gj[u], rots(fj[u], unit))
    return acc + (up - down)


def residual2(padded, halo, a, unit, start=0):
    n = len(padded) - 4
    k, j = iota_k(), iota_j()
    weights = j_weights(unit)
    ends = (j < unit, j >= 8 - unit)
    low1, low2 = k < unit, k < 2 * unit
    high1, high2 = k >= 128 - unit, k >= 128 - 2 * unit
    upper = place() >= HALO
    edge = []
    for tile in halo or ():
        f = flux(tile, a, 2)
        edge.append([jnp.where(upper, f[u] + C1 * tile[u], f[u] - C1 * tile[u]) for u in range(NV)])
    beside = []
    for i in range(n if halo else 0):
        g, first = unit * (start + i) // 4, unit * (start + i) % 4 * SEG + HALO
        beside.append([(rotl(halo[g][u], -first), rotl(edge[g][u], -first)) for u in range(NV)])
    fi = {m: flux(padded[m], a, 0) for m in range(1, n + 3)}
    result = []
    for i in range(n):
        m = i + 2
        q = padded[m]
        fj, gj = flux_j(q, a)
        fk = flux(q, a, 2)
        row = []
        for u in range(NV):
            x = q[u]
            s, e = beside[i][u] if halo else (0.0, 0.0)
            acc = second_index(fj, gj, q, u, unit, weights, ends)
            acc = acc + (fi[m + 1][u] - fi[m - 1][u])
            acc = acc + C1 * (padded[m + 1][u] + padded[m - 1][u]) + C2 * (padded[m + 2][u] + padded[m - 2][u])
            t = C1 * x
            acc = acc + rotl(jnp.where(low1, e, fk[u] + t), -unit)
            acc = acc - rotl(jnp.where(high1, e, fk[u] - t), unit)
            acc = acc + C2 * (rotl(jnp.where(low2, s, x), -2 * unit) + rotl(jnp.where(high2, s, x), 2 * unit))
            row.append(acc)
        result.append(row)
    return result


def halo_residual2(halo, ghost, own, a):
    r, o = seg(), place()
    j = iota_j()
    weights = j_weights(1)
    ends = (j < 1, j >= 7)
    first, last, low, high = r == 0, r == 3, r < 2, r >= 2
    tiles = [halo[0], halo[1], ghost]
    up_i, down_i = [], []
    for t in tiles:
        f = flux(t, a, 0)
        up_i.append([f[u] + C1 * t[u] for u in range(NV)])
        down_i.append([f[u] - C1 * t[u] for u in range(NV)])
    upper = o >= HALO
    after1, after2 = o == HALO, (o == HALO) | (o == HALO + 1)
    before1, before2 = o == HALO - 1, (o == HALO - 1) | (o == HALO - 2)
    result = []
    for g in range(2):
        q, nxt, prv = tiles[g], (g + 1) % 3, (g + 2) % 3
        fj, gj = flux_j(q, a)
        fk = flux(q, a, 2)
        fo = flux(own[g], a, 2)
        row = []
        for u in range(NV):
            x, y = q[u], own[g][u]
            acc = second_index(fj, gj, q, u, 1, weights, ends)
            acc = acc + rotl(jnp.where(first, up_i[nxt][u], up_i[g][u]), -SEG)
            acc = acc - rotl(jnp.where(last, down_i[prv][u], down_i[g][u]), SEG)
            acc = acc + C2 * rotl(jnp.where(low, tiles[nxt][u], x) + jnp.where(high, tiles[prv][u], x), 2 * SEG)
            t = C1 * x
            e = jnp.where(upper, fo[u] + C1 * y, fo[u] - C1 * y)
            acc = acc + rotl(jnp.where(after1, e, fk[u] + t), -1)
            acc = acc - rotl(jnp.where(before1, e, fk[u] - t), 1)
            acc = acc + C2 * (rotl(jnp.where(after2, y, x), -2) + rotl(jnp.where(before2, y, x), 2))
            row.append(acc)
        result.append(row)
    return result


def pack_ends(rows):
    r = seg()
    out = []
    for g in range(2):
        tile = []
        for v in range(NV):
            acc = rotl(rows[4 * g][v], HALO)
            for p in range(1, 4):
                acc = jnp.where(r == p, rotl(rows[4 * g + p][v], HALO + p * SEG), acc)
            tile.append(acc)
        out.append(tile)
    return out


def halo_ghost(halo, below, above, meta):
    t_lo, flip_lo, turn_lo, t_hi, flip_hi, turn_hi = meta
    r = seg()
    high_side = r < 2
    even_part = r % 2 == 0

    def turned(x):
        return jnp.where(even_part, rotl(x, SEG), rotl(x, -SEG))

    flip = jnp.where(high_side, flip_hi, flip_lo)
    picked = []
    for v in range(NV):
        wall_lo, wall_hi = turned(halo[0][v]), turned(halo[1][v])
        if v == 1:
            wall_lo, wall_hi = -wall_lo, -wall_hi
        hi = jnp.where(t_hi == 2, wall_hi, 0.0)
        hi = jnp.where(t_hi == 1, turned(below[v]), hi)
        hi = jnp.where(t_hi == 0, above[v], hi)
        lo = jnp.where(t_lo == 2, wall_lo, 0.0)
        lo = jnp.where(t_lo == 1, turned(above[v]), lo)
        lo = jnp.where(t_lo == 0, below[v], lo)
        x = jnp.where(high_side, hi, lo)
        picked.append(jnp.where(flip == 1, reverse_j(x), x))
    turn = jnp.where(high_side, turn_hi, turn_lo) == 1
    b, c = picked[2], picked[3]
    picked[2], picked[3] = jnp.where(turn, -c, b), jnp.where(turn, b, c)
    return picked


def cell_mean(x):
    x = x + jnp.where(iota_j() % 2 == 0, rots(x, -1), rots(x, 1))
    x = x + jnp.where(iota_k() % 2 == 0, rotl(x, -1), rotl(x, 1))
    return 0.125 * x


def restrict_rows(rows):
    return [[cell_mean(rows[2 * c][v] + rows[2 * c + 1][v]) for v in range(len(rows[0]))] for c in range(len(rows) // 2)]


def halo_means(tiles):
    even = seg() % 2 == 0
    tiles = [x + jnp.where(even, rotl(x, -SEG), rotl(x, SEG)) for x in tiles]
    return [cell_mean(x) for x in tiles]


def load(ref, first, count):
    return [[ref[v, first + r] for v in range(NV)] for r in range(count)]


def store(ref, first, rows):
    for r, row in enumerate(rows):
        for v in range(NV):
            ref[v, first + r] = row[v]


def load_tiles(ref):
    return [[ref[g, v] for v in range(NV)] for g in range(2)]


def store_tiles(ref, tiles):
    for g in range(2):
        for v in range(NV):
            ref[g, v] = tiles[g][v]


def table_kernel(a_ref, type_ref, rot_ref, table_ref):
    values = [a_ref[d, u, v] for d in range(3) for u in range(NV) for v in range(NV)]
    for face in range(2):
        kind, rot = type_ref[0, face], rot_ref[0, face]
        values += [kind.astype(jnp.float32), (rot % 2).astype(jnp.float32), (rot // 2 % 2).astype(jnp.float32)]
    for n, value in enumerate(values):
        table_ref[n] = jnp.full((8, 128), value, jnp.float32)


def coefficients(table_ref):
    return lambda d, u, v: table_ref[(d * NV + u) * NV + v]


def meta_of(table_ref):
    first = 3 * NV * NV
    return [table_ref[first + n] for n in range(6)]


def masked(tiles):
    o = place()
    s = lax.axis_index("sub")
    final = lax.axis_size("sub") - 1
    inside = ((o < HALO) & (s != 0)) | ((o >= HALO) & (o < 2 * HALO) & (s != final))
    return [[jnp.where(inside, x, 0.0) for x in tile] for tile in tiles]


def is_even():
    return lax.axis_index("blk") % 2 == 0


def send(ma, mb, at, first, last):
    even = is_even()
    for n, (lo, hi) in enumerate(zip(first, last)):
        ma[at + n] = jnp.where(even, hi, lo)
        if mb is not None:
            mb[at + n] = jnp.where(even, lo, hi)


def at_link(work):
    even = is_even()
    pl.when(even)(lambda: work(True))
    pl.when(jnp.logical_not(even))(lambda: work(False))


def put(ref, at, tiles):
    for n, x in enumerate(tiles):
        ref[at + n] = x


def receive(ga, gb, at, count):
    even = is_even()
    below, above = [], []
    for n in range(at, at + count):
        a, b = ga[n], gb[n]
        below.append(jnp.where(even, b, a))
        above.append(jnp.where(even, a, b))
    return below, above


def send_rows(ma, mb, at, rows):
    send(ma, mb, at, rows[0] + rows[1], rows[-2] + rows[-1])


def receive_rows(ga, gb, at):
    below, above = receive(ga, gb, at, 2 * NV)
    return [below[:NV], below[NV:]], [above[:NV], above[NV:]]


def halo_first(halo):
    low = seg() < 2
    return [jnp.where(low, halo[0][p], rotl(halo[0][p + 1], 64)) for p in range(0, NV, 2)]


def halo_last(halo):
    low = seg() < 2
    return [jnp.where(low, rotl(halo[1][p + 1], 64), halo[1][p]) for p in range(0, NV, 2)]


def send_halo(ma, at, halo):
    send(ma, None, at, halo_first(halo), halo_last(halo))


def receive_halo(ga, gb, at):
    below, above = receive(ga, gb, at, NV // 2)

    def spread(tiles):
        return [y for x in tiles for y in (x, rotl(x, 64))]

    return spread(below), spread(above)


def joined(first, second):
    j_even, k_even = iota_j() % 2 == 0, iota_k() % 2 == 0
    out = []
    for v in range(NV):
        x, y = (jnp.where(j_even, first[r][v], second[r][v]) for r in range(2))
        out.append(jnp.where(k_even, x, y))
    return out


def receive_coarse(ga, gb, at):
    j_even, k_even = iota_j() % 2 == 0, iota_k() % 2 == 0
    fields = ([], [])
    for tiles in receive(ga, gb, at, NV):
        rows = ([], [])
        for x in tiles:
            rows[0].append(jnp.where(k_even, x, rotl(x, 1)))
            rows[1].append(jnp.where(k_even, rotl(x, -1), x))
        fields[0].append([[jnp.where(j_even, x, rots(x, 1)) for x in row] for row in rows])
        fields[1].append([[jnp.where(j_even, rots(x, -1), x) for x in row] for row in rows])
    return fields


def prime_kernel(out_ref):
    out_ref[...] = jnp.zeros_like(out_ref)


def pack_kernel(prime_ref, q_ref, dt_ref, ends_ref, ma, mb, to_left, to_right):
    rows = load(q_ref, 0, NI)
    ends = pack_ends(rows)
    store_tiles(ends_ref, ends)
    r, lower = seg(), place() < HALO
    tiles = ends[0] + ends[1]
    for g in range(2):
        acc = rotl(dt_ref[4 * g], HALO)
        for p in range(1, 4):
            acc = jnp.where(r == p, rotl(dt_ref[4 * g + p], HALO + p * SEG), acc)
        tiles.append(acc)
    for n in range(NV + 1):
        x, y = tiles[2 * n], tiles[2 * n + 1]
        to_right[n] = jnp.where(lower, x, rotl(y, HALO))
        to_left[n] = jnp.where(lower, rotl(y, -HALO), x)
    send_rows(ma, mb, 0, rows)


def unpack(from_right, from_left):
    lower = place() < HALO
    tiles = []
    for n in range(NV + 1):
        x, y = from_left[n], from_right[n]
        tiles.append(jnp.where(lower, x, y))
        tiles.append(jnp.where(lower, rotl(x, -HALO), rotl(y, HALO)))
    halo = masked([tiles[:NV], tiles[NV : 2 * NV]])
    return halo, tiles[2 * NV :]


def advance(start, dt, twice, factor):
    return [[start[i][v] - (0.5 * factor * dt[i]) * twice[i][v] for v in range(NV)] for i in range(len(start))]


def link_rows(rows, below, above, meta, count, lower):
    if lower:
        return low_ghosts(rows, below, above, meta) + rows[: count + 2]
    return rows[-count - 2 :] + high_ghosts(rows, below, above, meta)


def at_end(rows, count, lower):
    return rows[:count] if lower else rows[-count:]


def first_ends_kernel(table_ref, q_ref, dt_ref, ga, gb, from_right, from_left, h0_ref, dth_ref, ma, mb):
    a, meta = coefficients(table_ref), meta_of(table_ref)
    h0, dth = unpack(from_right, from_left)
    store_tiles(h0_ref, h0)
    put(dth_ref, 0, dth)
    send(ma, mb, 2 * NV, halo_first(h0), halo_last(h0))
    rows = load(q_ref, 0, NI)
    below, above = receive_rows(ga, gb, 0)
    ends = []
    for lower in (True, False):
        padded = link_rows(rows, below, above, meta, 2, lower)
        twice = residual2(padded, h0, a, 1, 0 if lower else NI - 2)
        dt = at_end([dt_ref[i] for i in range(NI)], 2, lower)
        ends += advance(at_end(rows, 2, lower), dt, twice, 0.4)
    send_rows(ma, mb, 0, ends)


def first_kernel(table_ref, q_ref, dt_ref, ga, gb, h0_ref, t1_ref):
    a, meta = coefficients(table_ref), meta_of(table_ref)
    t0 = load(q_ref, 0, NI)
    below, above = receive_rows(ga, gb, 0)
    twice = residual2(with_ghosts(t0, below, above, meta), load_tiles(h0_ref), a, 1)
    store(t1_ref, 0, advance(t0, [dt_ref[i] for i in range(NI)], twice, 0.4))


def second_link_kernel(table_ref, q_ref, t1_ref, h0_ref, ends_ref, dt_ref, dth_ref, ga, gb, h1_ref, mb):
    a, meta = coefficients(table_ref), meta_of(table_ref)
    h0 = load_tiles(h0_ref)
    below, above = receive_halo(ga, gb, 2 * NV)
    twice = halo_residual2(h0, halo_ghost(h0, below, above, meta), load_tiles(ends_ref), a)
    h1 = masked(advance(h0, [dth_ref[g] for g in range(2)], twice, 0.4))
    store_tiles(h1_ref, h1)

    def work(lower):
        rows = load(t1_ref, 0, NI)
        below, above = receive_rows(ga, gb, 0)
        padded = link_rows(rows, below, above, meta, 2, lower)
        twice = residual2(padded, h1, a, 1, 0 if lower else NI - 2)
        dt = at_end([dt_ref[i] for i in range(NI)], 2, lower)
        done = advance(at_end(load(q_ref, 0, NI), 2, lower), dt, twice, 1.0)
        put(mb, 0, done[0] + done[1])
        put(mb, 2 * NV, halo_first(h1) if lower else halo_last(h1))

    at_link(work)


def second_kernel(table_ref, q_ref, t1_ref, h1_ref, dt_ref, ga, gb, t2_ref, ma):
    a, meta = coefficients(table_ref), meta_of(table_ref)
    h1 = load_tiles(h1_ref)
    send_halo(ma, 2 * NV, h1)
    t0, t1 = load(q_ref, 0, NI), load(t1_ref, 0, NI)
    below, above = receive_rows(ga, gb, 0)
    twice = residual2(with_ghosts(t1, below, above, meta), h1, a, 1)
    t2 = advance(t0, [dt_ref[i] for i in range(NI)], twice, 1.0)
    store(t2_ref, 0, t2)
    send_rows(ma, None, 0, t2)


def first_section(rows, res, dt):
    start, mean = restrict_rows(rows), restrict_rows(res)
    c1 = []
    for c in range(len(start)):
        step = cell_mean(dt[2 * c] + dt[2 * c + 1])
        c1.append([start[c][v] - (0.4 * step) * mean[c][v] for v in range(NV)])
    return start, mean, c1


def third_link_kernel(table_ref, t1_ref, t2_ref, h0_ref, h1_ref, dt_ref, dth_ref, ga, gb, h2_ref, mb):
    a, meta = coefficients(table_ref), meta_of(table_ref)
    h0, h1 = load_tiles(h0_ref), load_tiles(h1_ref)
    below, above = receive_halo(ga, gb, 2 * NV)
    twice = halo_residual2(h1, halo_ghost(h1, below, above, meta), pack_ends(load(t1_ref, 0, NI)), a)
    h2 = masked(advance(h0, [dth_ref[g] for g in range(2)], twice, 1.0))
    store_tiles(h2_ref, h2)

    def work(lower):
        rows = load(t2_ref, 0, NI)
        below, above = receive_rows(ga, gb, 0)
        padded = link_rows(rows, below, above, meta, 4, lower)
        twice = residual2(padded, h2, a, 1, 0 if lower else NI - 4)
        res = [[0.5 * x for x in row] for row in twice]
        dt = at_end([dt_ref[i] for i in range(NI)], 4, lower)
        start, _, c1 = first_section(at_end(rows, 4, lower), res, dt)
        put(mb, 0, joined(c1, start))
        put(mb, NV, halo_first(h2) if lower else halo_last(h2))

    at_link(work)


def third_kernel(table_ref, t2_ref, h2_ref, dt_ref, ga, gb, res_ref, start_ref, c1_ref, mean_ref, ma):
    a, meta = coefficients(table_ref), meta_of(table_ref)
    h2, t2 = load_tiles(h2_ref), load(t2_ref, 0, NI)
    send_halo(ma, NV, h2)
    below, above = receive_rows(ga, gb, 0)
    twice = residual2(with_ghosts(t2, below, above, meta), h2, a, 1)
    res = [[0.5 * x for x in row] for row in twice]
    store(res_ref, 0, res)
    start, mean, c1 = first_section(t2, res, [dt_ref[i] for i in range(NI)])
    store(start_ref, 0, start)
    store(mean_ref, 0, mean)
    store(c1_ref, 0, c1)
    send(ma, None, 0, joined(c1[:2], start[:2]), joined(c1[2:], start[2:]))


def early_kernel(table_ref, start_ref, c1_ref, h2_ref, part_ref):
    a = coefficients(table_ref)
    half = NI // 2
    h2 = load_tiles(h2_ref)
    start_h = halo_means(h2[0] + h2[1])
    ghost = [[jnp.zeros((8, 128), jnp.float32)] * NV] * 2
    twice0 = residual2(ghost + load(start_ref, 0, half) + ghost, [start_h[:NV], start_h[NV:]], a, 2)
    twice1 = residual2(ghost + load(c1_ref, 0, half) + ghost, None, a, 2)
    store(part_ref, 0, [[twice1[c][v] - twice0[c][v] for v in range(NV)] for c in range(half)])


def halo_part(halo, a):
    o, k = place(), iota_k()
    high1, low1 = (o == HALO - 2) | (o == HALO - 1), (o == HALO) | (o == HALO + 1)
    high2, low2 = (o >= HALO - 4) & (o < HALO), (o >= HALO) & (o < HALO + 4)
    spread = []
    for tile in halo:
        f = flux(tile, a, 2)
        row = []
        for u in range(NV):
            x = tile[u]
            w = jnp.where(high1, rotl(f[u] + C1 * x, -2), 0.0) - jnp.where(low1, rotl(f[u] - C1 * x, 2), 0.0)
            row.append(w + C2 * (jnp.where(high2, rotl(x, -4), 0.0) + jnp.where(low2, rotl(x, 4), 0.0)))
        spread.append(row)
    near = (k < 4) | (k >= 124)
    out = []
    for c in range(NI // 2):
        g, first = 2 * c // 4, 2 * c % 4 * SEG + HALO
        out.append([jnp.where(near, rotl(spread[g][u], -first), 0.0) for u in range(NV)])
    return out


def ghost_part(low, high, a):
    fl, fh = flux(low[1], a, 0), flux(high[0], a, 0)
    rows = ([], [], [], [])
    for u in range(NV):
        rows[0].append(C1 * low[1][u] + C2 * low[0][u] - fl[u])
        rows[1].append(C2 * low[1][u])
        rows[2].append(C2 * high[0][u])
        rows[3].append(C1 * high[0][u] + C2 * high[1][u] + fh[u])
    return rows


def fourth_kernel(
    table_ref, t2_ref, h2_ref, start_ref, c1_ref, mean_ref, part_ref, dt_ref, dth_ref, res_ref, ga, gb, out_hbm, res_hbm, out_ref, sems
):
    a, meta = coefficients(table_ref), meta_of(table_ref)
    half = NI // 2
    copies = [pltpu.make_async_copy(res_ref, res_hbm, sems.at[half])]
    copies[0].start()
    h2, t2 = load_tiles(h2_ref), load(t2_ref, 0, NI)
    below, above = receive_halo(ga, gb, NV)
    twice = halo_residual2(h2, halo_ghost(h2, below, above, meta), pack_ends(t2), a)
    means = halo_means(h2[0] + h2[1] + [dth_ref[0], dth_ref[1]] + twice[0] + twice[1])
    start_h, step_h, mean_h = means[: 2 * NV], means[2 * NV : 2 * NV + 2], means[2 * NV + 2 :]
    c1_h = [start_h[t] - (0.2 * step_h[t // NV]) * mean_h[t] for t in range(2 * NV)]
    halo = halo_part(masked([c1_h[:NV], c1_h[NV:]]), a)
    ghosts = []
    for ref, (below, above) in zip((c1_ref, start_ref), receive_coarse(ga, gb, 0)):
        rows = load(ref, 0, half)
        ghosts.append(ghost_part(low_ghosts(rows, below, above, meta), high_ghosts(rows, below, above, meta), a))
    for c in range(half):
        step = cell_mean(dt_ref[2 * c] + dt_ref[2 * c + 1])
        for v in range(NV):
            twice_change = part_ref[v, c] + (ghosts[0][c][v] - ghosts[1][c][v]) + halo[c][v]
            change = -step * (0.5 * twice_change + mean_ref[v, c])
            out_ref[v, 2 * c] = t2[2 * c][v] + change
            out_ref[v, 2 * c + 1] = t2[2 * c + 1][v] + change
    for c in range(half):
        rows = pl.ds(2 * c, 2)
        copies.append(pltpu.make_async_copy(out_ref.at[:, rows], out_hbm.at[:, rows], sems.at[c]))
        copies[-1].start()
    for copy in copies:
        copy.wait()


def field(rows):
    return (NV, rows, 8, 128)


def tiles_of(*count):
    return (*count, 8, 128)


def call(kernel, arrays, outs, scalars=(), out_space=pltpu.VMEM, scratch=()):
    smem, vmem = pl.BlockSpec(memory_space=pltpu.SMEM), pl.BlockSpec(memory_space=pltpu.VMEM)
    return pl.pallas_call(
        kernel,
        out_shape=[jax.ShapeDtypeStruct(shape, jnp.float32) for shape in outs],
        in_specs=[smem] * len(scalars) + [vmem] * len(arrays),
        out_specs=[pl.BlockSpec(memory_space=out_space)] * len(outs),
        scratch_shapes=scratch,
        compiler_params=pltpu.CompilerParams(vmem_limit_bytes=VMEM_LIMIT),
    )(*scalars, *arrays)


def cycle(flow_state, timestep, coupling, face_type, face_rot):
    blocks, parts = lax.axis_size("blk"), lax.axis_size("sub")
    chip = [(b, b ^ 1) for b in range(blocks)]
    link = [(b, (b + 1) % blocks if b % 2 else (b - 1) % blocks) for b in range(blocks)]
    ahead = [(s, s + 1) for s in range(parts - 1)]
    back = [(s + 1, s) for s in range(parts - 1)]
    pair = tiles_of(2, NV)

    def exchange(ma, mb):
        gb = lax.ppermute(mb, "blk", link)
        ga = lax.ppermute(ma, "blk", chip)
        return ga, gb

    (table,) = call(table_kernel, (), (tiles_of(3 * NV * NV + 6),), (coupling, face_type, face_rot))
    (prime,) = call(prime_kernel, (), (tiles_of(114),))
    ends, ma, mb, to_left, to_right = call(
        pack_kernel,
        (prime, flow_state, timestep),
        (pair, tiles_of(2 * NV), tiles_of(2 * NV), tiles_of(NV + 1), tiles_of(NV + 1)),
    )
    ga, gb = exchange(ma, mb)
    from_right = lax.ppermute(to_left, "sub", back)
    from_left = lax.ppermute(to_right, "sub", ahead)

    message = tiles_of(2 * NV + NV // 2)
    h0, dth, ma, mb = call(
        first_ends_kernel,
        (table, flow_state, timestep, ga, gb, from_right, from_left),
        (pair, tiles_of(2), message, message),
    )
    (t1,) = call(first_kernel, (table, flow_state, timestep, ga, gb, h0), (field(NI),))
    ga, gb = exchange(ma, mb)

    h1, mb = call(
        second_link_kernel, (table, flow_state, t1, h0, ends, timestep, dth, ga, gb), (pair, message)
    )
    t2, ma = call(second_kernel, (table, flow_state, t1, h1, timestep, ga, gb), (field(NI), message))
    ga, gb = exchange(ma, mb)

    message = tiles_of(NV + NV // 2)
    h2, mb = call(third_link_kernel, (table, t1, t2, h0, h1, timestep, dth, ga, gb), (pair, message))
    res, start, c1, mean, ma = call(
        third_kernel,
        (table, t2, h2, timestep, ga, gb),
        (field(NI), field(NI // 2), field(NI // 2), field(NI // 2), message),
    )
    (part,) = call(early_kernel, (table, start, c1, h2), (field(NI // 2),))
    ga, gb = exchange(ma, mb)

    updated, res = call(
        fourth_kernel,
        (table, t2, h2, start, c1, mean, part, timestep, dth, res, ga, gb),
        (field(NI), field(NI)),
        out_space=pltpu.HBM,
        scratch=(pltpu.VMEM(field(NI), jnp.float32), pltpu.SemaphoreType.DMA((NI // 2 + 1,))),
    )
    return (updated, res)


def solution(mesh):
    return jax.shard_map(
        cycle,
        mesh=mesh,
        in_specs=(
            P(None, "blk", None, "sub"),
            P("blk", None, "sub"),
            P(),
            P("blk", None),
            P("blk", None),
        ),
        out_specs=(P(None, "blk", None, "sub"), P(None, "blk", None, "sub")),
        check_vma=False,
    )
```

```python
import jax
import jax.numpy as jnp
from jax import lax
from jax.experimental import pallas as pl
from jax.experimental.pallas import tpu as pltpu
from jax.sharding import PartitionSpec as P


NV = 6
NI = 8
HALO = 10
SEG = 32
VMEM_LIMIT = 12 * 1024 * 1024

C0, C1, C2 = 0.44, -0.26, 0.04


def iota_j():
    return lax.broadcasted_iota(jnp.int32, (8, 128), 0)


def iota_k():
    return lax.broadcasted_iota(jnp.int32, (8, 128), 1)


def rotl(x, shift):
    return pltpu.roll(x, shift % 128, 1)


def rots(x, shift):
    return pltpu.roll(x, shift % 8, 0)


def reverse_j(x):
    j = iota_j()
    x = rots(x, 4)
    x = jnp.where((j // 2) % 2 == 0, rots(x, -2), rots(x, 2))
    return jnp.where(j % 2 == 0, rots(x, -1), rots(x, 1))


def ghost_rows(own2, prev2, next2, kind, flip, turn):
    nearest = []
    for r in range(2):
        picked = []
        for v in range(NV):
            wall = -own2[r][v] if v == 1 else own2[r][v]
            x = jnp.where(kind == 2, wall, 0.0)
            x = jnp.where(kind == 1, next2[r][v], x)
            x = jnp.where(kind == 0, prev2[r][v], x)
            picked.append(jnp.where(flip == 1, reverse_j(x), x))
        a, b = picked[2], picked[3]
        picked[2], picked[3] = jnp.where(turn == 1, -b, a), jnp.where(turn == 1, a, b)
        nearest.append(picked)
    return nearest


def low_ghosts(rows, below, above, meta):
    lo = ghost_rows([rows[0], rows[1]], [below[1], below[0]], [above[0], above[1]], *meta[:3])
    return [lo[1], lo[0]]


def high_ghosts(rows, below, above, meta):
    return ghost_rows([rows[-1], rows[-2]], [above[0], above[1]], [below[1], below[0]], *meta[3:])


def with_ghosts(rows, below, above, meta):
    return low_ghosts(rows, below, above, meta) + rows + high_ghosts(rows, below, above, meta)


def flux(q, a, d):
    half = 0.5 * q[1 + d]
    out = []
    for u in range(NV):
        acc = (a(d, u, u) + half) * q[u]
        for v in range(NV):
            if v != u:
                acc = acc + a(d, u, v) * q[v]
        out.append(acc)
    return out


def flux_j(q, a):
    out, mirrored = [], []
    for u in range(NV):
        even = None
        for v in range(NV):
            if v != 2:
                term = a(1, u, v) * q[v]
                even = term if even is None else even + term
        if u == 2:
            even = even + 0.5 * (q[2] * q[2])
            odd = a(1, 2, 2) * q[2]
        else:
            odd = q[2] * (a(1, u, 2) + 0.5 * q[u])
        out.append(even + odd)
        mirrored.append(even - odd)
    return out, mirrored


def j_weights(unit):
    j = iota_j() // unit
    n = 8 // unit
    out = []
    for sign in (1.0, -1.0):
        end = (j == 0) | (j == n - 1)
        centre = jnp.where(end, C0 + sign * C1, C0) + 2 * C0
        near = C1 + sign * C2
        below = jnp.where(j == 0, 0.0, jnp.where((j == 1) | (j == n - 1), near, C1))
        above = jnp.where(j == n - 1, 0.0, jnp.where((j == 0) | (j == n - 2), near, C1))
        if n == 4:
            two = None
        else:
            two = (jnp.where(j >= 2, C2, 0.0), jnp.where(j <= n - 3, C2, 0.0))
        out.append((centre, below, above, two))
    return out


def seg():
    return iota_k() // SEG


def place():
    return iota_k() % SEG


def second_index(fj, gj, q, u, unit, weights, ends):
    centre, below, above, two = weights[1 if u == 2 else 0]
    x = q[u]
    acc = centre * x + below * rots(x, unit) + above * rots(x, -unit)
    if two is None:
        acc = acc + C2 * rots(x, 4)
    else:
        acc = acc + two[0] * rots(x, 2) + two[1] * rots(x, -2)
    up = jnp.where(ends[1], gj[u], rots(fj[u], -unit))
    down = jnp.where(ends[0], gj[u], rots(fj[u], unit))
    return acc + (up - down)


def residual2(padded, halo, a, unit, start=0):
    n = len(padded) - 4
    k, j = iota_k(), iota_j()
    weights = j_weights(unit)
    ends = (j < unit, j >= 8 - unit)
    low1, low2 = k < unit, k < 2 * unit
    high1, high2 = k >= 128 - unit, k >= 128 - 2 * unit
    upper = place() >= HALO
    edge = []
    for tile in halo or ():
        f = flux(tile, a, 2)
        edge.append([jnp.where(upper, f[u] + C1 * tile[u], f[u] - C1 * tile[u]) for u in range(NV)])
    beside = []
    for i in range(n if halo else 0):
        g, first = unit * (start + i) // 4, unit * (start + i) % 4 * SEG + HALO
        beside.append([(rotl(halo[g][u], -first), rotl(edge[g][u], -first)) for u in range(NV)])
    fi = {m: flux(padded[m], a, 0) for m in range(1, n + 3)}
    result = []
    for i in range(n):
        m = i + 2
        q = padded[m]
        fj, gj = flux_j(q, a)
        fk = flux(q, a, 2)
        row = []
        for u in range(NV):
            x = q[u]
            s, e = beside[i][u] if halo else (0.0, 0.0)
            acc = second_index(fj, gj, q, u, unit, weights, ends)
            acc = acc + (fi[m + 1][u] - fi[m - 1][u])
            acc = acc + C1 * (padded[m + 1][u] + padded[m - 1][u]) + C2 * (padded[m + 2][u] + padded[m - 2][u])
            t = C1 * x
            acc = acc + rotl(jnp.where(low1, e, fk[u] + t), -unit)
            acc = acc - rotl(jnp.where(high1, e, fk[u] - t), unit)
            acc = acc + C2 * (rotl(jnp.where(low2, s, x), -2 * unit) + rotl(jnp.where(high2, s, x), 2 * unit))
            row.append(acc)
        result.append(row)
    return result


def halo_residual2(halo, ghost, own, a):
    r, o = seg(), place()
    j = iota_j()
    weights = j_weights(1)
    ends = (j < 1, j >= 7)
    first, last, low, high = r == 0, r == 3, r < 2, r >= 2
    tiles = [halo[0], halo[1], ghost]
    up_i, down_i = [], []
    for t in tiles:
        f = flux(t, a, 0)
        up_i.append([f[u] + C1 * t[u] for u in range(NV)])
        down_i.append([f[u] - C1 * t[u] for u in range(NV)])
    upper = o >= HALO
    after1, after2 = o == HALO, (o == HALO) | (o == HALO + 1)
    before1, before2 = o == HALO - 1, (o == HALO - 1) | (o == HALO - 2)
    result = []
    for g in range(2):
        q, nxt, prv = tiles[g], (g + 1) % 3, (g + 2) % 3
        fj, gj = flux_j(q, a)
        fk = flux(q, a, 2)
        fo = flux(own[g], a, 2)
        row = []
        for u in range(NV):
            x, y = q[u], own[g][u]
            acc = second_index(fj, gj, q, u, 1, weights, ends)
            acc = acc + rotl(jnp.where(first, up_i[nxt][u], up_i[g][u]), -SEG)
            acc = acc - rotl(jnp.where(last, down_i[prv][u], down_i[g][u]), SEG)
            acc = acc + C2 * rotl(jnp.where(low, tiles[nxt][u], x) + jnp.where(high, tiles[prv][u], x), 2 * SEG)
            t = C1 * x
            e = jnp.where(upper, fo[u] + C1 * y, fo[u] - C1 * y)
            acc = acc + rotl(jnp.where(after1, e, fk[u] + t), -1)
            acc = acc - rotl(jnp.where(before1, e, fk[u] - t), 1)
            acc = acc + C2 * (rotl(jnp.where(after2, y, x), -2) + rotl(jnp.where(before2, y, x), 2))
            row.append(acc)
        result.append(row)
    return result


def pack_ends(rows):
    r = seg()
    out = []
    for g in range(2):
        tile = []
        for v in range(NV):
            acc = rotl(rows[4 * g][v], HALO)
            for p in range(1, 4):
                acc = jnp.where(r == p, rotl(rows[4 * g + p][v], HALO + p * SEG), acc)
            tile.append(acc)
        out.append(tile)
    return out


def halo_ghost(halo, below, above, meta):
    t_lo, flip_lo, turn_lo, t_hi, flip_hi, turn_hi = meta
    r = seg()
    high_side = r < 2
    even_part = r % 2 == 0

    def turned(x):
        return jnp.where(even_part, rotl(x, SEG), rotl(x, -SEG))

    flip = jnp.where(high_side, flip_hi, flip_lo)
    picked = []
    for v in range(NV):
        wall_lo, wall_hi = turned(halo[0][v]), turned(halo[1][v])
        if v == 1:
            wall_lo, wall_hi = -wall_lo, -wall_hi
        hi = jnp.where(t_hi == 2, wall_hi, 0.0)
        hi = jnp.where(t_hi == 1, turned(below[v]), hi)
        hi = jnp.where(t_hi == 0, above[v], hi)
        lo = jnp.where(t_lo == 2, wall_lo, 0.0)
        lo = jnp.where(t_lo == 1, turned(above[v]), lo)
        lo = jnp.where(t_lo == 0, below[v], lo)
        x = jnp.where(high_side, hi, lo)
        picked.append(jnp.where(flip == 1, reverse_j(x), x))
    turn = jnp.where(high_side, turn_hi, turn_lo) == 1
    b, c = picked[2], picked[3]
    picked[2], picked[3] = jnp.where(turn, -c, b), jnp.where(turn, b, c)
    return picked


def cell_mean(x):
    x = x + jnp.where(iota_j() % 2 == 0, rots(x, -1), rots(x, 1))
    x = x + jnp.where(iota_k() % 2 == 0, rotl(x, -1), rotl(x, 1))
    return 0.125 * x


def restrict_rows(rows):
    return [[cell_mean(rows[2 * c][v] + rows[2 * c + 1][v]) for v in range(len(rows[0]))] for c in range(len(rows) // 2)]


def halo_means(tiles):
    even = seg() % 2 == 0
    tiles = [x + jnp.where(even, rotl(x, -SEG), rotl(x, SEG)) for x in tiles]
    return [cell_mean(x) for x in tiles]


def load(ref, first, count):
    return [[ref[v, first + r] for v in range(NV)] for r in range(count)]


def store(ref, first, rows):
    for r, row in enumerate(rows):
        for v in range(NV):
            ref[v, first + r] = row[v]


def load_tiles(ref):
    return [[ref[g, v] for v in range(NV)] for g in range(2)]


def store_tiles(ref, tiles):
    for g in range(2):
        for v in range(NV):
            ref[g, v] = tiles[g][v]


def table_kernel(a_ref, type_ref, rot_ref, table_ref):
    values = [a_ref[d, u, v] for d in range(3) for u in range(NV) for v in range(NV)]
    for face in range(2):
        kind, rot = type_ref[0, face], rot_ref[0, face]
        values += [kind.astype(jnp.float32), (rot % 2).astype(jnp.float32), (rot // 2 % 2).astype(jnp.float32)]
    for n, value in enumerate(values):
        table_ref[n] = jnp.full((8, 128), value, jnp.float32)


def coefficients(table_ref):
    return lambda d, u, v: table_ref[(d * NV + u) * NV + v]


def meta_of(table_ref):
    first = 3 * NV * NV
    return [table_ref[first + n] for n in range(6)]


def masked(tiles):
    o = place()
    s = lax.axis_index("sub")
    final = lax.axis_size("sub") - 1
    inside = ((o < HALO) & (s != 0)) | ((o >= HALO) & (o < 2 * HALO) & (s != final))
    return [[jnp.where(inside, x, 0.0) for x in tile] for tile in tiles]


def is_even():
    return lax.axis_index("blk") % 2 == 0


def send(ma, mb, at, first, last):
    even = is_even()
    for n, (lo, hi) in enumerate(zip(first, last)):
        ma[at + n] = jnp.where(even, hi, lo)
        mb[at + n] = jnp.where(even, lo, hi)


def put(ref, at, tiles):
    for n, x in enumerate(tiles):
        ref[at + n] = x


def receive(ga, gb, at, count):
    even = is_even()
    below, above = [], []
    for n in range(at, at + count):
        a, b = ga[n], gb[n]
        below.append(jnp.where(even, b, a))
        above.append(jnp.where(even, a, b))
    return below, above


def send_rows(ma, mb, at, rows):
    send(ma, mb, at, rows[0] + rows[1], rows[-2] + rows[-1])


def receive_rows(ga, gb, at):
    below, above = receive(ga, gb, at, 2 * NV)
    return [below[:NV], below[NV:]], [above[:NV], above[NV:]]


def halo_first(halo):
    low = seg() < 2
    return [jnp.where(low, halo[0][p], rotl(halo[0][p + 1], 64)) for p in range(0, NV, 2)]


def halo_last(halo):
    low = seg() < 2
    return [jnp.where(low, rotl(halo[1][p + 1], 64), halo[1][p]) for p in range(0, NV, 2)]


def send_halo(ma, mb, at, halo):
    send(ma, mb, at, halo_first(halo), halo_last(halo))


def receive_halo(ga, gb, at):
    below, above = receive(ga, gb, at, NV // 2)

    def spread(tiles):
        return [y for x in tiles for y in (x, rotl(x, 64))]

    return spread(below), spread(above)


def joined(first, second):
    j_even, k_even = iota_j() % 2 == 0, iota_k() % 2 == 0
    out = []
    for v in range(NV):
        x, y = (jnp.where(j_even, first[r][v], second[r][v]) for r in range(2))
        out.append(jnp.where(k_even, x, y))
    return out


def receive_coarse(ga, gb, at):
    j_even, k_even = iota_j() % 2 == 0, iota_k() % 2 == 0
    fields = ([], [])
    for tiles in receive(ga, gb, at, NV):
        rows = ([], [])
        for x in tiles:
            rows[0].append(jnp.where(k_even, x, rotl(x, 1)))
            rows[1].append(jnp.where(k_even, rotl(x, -1), x))
        fields[0].append([[jnp.where(j_even, x, rots(x, 1)) for x in row] for row in rows])
        fields[1].append([[jnp.where(j_even, rots(x, -1), x) for x in row] for row in rows])
    return fields


def prime_kernel(out_ref):
    out_ref[...] = jnp.zeros_like(out_ref)


def pack_kernel(prime_ref, q_ref, dt_ref, ends_ref, ma, mb, to_left, to_right):
    rows = load(q_ref, 0, NI)
    ends = pack_ends(rows)
    store_tiles(ends_ref, ends)
    r, lower = seg(), place() < HALO
    tiles = ends[0] + ends[1]
    for g in range(2):
        acc = rotl(dt_ref[4 * g], HALO)
        for p in range(1, 4):
            acc = jnp.where(r == p, rotl(dt_ref[4 * g + p], HALO + p * SEG), acc)
        tiles.append(acc)
    for n in range(NV + 1):
        x, y = tiles[2 * n], tiles[2 * n + 1]
        to_right[n] = jnp.where(lower, x, rotl(y, HALO))
        to_left[n] = jnp.where(lower, rotl(y, -HALO), x)
    send_rows(ma, mb, 0, rows)


def unpack(from_right, from_left):
    lower = place() < HALO
    tiles = []
    for n in range(NV + 1):
        x, y = from_left[n], from_right[n]
        tiles.append(jnp.where(lower, x, y))
        tiles.append(jnp.where(lower, rotl(x, -HALO), rotl(y, HALO)))
    halo = masked([tiles[:NV], tiles[NV : 2 * NV]])
    return halo, tiles[2 * NV :]


def advance(start, dt, twice, factor):
    return [[start[i][v] - (0.5 * factor * dt[i]) * twice[i][v] for v in range(NV)] for i in range(len(start))]


def end_rows(start, rows, halo, dt_ref, ga, gb, a, meta, factor):
    below, above = receive_rows(ga, gb, 0)
    dt = [dt_ref[i] for i in range(NI)]
    low = low_ghosts(rows, below, above, meta) + rows[:4]
    high = rows[-4:] + high_ghosts(rows, below, above, meta)
    first = advance(start[:2], dt[:2], residual2(low, halo, a, 1), factor)
    last = advance(start[-2:], dt[-2:], residual2(high, halo, a, 1, NI - 2), factor)
    return first + last


def first_ends_kernel(table_ref, q_ref, dt_ref, ga, gb, from_right, from_left, h0_ref, dth_ref, ma, mb):
    a, meta = coefficients(table_ref), meta_of(table_ref)
    h0, dth = unpack(from_right, from_left)
    store_tiles(h0_ref, h0)
    put(dth_ref, 0, dth)
    send_halo(ma, mb, 2 * NV, h0)
    rows = load(q_ref, 0, NI)
    send_rows(ma, mb, 0, end_rows(rows, rows, h0, dt_ref, ga, gb, a, meta, 0.4))


def first_kernel(table_ref, q_ref, dt_ref, ga, gb, h0_ref, t1_ref):
    a, meta = coefficients(table_ref), meta_of(table_ref)
    t0 = load(q_ref, 0, NI)
    below, above = receive_rows(ga, gb, 0)
    twice = residual2(with_ghosts(t0, below, above, meta), load_tiles(h0_ref), a, 1)
    store(t1_ref, 0, advance(t0, [dt_ref[i] for i in range(NI)], twice, 0.4))


def second_ends_kernel(table_ref, q_ref, t1_ref, h0_ref, ends_ref, dt_ref, dth_ref, ga, gb, h1_ref, ma, mb):
    a, meta = coefficients(table_ref), meta_of(table_ref)
    h0 = load_tiles(h0_ref)
    below, above = receive_halo(ga, gb, 2 * NV)
    twice = halo_residual2(h0, halo_ghost(h0, below, above, meta), load_tiles(ends_ref), a)
    h1 = masked(advance(h0, [dth_ref[g] for g in range(2)], twice, 0.4))
    store_tiles(h1_ref, h1)
    send_halo(ma, mb, 2 * NV, h1)
    t0, t1 = load(q_ref, 0, NI), load(t1_ref, 0, NI)
    send_rows(ma, mb, 0, end_rows(t0, t1, h1, dt_ref, ga, gb, a, meta, 1.0))


def second_kernel(table_ref, q_ref, t1_ref, h1_ref, dt_ref, ga, gb, t2_ref):
    a, meta = coefficients(table_ref), meta_of(table_ref)
    t0, t1 = load(q_ref, 0, NI), load(t1_ref, 0, NI)
    below, above = receive_rows(ga, gb, 0)
    twice = residual2(with_ghosts(t1, below, above, meta), load_tiles(h1_ref), a, 1)
    store(t2_ref, 0, advance(t0, [dt_ref[i] for i in range(NI)], twice, 1.0))


def first_section(rows, res, dt):
    start, mean = restrict_rows(rows), restrict_rows(res)
    c1 = []
    for c in range(len(start)):
        step = cell_mean(dt[2 * c] + dt[2 * c + 1])
        c1.append([start[c][v] - (0.4 * step) * mean[c][v] for v in range(NV)])
    return start, mean, c1


def third_kernel(
    table_ref, t1_ref, t2_ref, h0_ref, h1_ref, dt_ref, dth_ref, ga, gb, res_ref, h2_ref, start_ref, c1_ref, mean_ref, ma, mb
):
    a, meta = coefficients(table_ref), meta_of(table_ref)
    h0, h1 = load_tiles(h0_ref), load_tiles(h1_ref)
    below, above = receive_halo(ga, gb, 2 * NV)
    twice = halo_residual2(h1, halo_ghost(h1, below, above, meta), pack_ends(load(t1_ref, 0, NI)), a)
    h2 = masked(advance(h0, [dth_ref[g] for g in range(2)], twice, 1.0))
    store_tiles(h2_ref, h2)
    send_halo(ma, mb, NV, h2)
    t2 = load(t2_ref, 0, NI)
    below, above = receive_rows(ga, gb, 0)
    twice = residual2(with_ghosts(t2, below, above, meta), h2, a, 1)
    res = [[0.5 * x for x in row] for row in twice]
    store(res_ref, 0, res)
    start, mean, c1 = first_section(t2, res, [dt_ref[i] for i in range(NI)])
    store(start_ref, 0, start)
    store(mean_ref, 0, mean)
    store(c1_ref, 0, c1)
    send(ma, mb, 0, joined(c1[:2], start[:2]), joined(c1[2:], start[2:]))


def early_kernel(table_ref, start_ref, c1_ref, h2_ref, part_ref):
    a = coefficients(table_ref)
    half = NI // 2
    h2 = load_tiles(h2_ref)
    start_h = halo_means(h2[0] + h2[1])
    ghost = [[jnp.zeros((8, 128), jnp.float32)] * NV] * 2
    twice0 = residual2(ghost + load(start_ref, 0, half) + ghost, [start_h[:NV], start_h[NV:]], a, 2)
    twice1 = residual2(ghost + load(c1_ref, 0, half) + ghost, None, a, 2)
    store(part_ref, 0, [[twice1[c][v] - twice0[c][v] for v in range(NV)] for c in range(half)])


def halo_part(halo, a):
    o, k = place(), iota_k()
    high1, low1 = (o == HALO - 2) | (o == HALO - 1), (o == HALO) | (o == HALO + 1)
    high2, low2 = (o >= HALO - 4) & (o < HALO), (o >= HALO) & (o < HALO + 4)
    spread = []
    for tile in halo:
        f = flux(tile, a, 2)
        row = []
        for u in range(NV):
            x = tile[u]
            w = jnp.where(high1, rotl(f[u] + C1 * x, -2), 0.0) - jnp.where(low1, rotl(f[u] - C1 * x, 2), 0.0)
            row.append(w + C2 * (jnp.where(high2, rotl(x, -4), 0.0) + jnp.where(low2, rotl(x, 4), 0.0)))
        spread.append(row)
    near = (k < 4) | (k >= 124)
    out = []
    for c in range(NI // 2):
        g, first = 2 * c // 4, 2 * c % 4 * SEG + HALO
        out.append([jnp.where(near, rotl(spread[g][u], -first), 0.0) for u in range(NV)])
    return out


def ghost_part(low, high, a):
    fl, fh = flux(low[1], a, 0), flux(high[0], a, 0)
    rows = ([], [], [], [])
    for u in range(NV):
        rows[0].append(C1 * low[1][u] + C2 * low[0][u] - fl[u])
        rows[1].append(C2 * low[1][u])
        rows[2].append(C2 * high[0][u])
        rows[3].append(C1 * high[0][u] + C2 * high[1][u] + fh[u])
    return rows


def fourth_kernel(
    table_ref, t2_ref, h2_ref, start_ref, c1_ref, mean_ref, part_ref, dt_ref, dth_ref, res_ref, ga, gb, out_hbm, res_hbm, out_ref, sems
):
    a, meta = coefficients(table_ref), meta_of(table_ref)
    half = NI // 2
    copies = [pltpu.make_async_copy(res_ref, res_hbm, sems.at[half])]
    copies[0].start()
    h2, t2 = load_tiles(h2_ref), load(t2_ref, 0, NI)
    below, above = receive_halo(ga, gb, NV)
    twice = halo_residual2(h2, halo_ghost(h2, below, above, meta), pack_ends(t2), a)
    means = halo_means(h2[0] + h2[1] + [dth_ref[0], dth_ref[1]] + twice[0] + twice[1])
    start_h, step_h, mean_h = means[: 2 * NV], means[2 * NV : 2 * NV + 2], means[2 * NV + 2 :]
    c1_h = [start_h[t] - (0.2 * step_h[t // NV]) * mean_h[t] for t in range(2 * NV)]
    halo = halo_part(masked([c1_h[:NV], c1_h[NV:]]), a)
    ghosts = []
    for ref, (below, above) in zip((c1_ref, start_ref), receive_coarse(ga, gb, 0)):
        rows = load(ref, 0, half)
        ghosts.append(ghost_part(low_ghosts(rows, below, above, meta), high_ghosts(rows, below, above, meta), a))
    for c in range(half):
        step = cell_mean(dt_ref[2 * c] + dt_ref[2 * c + 1])
        for v in range(NV):
            twice_change = part_ref[v, c] + (ghosts[0][c][v] - ghosts[1][c][v]) + halo[c][v]
            change = -step * (0.5 * twice_change + mean_ref[v, c])
            out_ref[v, 2 * c] = t2[2 * c][v] + change
            out_ref[v, 2 * c + 1] = t2[2 * c + 1][v] + change
    for c in range(half):
        rows = pl.ds(2 * c, 2)
        copies.append(pltpu.make_async_copy(out_ref.at[:, rows], out_hbm.at[:, rows], sems.at[c]))
        copies[-1].start()
    for copy in copies:
        copy.wait()


def field(rows):
    return (NV, rows, 8, 128)


def tiles_of(*count):
    return (*count, 8, 128)


def call(kernel, arrays, outs, scalars=(), out_space=pltpu.VMEM, scratch=()):
    smem, vmem = pl.BlockSpec(memory_space=pltpu.SMEM), pl.BlockSpec(memory_space=pltpu.VMEM)
    return pl.pallas_call(
        kernel,
        out_shape=[jax.ShapeDtypeStruct(shape, jnp.float32) for shape in outs],
        in_specs=[smem] * len(scalars) + [vmem] * len(arrays),
        out_specs=[pl.BlockSpec(memory_space=out_space)] * len(outs),
        scratch_shapes=scratch,
        compiler_params=pltpu.CompilerParams(vmem_limit_bytes=VMEM_LIMIT),
    )(*scalars, *arrays)


def cycle(flow_state, timestep, coupling, face_type, face_rot):
    blocks, parts = lax.axis_size("blk"), lax.axis_size("sub")
    chip = [(b, b ^ 1) for b in range(blocks)]
    link = [(b, (b + 1) % blocks if b % 2 else (b - 1) % blocks) for b in range(blocks)]
    ahead = [(s, s + 1) for s in range(parts - 1)]
    back = [(s + 1, s) for s in range(parts - 1)]
    pair = tiles_of(2, NV)

    def exchange(ma, mb):
        gb = lax.ppermute(mb, "blk", link)
        ga = lax.ppermute(ma, "blk", chip)
        return ga, gb

    (table,) = call(table_kernel, (), (tiles_of(3 * NV * NV + 6),), (coupling, face_type, face_rot))
    (prime,) = call(prime_kernel, (), (tiles_of(114),))
    ends, ma, mb, to_left, to_right = call(
        pack_kernel,
        (prime, flow_state, timestep),
        (pair, tiles_of(2 * NV), tiles_of(2 * NV), tiles_of(NV + 1), tiles_of(NV + 1)),
    )
    ga, gb = exchange(ma, mb)
    from_right = lax.ppermute(to_left, "sub", back)
    from_left = lax.ppermute(to_right, "sub", ahead)

    message = tiles_of(2 * NV + NV // 2)
    h0, dth, ma, mb = call(
        first_ends_kernel,
        (table, flow_state, timestep, ga, gb, from_right, from_left),
        (pair, tiles_of(2), message, message),
    )
    (t1,) = call(first_kernel, (table, flow_state, timestep, ga, gb, h0), (field(NI),))
    ga, gb = exchange(ma, mb)

    h1, ma, mb = call(
        second_ends_kernel,
        (table, flow_state, t1, h0, ends, timestep, dth, ga, gb),
        (pair, message, message),
    )
    (t2,) = call(second_kernel, (table, flow_state, t1, h1, timestep, ga, gb), (field(NI),))
    ga, gb = exchange(ma, mb)

    message = tiles_of(NV + NV // 2)
    coarse = field(NI // 2)
    res, h2, start, c1, mean, ma, mb = call(
        third_kernel,
        (table, t1, t2, h0, h1, timestep, dth, ga, gb),
        (field(NI), pair, coarse, coarse, coarse, message, message),
    )
    (part,) = call(early_kernel, (table, start, c1, h2), (coarse,))
    ga, gb = exchange(ma, mb)

    updated, res = call(
        fourth_kernel,
        (table, t2, h2, start, c1, mean, part, timestep, dth, res, ga, gb),
        (field(NI), field(NI)),
        out_space=pltpu.HBM,
        scratch=(pltpu.VMEM(field(NI), jnp.float32), pltpu.SemaphoreType.DMA((NI // 2 + 1,))),
    )
    return (updated, res)


def solution(mesh):
    return jax.shard_map(
        cycle,
        mesh=mesh,
        in_specs=(
            P(None, "blk", None, "sub"),
            P("blk", None, "sub"),
            P(),
            P("blk", None),
            P("blk", None),
        ),
        out_specs=(P(None, "blk", None, "sub"), P(None, "blk", None, "sub")),
        check_vma=False,
    )
```

```python
import jax
import jax.numpy as jnp
from jax import lax
from jax.experimental import pallas as pl
from jax.experimental.pallas import tpu as pltpu
from jax.sharding import PartitionSpec as P


NV = 6
NI = 8
HALO = 10
SEG = 32
VMEM_LIMIT = 12 * 1024 * 1024

C0, C1, C2 = 0.44, -0.26, 0.04


def iota_j():
    return lax.broadcasted_iota(jnp.int32, (8, 128), 0)


def iota_k():
    return lax.broadcasted_iota(jnp.int32, (8, 128), 1)


def rotl(x, shift):
    return pltpu.roll(x, shift % 128, 1)


def rots(x, shift):
    return pltpu.roll(x, shift % 8, 0)


def reverse_j(x):
    j = iota_j()
    x = rots(x, 4)
    x = jnp.where((j // 2) % 2 == 0, rots(x, -2), rots(x, 2))
    return jnp.where(j % 2 == 0, rots(x, -1), rots(x, 1))


def ghost_rows(own2, prev2, next2, kind, flip, turn):
    nearest = []
    for r in range(2):
        picked = []
        for v in range(NV):
            wall = -own2[r][v] if v == 1 else own2[r][v]
            x = jnp.where(kind == 2, wall, 0.0)
            x = jnp.where(kind == 1, next2[r][v], x)
            x = jnp.where(kind == 0, prev2[r][v], x)
            picked.append(jnp.where(flip == 1, reverse_j(x), x))
        a, b = picked[2], picked[3]
        picked[2], picked[3] = jnp.where(turn == 1, -b, a), jnp.where(turn == 1, a, b)
        nearest.append(picked)
    return nearest


def low_ghosts(rows, below, above, meta):
    lo = ghost_rows([rows[0], rows[1]], [below[1], below[0]], [above[0], above[1]], *meta[:3])
    return [lo[1], lo[0]]


def high_ghosts(rows, below, above, meta):
    return ghost_rows([rows[-1], rows[-2]], [above[0], above[1]], [below[1], below[0]], *meta[3:])


def with_ghosts(rows, below, above, meta):
    return low_ghosts(rows, below, above, meta) + rows + high_ghosts(rows, below, above, meta)


def flux(q, a, d):
    half = 0.5 * q[1 + d]
    out = []
    for u in range(NV):
        acc = (a(d, u, u) + half) * q[u]
        for v in range(NV):
            if v != u:
                acc = acc + a(d, u, v) * q[v]
        out.append(acc)
    return out


def flux_j(q, a):
    out, mirrored = [], []
    for u in range(NV):
        even = None
        for v in range(NV):
            if v != 2:
                term = a(1, u, v) * q[v]
                even = term if even is None else even + term
        if u == 2:
            even = even + 0.5 * (q[2] * q[2])
            odd = a(1, 2, 2) * q[2]
        else:
            odd = q[2] * (a(1, u, 2) + 0.5 * q[u])
        out.append(even + odd)
        mirrored.append(even - odd)
    return out, mirrored


def j_weights(unit):
    j = iota_j() // unit
    n = 8 // unit
    out = []
    for sign in (1.0, -1.0):
        end = (j == 0) | (j == n - 1)
        centre = jnp.where(end, C0 + sign * C1, C0) + 2 * C0
        near = C1 + sign * C2
        below = jnp.where(j == 0, 0.0, jnp.where((j == 1) | (j == n - 1), near, C1))
        above = jnp.where(j == n - 1, 0.0, jnp.where((j == 0) | (j == n - 2), near, C1))
        if n == 4:
            two = None
        else:
            two = (jnp.where(j >= 2, C2, 0.0), jnp.where(j <= n - 3, C2, 0.0))
        out.append((centre, below, above, two))
    return out


def seg():
    return iota_k() // SEG


def place():
    return iota_k() % SEG


def second_index(fj, gj, q, u, unit, weights, ends):
    centre, below, above, two = weights[1 if u == 2 else 0]
    x = q[u]
    acc = centre * x + below * rots(x, unit) + above * rots(x, -unit)
    if two is None:
        acc = acc + C2 * rots(x, 4)
    else:
        acc = acc + two[0] * rots(x, 2) + two[1] * rots(x, -2)
    up = jnp.where(ends[1], gj[u], rots(fj[u], -unit))
    down = jnp.where(ends[0], gj[u], rots(fj[u], unit))
    return acc + (up - down)


def residual2(padded, halo, a, unit, start=0):
    n = len(padded) - 4
    k, j = iota_k(), iota_j()
    weights = j_weights(unit)
    ends = (j < unit, j >= 8 - unit)
    low1, low2 = k < unit, k < 2 * unit
    high1, high2 = k >= 128 - unit, k >= 128 - 2 * unit
    upper = place() >= HALO
    edge = []
    for tile in halo or ():
        f = flux(tile, a, 2)
        edge.append([jnp.where(upper, f[u] + C1 * tile[u], f[u] - C1 * tile[u]) for u in range(NV)])
    beside = []
    for i in range(n if halo else 0):
        g, first = unit * (start + i) // 4, unit * (start + i) % 4 * SEG + HALO
        beside.append([(rotl(halo[g][u], -first), rotl(edge[g][u], -first)) for u in range(NV)])
    fi = {m: flux(padded[m], a, 0) for m in range(1, n + 3)}
    result = []
    for i in range(n):
        m = i + 2
        q = padded[m]
        fj, gj = flux_j(q, a)
        fk = flux(q, a, 2)
        row = []
        for u in range(NV):
            x = q[u]
            s, e = beside[i][u] if halo else (0.0, 0.0)
            acc = second_index(fj, gj, q, u, unit, weights, ends)
            acc = acc + (fi[m + 1][u] - fi[m - 1][u])
            acc = acc + C1 * (padded[m + 1][u] + padded[m - 1][u]) + C2 * (padded[m + 2][u] + padded[m - 2][u])
            t = C1 * x
            acc = acc + rotl(jnp.where(low1, e, fk[u] + t), -unit)
            acc = acc - rotl(jnp.where(high1, e, fk[u] - t), unit)
            acc = acc + C2 * (rotl(jnp.where(low2, s, x), -2 * unit) + rotl(jnp.where(high2, s, x), 2 * unit))
            row.append(acc)
        result.append(row)
    return result


def halo_residual2(halo, ghost, own, a):
    r, o = seg(), place()
    j = iota_j()
    weights = j_weights(1)
    ends = (j < 1, j >= 7)
    first, last, low, high = r == 0, r == 3, r < 2, r >= 2
    tiles = [halo[0], halo[1], ghost]
    up_i, down_i = [], []
    for t in tiles:
        f = flux(t, a, 0)
        up_i.append([f[u] + C1 * t[u] for u in range(NV)])
        down_i.append([f[u] - C1 * t[u] for u in range(NV)])
    upper = o >= HALO
    after1, after2 = o == HALO, (o == HALO) | (o == HALO + 1)
    before1, before2 = o == HALO - 1, (o == HALO - 1) | (o == HALO - 2)
    result = []
    for g in range(2):
        q, nxt, prv = tiles[g], (g + 1) % 3, (g + 2) % 3
        fj, gj = flux_j(q, a)
        fk = flux(q, a, 2)
        fo = flux(own[g], a, 2)
        row = []
        for u in range(NV):
            x, y = q[u], own[g][u]
            acc = second_index(fj, gj, q, u, 1, weights, ends)
            acc = acc + rotl(jnp.where(first, up_i[nxt][u], up_i[g][u]), -SEG)
            acc = acc - rotl(jnp.where(last, down_i[prv][u], down_i[g][u]), SEG)
            acc = acc + C2 * rotl(jnp.where(low, tiles[nxt][u], x) + jnp.where(high, tiles[prv][u], x), 2 * SEG)
            t = C1 * x
            e = jnp.where(upper, fo[u] + C1 * y, fo[u] - C1 * y)
            acc = acc + rotl(jnp.where(after1, e, fk[u] + t), -1)
            acc = acc - rotl(jnp.where(before1, e, fk[u] - t), 1)
            acc = acc + C2 * (rotl(jnp.where(after2, y, x), -2) + rotl(jnp.where(before2, y, x), 2))
            row.append(acc)
        result.append(row)
    return result


def pack_ends(rows):
    r = seg()
    out = []
    for g in range(2):
        tile = []
        for v in range(NV):
            acc = rotl(rows[4 * g][v], HALO)
            for p in range(1, 4):
                acc = jnp.where(r == p, rotl(rows[4 * g + p][v], HALO + p * SEG), acc)
            tile.append(acc)
        out.append(tile)
    return out


def halo_ghost(halo, below, above, meta):
    t_lo, flip_lo, turn_lo, t_hi, flip_hi, turn_hi = meta
    r = seg()
    high_side = r < 2
    even_part = r % 2 == 0

    def turned(x):
        return jnp.where(even_part, rotl(x, SEG), rotl(x, -SEG))

    flip = jnp.where(high_side, flip_hi, flip_lo)
    picked = []
    for v in range(NV):
        wall_lo, wall_hi = turned(halo[0][v]), turned(halo[1][v])
        if v == 1:
            wall_lo, wall_hi = -wall_lo, -wall_hi
        hi = jnp.where(t_hi == 2, wall_hi, 0.0)
        hi = jnp.where(t_hi == 1, turned(below[v]), hi)
        hi = jnp.where(t_hi == 0, above[v], hi)
        lo = jnp.where(t_lo == 2, wall_lo, 0.0)
        lo = jnp.where(t_lo == 1, turned(above[v]), lo)
        lo = jnp.where(t_lo == 0, below[v], lo)
        x = jnp.where(high_side, hi, lo)
        picked.append(jnp.where(flip == 1, reverse_j(x), x))
    turn = jnp.where(high_side, turn_hi, turn_lo) == 1
    b, c = picked[2], picked[3]
    picked[2], picked[3] = jnp.where(turn, -c, b), jnp.where(turn, b, c)
    return picked


def cell_mean(x):
    x = x + jnp.where(iota_j() % 2 == 0, rots(x, -1), rots(x, 1))
    x = x + jnp.where(iota_k() % 2 == 0, rotl(x, -1), rotl(x, 1))
    return 0.125 * x


def restrict_rows(rows):
    return [[cell_mean(rows[2 * c][v] + rows[2 * c + 1][v]) for v in range(len(rows[0]))] for c in range(len(rows) // 2)]


def halo_means(tiles):
    even = seg() % 2 == 0
    tiles = [x + jnp.where(even, rotl(x, -SEG), rotl(x, SEG)) for x in tiles]
    return [cell_mean(x) for x in tiles]


def load(ref, first, count):
    return [[ref[v, first + r] for v in range(NV)] for r in range(count)]


def store(ref, first, rows):
    for r, row in enumerate(rows):
        for v in range(NV):
            ref[v, first + r] = row[v]


def load_tiles(ref):
    return [[ref[g, v] for v in range(NV)] for g in range(2)]


def store_tiles(ref, tiles):
    for g in range(2):
        for v in range(NV):
            ref[g, v] = tiles[g][v]


def table_kernel(a_ref, type_ref, rot_ref, table_ref):
    values = [a_ref[d, u, v] for d in range(3) for u in range(NV) for v in range(NV)]
    for face in range(2):
        kind, rot = type_ref[0, face], rot_ref[0, face]
        values += [kind.astype(jnp.float32), (rot % 2).astype(jnp.float32), (rot // 2 % 2).astype(jnp.float32)]
    for n, value in enumerate(values):
        table_ref[n] = jnp.full((8, 128), value, jnp.float32)


def coefficients(table_ref):
    return lambda d, u, v: table_ref[(d * NV + u) * NV + v]


def meta_of(table_ref):
    first = 3 * NV * NV
    return [table_ref[first + n] for n in range(6)]


def masked(tiles):
    o = place()
    s = lax.axis_index("sub")
    final = lax.axis_size("sub") - 1
    inside = ((o < HALO) & (s != 0)) | ((o >= HALO) & (o < 2 * HALO) & (s != final))
    return [[jnp.where(inside, x, 0.0) for x in tile] for tile in tiles]


def is_even():
    return lax.axis_index("blk") % 2 == 0


def send(ma, mb, at, first, last):
    even = is_even()
    for n, (lo, hi) in enumerate(zip(first, last)):
        ma[at + n] = jnp.where(even, hi, lo)
        mb[at + n] = jnp.where(even, lo, hi)


def put(ref, at, tiles):
    for n, x in enumerate(tiles):
        ref[at + n] = x


def receive(ga, gb, at, count):
    even = is_even()
    below, above = [], []
    for n in range(at, at + count):
        a, b = ga[n], gb[n]
        below.append(jnp.where(even, b, a))
        above.append(jnp.where(even, a, b))
    return below, above


def send_rows(ma, mb, at, rows):
    send(ma, mb, at, rows[0] + rows[1], rows[-2] + rows[-1])


def receive_rows(ga, gb, at):
    below, above = receive(ga, gb, at, 2 * NV)
    return [below[:NV], below[NV:]], [above[:NV], above[NV:]]


def halo_first(halo):
    low = seg() < 2
    return [jnp.where(low, halo[0][p], rotl(halo[0][p + 1], 64)) for p in range(0, NV, 2)]


def halo_last(halo):
    low = seg() < 2
    return [jnp.where(low, rotl(halo[1][p + 1], 64), halo[1][p]) for p in range(0, NV, 2)]


def send_halo(ma, mb, at, halo):
    send(ma, mb, at, halo_first(halo), halo_last(halo))


def receive_halo(ga, gb, at):
    below, above = receive(ga, gb, at, NV // 2)

    def spread(tiles):
        return [y for x in tiles for y in (x, rotl(x, 64))]

    return spread(below), spread(above)


def joined(first, second):
    j_even, k_even = iota_j() % 2 == 0, iota_k() % 2 == 0
    out = []
    for v in range(NV):
        x, y = (jnp.where(j_even, first[r][v], second[r][v]) for r in range(2))
        out.append(jnp.where(k_even, x, y))
    return out


def receive_coarse(ga, gb, at):
    j_even, k_even = iota_j() % 2 == 0, iota_k() % 2 == 0
    fields = ([], [])
    for tiles in receive(ga, gb, at, NV):
        rows = ([], [])
        for x in tiles:
            rows[0].append(jnp.where(k_even, x, rotl(x, 1)))
            rows[1].append(jnp.where(k_even, rotl(x, -1), x))
        fields[0].append([[jnp.where(j_even, x, rots(x, 1)) for x in row] for row in rows])
        fields[1].append([[jnp.where(j_even, rots(x, -1), x) for x in row] for row in rows])
    return fields


def prime_kernel(out_ref):
    out_ref[...] = jnp.zeros_like(out_ref)


def pack_kernel(prime_ref, q_ref, dt_ref, ma, mb):
    rows = [[q_ref[v, i] for v in range(NV)] for i in (0, 1, NI - 2, NI - 1)]
    send_rows(ma, mb, 0, rows)


def side_kernel(q_ref, dt_ref, ends_ref, to_left, to_right):
    ends = pack_ends(load(q_ref, 0, NI))
    store_tiles(ends_ref, ends)
    r, lower = seg(), place() < HALO
    tiles = ends[0] + ends[1]
    for g in range(2):
        acc = rotl(dt_ref[4 * g], HALO)
        for p in range(1, 4):
            acc = jnp.where(r == p, rotl(dt_ref[4 * g + p], HALO + p * SEG), acc)
        tiles.append(acc)
    for n in range(NV + 1):
        x, y = tiles[2 * n], tiles[2 * n + 1]
        to_right[n] = jnp.where(lower, x, rotl(y, HALO))
        to_left[n] = jnp.where(lower, rotl(y, -HALO), x)


def unpack(from_right, from_left):
    lower = place() < HALO
    tiles = []
    for n in range(NV + 1):
        x, y = from_left[n], from_right[n]
        tiles.append(jnp.where(lower, x, y))
        tiles.append(jnp.where(lower, rotl(x, -HALO), rotl(y, HALO)))
    halo = masked([tiles[:NV], tiles[NV : 2 * NV]])
    return halo, tiles[2 * NV :]


def advance(start, dt, twice, factor):
    return [[start[i][v] - (0.5 * factor * dt[i]) * twice[i][v] for v in range(NV)] for i in range(len(start))]


def end_rows(start, rows, halo, dt_ref, ga, gb, a, meta, factor):
    below, above = receive_rows(ga, gb, 0)
    dt = [dt_ref[i] for i in range(NI)]
    low = low_ghosts(rows, below, above, meta) + rows[:4]
    high = rows[-4:] + high_ghosts(rows, below, above, meta)
    first = advance(start[:2], dt[:2], residual2(low, halo, a, 1), factor)
    last = advance(start[-2:], dt[-2:], residual2(high, halo, a, 1, NI - 2), factor)
    return first + last


def first_ends_kernel(table_ref, q_ref, dt_ref, ga, gb, from_right, from_left, h0_ref, dth_ref, ma, mb):
    a, meta = coefficients(table_ref), meta_of(table_ref)
    h0, dth = unpack(from_right, from_left)
    store_tiles(h0_ref, h0)
    put(dth_ref, 0, dth)
    send_halo(ma, mb, 2 * NV, h0)
    rows = load(q_ref, 0, NI)
    send_rows(ma, mb, 0, end_rows(rows, rows, h0, dt_ref, ga, gb, a, meta, 0.4))


def first_kernel(table_ref, q_ref, dt_ref, ga, gb, h0_ref, t1_ref):
    a, meta = coefficients(table_ref), meta_of(table_ref)
    t0 = load(q_ref, 0, NI)
    below, above = receive_rows(ga, gb, 0)
    twice = residual2(with_ghosts(t0, below, above, meta), load_tiles(h0_ref), a, 1)
    store(t1_ref, 0, advance(t0, [dt_ref[i] for i in range(NI)], twice, 0.4))


def second_ends_kernel(table_ref, q_ref, t1_ref, h0_ref, ends_ref, dt_ref, dth_ref, ga, gb, h1_ref, ma, mb):
    a, meta = coefficients(table_ref), meta_of(table_ref)
    h0 = load_tiles(h0_ref)
    below, above = receive_halo(ga, gb, 2 * NV)
    twice = halo_residual2(h0, halo_ghost(h0, below, above, meta), load_tiles(ends_ref), a)
    h1 = masked(advance(h0, [dth_ref[g] for g in range(2)], twice, 0.4))
    store_tiles(h1_ref, h1)
    send_halo(ma, mb, 2 * NV, h1)
    t0, t1 = load(q_ref, 0, NI), load(t1_ref, 0, NI)
    send_rows(ma, mb, 0, end_rows(t0, t1, h1, dt_ref, ga, gb, a, meta, 1.0))


def second_kernel(table_ref, q_ref, t1_ref, h1_ref, dt_ref, ga, gb, t2_ref):
    a, meta = coefficients(table_ref), meta_of(table_ref)
    t0, t1 = load(q_ref, 0, NI), load(t1_ref, 0, NI)
    below, above = receive_rows(ga, gb, 0)
    twice = residual2(with_ghosts(t1, below, above, meta), load_tiles(h1_ref), a, 1)
    store(t2_ref, 0, advance(t0, [dt_ref[i] for i in range(NI)], twice, 1.0))


def first_section(rows, res, dt):
    start, mean = restrict_rows(rows), restrict_rows(res)
    c1 = []
    for c in range(len(start)):
        step = cell_mean(dt[2 * c] + dt[2 * c + 1])
        c1.append([start[c][v] - (0.4 * step) * mean[c][v] for v in range(NV)])
    return start, mean, c1


def third_kernel(
    table_ref, t1_ref, t2_ref, h0_ref, h1_ref, dt_ref, dth_ref, ga, gb, res_ref, h2_ref, start_ref, c1_ref, mean_ref, ma, mb
):
    a, meta = coefficients(table_ref), meta_of(table_ref)
    h0, h1 = load_tiles(h0_ref), load_tiles(h1_ref)
    below, above = receive_halo(ga, gb, 2 * NV)
    twice = halo_residual2(h1, halo_ghost(h1, below, above, meta), pack_ends(load(t1_ref, 0, NI)), a)
    h2 = masked(advance(h0, [dth_ref[g] for g in range(2)], twice, 1.0))
    store_tiles(h2_ref, h2)
    send_halo(ma, mb, NV, h2)
    t2 = load(t2_ref, 0, NI)
    below, above = receive_rows(ga, gb, 0)
    twice = residual2(with_ghosts(t2, below, above, meta), h2, a, 1)
    res = [[0.5 * x for x in row] for row in twice]
    store(res_ref, 0, res)
    start, mean, c1 = first_section(t2, res, [dt_ref[i] for i in range(NI)])
    store(start_ref, 0, start)
    store(mean_ref, 0, mean)
    store(c1_ref, 0, c1)
    send(ma, mb, 0, joined(c1[:2], start[:2]), joined(c1[2:], start[2:]))


def early_kernel(table_ref, start_ref, c1_ref, h2_ref, part_ref):
    a = coefficients(table_ref)
    half = NI // 2
    h2 = load_tiles(h2_ref)
    start_h = halo_means(h2[0] + h2[1])
    ghost = [[jnp.zeros((8, 128), jnp.float32)] * NV] * 2
    twice0 = residual2(ghost + load(start_ref, 0, half) + ghost, [start_h[:NV], start_h[NV:]], a, 2)
    twice1 = residual2(ghost + load(c1_ref, 0, half) + ghost, None, a, 2)
    store(part_ref, 0, [[twice1[c][v] - twice0[c][v] for v in range(NV)] for c in range(half)])


def halo_part(halo, a):
    o, k = place(), iota_k()
    high1, low1 = (o == HALO - 2) | (o == HALO - 1), (o == HALO) | (o == HALO + 1)
    high2, low2 = (o >= HALO - 4) & (o < HALO), (o >= HALO) & (o < HALO + 4)
    spread = []
    for tile in halo:
        f = flux(tile, a, 2)
        row = []
        for u in range(NV):
            x = tile[u]
            w = jnp.where(high1, rotl(f[u] + C1 * x, -2), 0.0) - jnp.where(low1, rotl(f[u] - C1 * x, 2), 0.0)
            row.append(w + C2 * (jnp.where(high2, rotl(x, -4), 0.0) + jnp.where(low2, rotl(x, 4), 0.0)))
        spread.append(row)
    near = (k < 4) | (k >= 124)
    out = []
    for c in range(NI // 2):
        g, first = 2 * c // 4, 2 * c % 4 * SEG + HALO
        out.append([jnp.where(near, rotl(spread[g][u], -first), 0.0) for u in range(NV)])
    return out


def ghost_part(low, high, a):
    fl, fh = flux(low[1], a, 0), flux(high[0], a, 0)
    rows = ([], [], [], [])
    for u in range(NV):
        rows[0].append(C1 * low[1][u] + C2 * low[0][u] - fl[u])
        rows[1].append(C2 * low[1][u])
        rows[2].append(C2 * high[0][u])
        rows[3].append(C1 * high[0][u] + C2 * high[1][u] + fh[u])
    return rows


def fourth_kernel(
    table_ref, t2_ref, h2_ref, start_ref, c1_ref, mean_ref, part_ref, dt_ref, dth_ref, res_ref, ga, gb, out_hbm, res_hbm, out_ref, sems
):
    a, meta = coefficients(table_ref), meta_of(table_ref)
    half = NI // 2
    copies = [pltpu.make_async_copy(res_ref, res_hbm, sems.at[half])]
    copies[0].start()
    h2, t2 = load_tiles(h2_ref), load(t2_ref, 0, NI)
    below, above = receive_halo(ga, gb, NV)
    twice = halo_residual2(h2, halo_ghost(h2, below, above, meta), pack_ends(t2), a)
    means = halo_means(h2[0] + h2[1] + [dth_ref[0], dth_ref[1]] + twice[0] + twice[1])
    start_h, step_h, mean_h = means[: 2 * NV], means[2 * NV : 2 * NV + 2], means[2 * NV + 2 :]
    c1_h = [start_h[t] - (0.2 * step_h[t // NV]) * mean_h[t] for t in range(2 * NV)]
    halo = halo_part(masked([c1_h[:NV], c1_h[NV:]]), a)
    ghosts = []
    for ref, (below, above) in zip((c1_ref, start_ref), receive_coarse(ga, gb, 0)):
        rows = load(ref, 0, half)
        ghosts.append(ghost_part(low_ghosts(rows, below, above, meta), high_ghosts(rows, below, above, meta), a))
    for c in range(half):
        step = cell_mean(dt_ref[2 * c] + dt_ref[2 * c + 1])
        for v in range(NV):
            twice_change = part_ref[v, c] + (ghosts[0][c][v] - ghosts[1][c][v]) + halo[c][v]
            change = -step * (0.5 * twice_change + mean_ref[v, c])
            out_ref[v, 2 * c] = t2[2 * c][v] + change
            out_ref[v, 2 * c + 1] = t2[2 * c + 1][v] + change
    for c in range(half):
        rows = pl.ds(2 * c, 2)
        copies.append(pltpu.make_async_copy(out_ref.at[:, rows], out_hbm.at[:, rows], sems.at[c]))
        copies[-1].start()
    for copy in copies:
        copy.wait()


def field(rows):
    return (NV, rows, 8, 128)


def tiles_of(*count):
    return (*count, 8, 128)


def call(kernel, arrays, outs, scalars=(), out_space=pltpu.VMEM, scratch=()):
    smem, vmem = pl.BlockSpec(memory_space=pltpu.SMEM), pl.BlockSpec(memory_space=pltpu.VMEM)
    return pl.pallas_call(
        kernel,
        out_shape=[jax.ShapeDtypeStruct(shape, jnp.float32) for shape in outs],
        in_specs=[smem] * len(scalars) + [vmem] * len(arrays),
        out_specs=[pl.BlockSpec(memory_space=out_space)] * len(outs),
        scratch_shapes=scratch,
        compiler_params=pltpu.CompilerParams(vmem_limit_bytes=VMEM_LIMIT),
    )(*scalars, *arrays)


def cycle(flow_state, timestep, coupling, face_type, face_rot):
    blocks, parts = lax.axis_size("blk"), lax.axis_size("sub")
    chip = [(b, b ^ 1) for b in range(blocks)]
    link = [(b, (b + 1) % blocks if b % 2 else (b - 1) % blocks) for b in range(blocks)]
    ahead = [(s, s + 1) for s in range(parts - 1)]
    back = [(s + 1, s) for s in range(parts - 1)]
    pair = tiles_of(2, NV)

    def exchange(ma, mb):
        gb = lax.ppermute(mb, "blk", link)
        ga = lax.ppermute(ma, "blk", chip)
        return ga, gb

    (table,) = call(table_kernel, (), (tiles_of(3 * NV * NV + 6),), (coupling, face_type, face_rot))
    (prime,) = call(prime_kernel, (), (tiles_of(114),))
    ma, mb = call(pack_kernel, (prime, flow_state, timestep), (tiles_of(2 * NV), tiles_of(2 * NV)))
    ends, to_left, to_right = call(
        side_kernel, (flow_state, timestep), (pair, tiles_of(NV + 1), tiles_of(NV + 1))
    )
    ga, gb = exchange(ma, mb)
    from_right = lax.ppermute(to_left, "sub", back)
    from_left = lax.ppermute(to_right, "sub", ahead)

    message = tiles_of(2 * NV + NV // 2)
    h0, dth, ma, mb = call(
        first_ends_kernel,
        (table, flow_state, timestep, ga, gb, from_right, from_left),
        (pair, tiles_of(2), message, message),
    )
    (t1,) = call(first_kernel, (table, flow_state, timestep, ga, gb, h0), (field(NI),))
    ga, gb = exchange(ma, mb)

    h1, ma, mb = call(
        second_ends_kernel,
        (table, flow_state, t1, h0, ends, timestep, dth, ga, gb),
        (pair, message, message),
    )
    (t2,) = call(second_kernel, (table, flow_state, t1, h1, timestep, ga, gb), (field(NI),))
    ga, gb = exchange(ma, mb)

    message = tiles_of(NV + NV // 2)
    coarse = field(NI // 2)
    res, h2, start, c1, mean, ma, mb = call(
        third_kernel,
        (table, t1, t2, h0, h1, timestep, dth, ga, gb),
        (field(NI), pair, coarse, coarse, coarse, message, message),
    )
    (part,) = call(early_kernel, (table, start, c1, h2), (coarse,))
    ga, gb = exchange(ma, mb)

    updated, res = call(
        fourth_kernel,
        (table, t2, h2, start, c1, mean, part, timestep, dth, res, ga, gb),
        (field(NI), field(NI)),
        out_space=pltpu.HBM,
        scratch=(pltpu.VMEM(field(NI), jnp.float32), pltpu.SemaphoreType.DMA((NI // 2 + 1,))),
    )
    return (updated, res)


def solution(mesh):
    return jax.shard_map(
        cycle,
        mesh=mesh,
        in_specs=(
            P(None, "blk", None, "sub"),
            P("blk", None, "sub"),
            P(),
            P("blk", None),
            P("blk", None),
        ),
        out_specs=(P(None, "blk", None, "sub"), P(None, "blk", None, "sub")),
        check_vma=False,
    )
```
